32 devices in a mesh: grp: 2 (over y), row: 4 (over z), col: 4 (over x, core).
Axes of the slice: x: 2, y: 2, z: 4, core: 2. Of those that a mesh axis runs over, the one named last changes fastest.
Arguments:
- z_spectra: float32 [32, 2, 2, 4096], P(('grp', 'row', 'col')), parts along dimension 0, may hold values from -6 to 6
- n_spectra: float32 [32, 2, 2, 4096], P(('grp', 'col', 'row')), parts along dimension 0, may hold values from -6 to 6
- z_flags: int32 [32, 2], P(('grp', 'row', 'col')), parts along dimension 0, may hold values 0 or 1
- n_flags: int32 [32, 2], P(('grp', 'col', 'row')), parts along dimension 0, may hold values 0 or 1
- pair_mask: int32 [32, 16], P(('grp', 'row'), 'col'), parts along dimension 0, may hold values 0 or 1
Outputs:
- stacks: float32 [32, 16, 512], P(('grp', 'row'), 'col'), parts along dimension 0
The draws below stay inside these ranges and needn't reach their ends.
There are 2 independent parts, one for each index of `grp`. The reference program is written for one: setup_inputs(seed, part) draws one part's arguments, and reference() takes and returns one part's arrays. A program takes and returns all parts, laid end to end along the dimension named above; each array names one. Nothing has to cross between parts.
All inputs are finite; a program needn't handle non-finite values. No bound on the sum of `z_flags` or of `n_flags` or of `pair_mask` on one device may be relied on, other than what follows from the above.
Results may differ from the reference program's by a relative error of at most 0.0037.
Values sent between devices are 32-bit elements; how exact they have to be, the bound alone decides.
A program may use at most 64 MiB of HBM per device.

```python
import math
import jax
import jax.numpy as jnp
from jax import lax

F = 4096
LAGS = 512
WIN = 2
S = 16


def place_ends(drawn, own_key, smallest, high):
    longest = drawn.shape.index(max(drawn.shape))
    spots = []
    for shift in (0, 1):
        where = [jax.random.randint(jax.random.fold_in(own_key, axis), (), 0, length) for axis, length in enumerate(drawn.shape)]
        where[longest] = (where[longest] + shift) % drawn.shape[longest]
        spots.append(tuple(where))
    return drawn.at[spots[0]].set(smallest).at[spots[1]].set(high)


def block_levels(stream_key, shape, pieces, least, high):
    def one(dim, blocks):
        steps = jax.random.uniform(jax.random.fold_in(jax.random.fold_in(stream_key, 6), dim), (blocks,), jnp.float32, least / len(pieces), high / len(pieces))
        return jnp.repeat(jnp.exp(steps), shape[dim] // blocks).reshape((-1,) + (1,) * (len(shape) - dim - 1))

    gain = one(*pieces[0])
    for cut in pieces[1:]:
        gain = gain * one(*cut)
    return gain


def scatter_about(stream_key, dims, scale, most, pieces=(), kind=jnp.bfloat16):
    loudness = block_levels(stream_key, dims, pieces, -0.22, 0.18) if pieces else 1.0
    array = jax.random.normal(stream_key, dims, jnp.float32) * scale * loudness
    return jnp.minimum(jnp.maximum(array, -most), most).astype(kind)


def setup_inputs(seed: int = 0, part: int = 0) -> dict:
    streams_of = jax.random.split(jax.random.key(seed), 6)
    part_splits = jax.random.split(jax.random.fold_in(streams_of[5], part), 6)
    z_spectra = scatter_about(part_splits[0], (S, WIN, 2, F), 1.0, 6.0, ((0, 16),), jnp.float32)
    n_spectra = scatter_about(part_splits[1], (S, WIN, 2, F), 1.0, 6.0, ((0, 16),), jnp.float32)
    z_flags = place_ends((jax.random.randint(part_splits[2], (S, WIN), 0, 5) < 4).astype(jnp.int32), jax.random.fold_in(part_splits[2], 1), 0, 1)
    n_flags = place_ends((jax.random.randint(part_splits[3], (S, WIN), 0, 5) < 4).astype(jnp.int32), jax.random.fold_in(part_splits[3], 1), 0, 1)
    pair_mask = place_ends((jax.random.randint(part_splits[4], (S, S), 0, 4) < 3).astype(jnp.int32), jax.random.fold_in(part_splits[4], 1), 0, 1)
    return {"z_spectra": z_spectra, "n_spectra": n_spectra, "z_flags": z_flags, "n_flags": n_flags, "pair_mask": pair_mask}


def lag_table(first_bin, bin_count, total_bins, lag_count):
    freq_bins = first_bin + jnp.arange(bin_count, dtype=jnp.int32)
    lag_steps = jnp.arange(lag_count, dtype=jnp.int32) - lag_count // 2
    phase_index = freq_bins[:, None] * lag_steps[None, :] % (2 * total_bins)
    angles = phase_index.astype(jnp.float32) * (math.pi / total_bins)
    weight = jnp.where(freq_bins == 0, 1.0, 2.0).astype(jnp.float32)[:, None]
    return jnp.concatenate([weight * jnp.cos(angles), -weight * jnp.sin(angles)], 0).astype(jnp.bfloat16)

def correlate(row_spec, col_spec, lag_tab):
    z_real = row_spec[:, None, :, 0, :]
    z_imag = row_spec[:, None, :, 1, :]
    n_real = col_spec[None, :, :, 0, :]
    n_imag = col_spec[None, :, :, 1, :]
    real_part = z_real * n_real + z_imag * n_imag
    imag_part = z_imag * n_real - z_real * n_imag
    row_count, col_count, windows, bins = real_part.shape
    cross_spec = jnp.stack([real_part, imag_part], 3).astype(jnp.bfloat16)
    merged = cross_spec.reshape(row_count * col_count * windows, 2 * bins)
    product = jnp.dot(merged, lag_tab, preferred_element_type=jnp.float32)
    return product.reshape(row_count, col_count, windows, lag_tab.shape[1])

def stack_windows(corr, pair_marks):
    spread = jnp.sqrt(lax.optimization_barrier(jnp.mean(corr * corr, -1, keepdims=True)) + 1e-05)
    unit_corr = corr / spread
    window_count = jnp.maximum(lax.optimization_barrier(jnp.sum(pair_marks, -1)), 1.0)
    summed = lax.optimization_barrier(jnp.sum(pair_marks[..., None] * unit_corr, -2))
    return summed / window_count[..., None]

def reference(z_spectra, n_spectra, z_flags, n_flags, pair_mask):
    lag_tab = lag_table(0, F, F, LAGS)
    z_marks = z_flags.astype(jnp.float32)
    n_marks = n_flags.astype(jnp.float32)

    def one_station(inputs):
        z_row, z_mark = inputs
        corr = correlate(z_row[None], n_spectra, lag_tab)[0]
        return stack_windows(corr, z_mark[None, :] * n_marks)
    stacked = lax.map(one_station, (z_spectra, z_marks))
    return stacked * pair_mask.astype(jnp.float32)[..., None]
```

```python
import functools
import math

import jax
import jax.numpy as jnp
import numpy as np
from jax import lax
from jax.experimental import pallas as pl
from jax.experimental.pallas import tpu as pltpu
from jax.sharding import PartitionSpec as P

LAGS = 512
LANES = 128
MESH = pl.DeviceIdType.MESH
REACH = 3


def tables(bins):
    rows = bins // LANES
    period = 2 * rows
    blocks = LAGS // period
    kt, short = np.arange(rows), np.arange(period)
    phi = 2 * np.pi * ((short[:, None] * kt[None, :]) % period) / period
    inner = np.block([[np.cos(phi), -np.sin(phi)], [np.sin(phi), np.cos(phi)]])
    lane = np.arange(LANES)
    psi = np.pi * (short[:, None] * lane[None, :]) / bins
    turn = np.stack([np.cos(psi), np.sin(psi)]).astype(np.float32)
    split = LANES // period
    hop = np.arange(blocks).reshape(-1, split).T.reshape(-1) - blocks // 2
    chi = np.pi * ((period * hop[:, None] * lane[None, :]) % (2 * bins)) / bins
    outer = np.concatenate([np.cos(chi), -np.sin(chi)], 1).astype(np.float32)
    high = outer.astype(jnp.bfloat16)
    low = (outer - high.astype(np.float32)).astype(jnp.bfloat16)
    return inner.astype(jnp.bfloat16), turn, np.concatenate([high, low], 0)


def kernel(R, C, reach, z_hbm, n_hbm, zf_hbm, nf_hbm, mask_hbm, inner_hbm, turn_hbm, outer_hbm, out_ref,
           z_buf, n_buf, zf_buf, nf_buf, mask_buf, inner, turn, outer,
           load_sem, z_send, z_recv, zf_send, zf_recv, right_send, left_send, n_recv,
           rf_send, lf_send, nf_recv, own_send, own_f_send, row_ready, col_ready, turn_sem, go_sem):
    row, col = lax.axis_index("row"), lax.axis_index("col")
    W = z_buf.shape[1]
    bin_rows = z_buf.shape[2] // 2
    period = inner.shape[0] // 2
    blocks = outer.shape[0] // 2

    loads = [
        pltpu.make_async_copy(n_hbm.at[0], n_buf.at[row], load_sem.at[0]),
        pltpu.make_async_copy(z_hbm.at[0], z_buf.at[col], load_sem.at[1]),
        pltpu.make_async_copy(nf_hbm, nf_buf.at[row], load_sem.at[2]),
        pltpu.make_async_copy(zf_hbm, zf_buf.at[col], load_sem.at[3]),
        pltpu.make_async_copy(mask_hbm, mask_buf, load_sem.at[4]),
        pltpu.make_async_copy(inner_hbm, inner, load_sem.at[5]),
        pltpu.make_async_copy(turn_hbm, turn, load_sem.at[6]),
        pltpu.make_async_copy(outer_hbm, outer, load_sem.at[7]),
    ]
    for load in loads:
        load.start()

    has_left, has_right = row > 0, row < R - 1
    barrier = pltpu.get_barrier_semaphore()
    hops = range(1, reach + 1)

    def there(hop):
        return (row + hop < R) if hop > 0 else (row + hop >= 0)

    for hop in hops:
        @pl.when(there(hop))
        def _():
            pl.semaphore_signal(barrier, inc=1, device_id={"row": row + hop}, device_id_type=MESH)

    for step in range(1, C):
        @pl.when(col + step < C)
        def _():
            pl.semaphore_signal(barrier, inc=1, device_id={"col": col + step}, device_id_type=MESH)

    ahead = col + jnp.minimum(row, reach)

    @pl.when(ahead > 0)
    def _():
        pl.semaphore_wait(barrier, ahead)

    for hop in hops:
        @pl.when(there(-hop))
        def _():
            pl.semaphore_signal(row_ready.at[hop], inc=1, device_id={"row": row - hop}, device_id_type=MESH)

    for step in range(1, C):
        @pl.when(col >= step)
        def _():
            pl.semaphore_signal(col_ready.at[step], inc=1, device_id={"col": col - step}, device_id_type=MESH)

    def spectrum(owner, w, send, to):
        return pltpu.make_async_remote_copy(
            n_buf.at[owner, w], n_buf.at[owner, w], send.at[owner, w], n_recv.at[owner, w],
            device_id={"row": to}, device_id_type=MESH)

    def flag(owner, send, to):
        return pltpu.make_async_remote_copy(
            nf_buf.at[owner], nf_buf.at[owner], send.at[owner], nf_recv.at[owner],
            device_id={"row": to}, device_id_type=MESH)

    def z_copy(owner, w, to):
        return pltpu.make_async_remote_copy(
            z_buf.at[owner, w], z_buf.at[owner, w], z_send.at[owner, to, w], z_recv.at[owner, w],
            device_id={"col": to}, device_id_type=MESH)

    def zf_copy(owner, to):
        return pltpu.make_async_remote_copy(
            zf_buf.at[owner], zf_buf.at[owner], zf_send.at[to], zf_recv.at[owner],
            device_id={"col": to}, device_id_type=MESH)

    def own_copy(hop, w):
        side, far = int(hop < 0), abs(hop) - 1
        return pltpu.make_async_remote_copy(
            n_buf.at[row, w], n_buf.at[row, w], own_send.at[side, far, w], n_recv.at[row, w],
            device_id={"row": row + hop}, device_id_type=MESH)

    def own_flag(hop):
        side, far = int(hop < 0), abs(hop) - 1
        return pltpu.make_async_remote_copy(
            nf_buf.at[row], nf_buf.at[row], own_f_send.at[side, far], nf_recv.at[row],
            device_id={"row": row + hop}, device_id_type=MESH)

    def send_own(hop):
        @pl.when(there(hop))
        def _():
            if hop > 0:
                pl.semaphore_wait(row_ready.at[hop], 1)
            own_flag(hop).start()

        @pl.when(there(hop) & sends(hop))
        def _():
            for w in range(W):
                own_copy(hop, w).start()

    relayed = C % 2 == 0
    partner = col + 1 - 2 * lax.rem(col, 2)

    loads[2].wait()
    loads[0].wait()
    far0 = jnp.minimum(row, reach)
    second = (row < 0)

    odd = lax.rem(col, 2) == 1
    relay_left = odd
    relay_right = (row >= 0)

    far = jnp.where(relay_left & (far0 == 2), 1, far0)

    def sends(hop):
        if hop == -2:
            return jnp.logical_not(relay_left)
        if hop == 2:
            return jnp.logical_not(relay_right)
        return row >= 0

    def left(hop):
        for w in range(W):
            own_copy(-hop, w).start()

    for hop in range(1, reach + 1):
        @pl.when(there(-hop))
        def _():
            own_flag(-hop).start()

        @pl.when((far == hop) & jnp.logical_not(second) & sends(-hop))
        def _():
            left(hop)

    @pl.when(second)
    def _():
        left(1)

    def own_done(hop):
        for w in range(W):
            own_copy(-hop, w).wait_send()

    def rest():
        @pl.when(second)
        def _():
            pl.semaphore_wait(turn_sem, 1)
            for hop in range(reach, 1, -1):
                @pl.when(sends(-hop))
                def _():
                    left(hop)

        @pl.when(jnp.logical_not(second))
        def _():
            if False:
                @pl.when((far > 1) & (row < R - 1))
                def _():
                    pl.semaphore_wait(go_sem, 1)
            for hop in range(reach - 1, 0, -1):
                @pl.when((far > hop) & sends(-hop))
                def _():
                    left(hop)

    def turns():
        last = row == R - 1
        if True:
            @pl.when(row < 0)
            def _():
                own_done(reach)
                pl.semaphore_signal(turn_sem, inc=1, device_id={"col": partner}, device_id_type=MESH)
        if False:
            @pl.when(last)
            def _():
                if True:
                    @pl.when(lax.rem(col, 2) == 1)
                    def _():
                        own_done(reach)
                else:
                    own_done(reach)
                pl.semaphore_signal(go_sem, inc=1, device_id={"row": row - 1}, device_id_type=MESH)

    loads[3].wait()
    loads[1].wait()
    def each_col(fn):
        for step in range(1, C):
            to = lax.rem(col + step, C)
            fn(step, to)

    def wanted(to):
        return ((lax.rem(to, 2) == 1) | (to == partner)) if relayed else (col >= 0)

    def send_z(step, to):
        @pl.when(wanted(to))
        def _():
            @pl.when(to > col)
            def _():
                pl.semaphore_wait(col_ready.at[step], 1)

            for w in range(W):
                z_copy(col, w, to).start()

    def send_zf(step, to):
        @pl.when((to > col) & jnp.logical_not(wanted(to)))
        def _():
            pl.semaphore_wait(col_ready.at[step], 1)

        zf_copy(col, to).start()

    def z_all():
        each_col(send_z)
        each_col(send_zf)

    def n_right():
        for hop in range(1, reach + 1):
            send_own(hop)
    turns()
    z_all()
    rest()
    n_right()
    from_left = relay_right & has_left & has_right
    from_right = relay_left & has_left & has_right

    @pl.when(from_right)
    def _():
        for w in range(W):
            spectrum(row + 1, w, left_send, row - 1).wait_recv()
            spectrum(row + 1, w, left_send, row - 1).start()

    @pl.when(from_left)
    def _():
        for w in range(W):
            spectrum(row - 1, w, right_send, row + 1).wait_recv()
            spectrum(row - 1, w, right_send, row + 1).start()

    if relayed:
        @pl.when(odd)
        def _():
            for step in range(1, C):
                owner = lax.rem(col + step, C)

                @pl.when(owner != partner)
                def _():
                    for w in range(W):
                        z_copy(owner, w, partner).wait_recv()
                        z_copy(owner, w, partner).start()

    for load in loads[4:]:
        load.wait()

    spot = lax.broadcasted_iota(jnp.int32, (bin_rows, LANES), 0) + lax.broadcasted_iota(
        jnp.int32, (bin_rows, LANES), 1)
    weight = jnp.where(spot == 0, 1.0, 2.0).astype(jnp.float32)

    split = LANES // period
    lines = blocks // split
    groups = C // split
    lane_side = lax.broadcasted_iota(jnp.int32, (blocks, LANES), 1) // period
    line_side = lax.broadcasted_iota(jnp.int32, (blocks, LANES), 0) // lines

    def spread_out(rows):
        picked = jnp.zeros((blocks, LANES), jnp.float32) + rows[0]
        for h in range(1, split):
            picked = jnp.where(line_side == h, rows[h], picked)
        return picked

    def gains(owner):
        n_flag = nf_buf[owner].astype(jnp.float32)
        mask = mask_buf[...].astype(jnp.float32)
        here = lax.broadcasted_iota(jnp.int32, mask.shape, 1) == owner
        kept = jnp.sum(jnp.where(here, mask, 0.0), axis=1, keepdims=True)
        each = []
        for i in range(C):
            marks = zf_buf[i].astype(jnp.float32) * n_flag
            count = jnp.maximum(jnp.sum(marks, axis=1, keepdims=True), 1.0)
            each.append(marks * kept[i:i + 1] / count)
        return [[spread_out([each[g * split + h][:, w:w + 1] for h in range(split)]) for g in range(groups)]
                for w in range(W)]

    def correlate(owner):
        cross = []
        for w in range(W):
            n_real = n_buf[owner, w, pl.ds(0, bin_rows, stride=2), :] * weight
            n_imag = n_buf[owner, w, pl.ds(1, bin_rows, stride=2), :] * weight
            for i in range(C):
                z_real = z_buf[i, w, pl.ds(0, bin_rows, stride=2), :]
                z_imag = z_buf[i, w, pl.ds(1, bin_rows, stride=2), :]
                cross.append(jnp.concatenate(
                    [z_real * n_real + z_imag * n_imag, z_imag * n_real - z_real * n_imag], 0
                ).astype(jnp.bfloat16))
        short = jnp.dot(inner[...], jnp.concatenate(cross, 1), preferred_element_type=jnp.float32)
        turned = []
        for at in range(W * C):
            real = short[:period, at * LANES:(at + 1) * LANES]
            imag = short[period:, at * LANES:(at + 1) * LANES]
            turned.append(jnp.concatenate(
                [real * turn[0] - imag * turn[1], real * turn[1] + imag * turn[0]], 1).astype(jnp.bfloat16))
        lags = lax.dot_general(outer[...], jnp.concatenate(turned, 0), (((1,), (1,)), ((), ())),
                               preferred_element_type=jnp.float32)
        lags = lags[:blocks] + lags[blocks:]
        return [[lags[:, (w * groups + g) * LANES:(w * groups + g + 1) * LANES] for g in range(groups)]
                for w in range(W)]

    def normal(corr, gain):
        power = jnp.sum(corr * corr, axis=0, keepdims=True)
        whole = spread_out([jnp.sum(jnp.where(lane_side[:1] == h, power, 0.0), axis=1, keepdims=True)
                            for h in range(split)])
        laid = corr
        for by in range(1, split):
            moved = pltpu.roll(pltpu.roll(corr, by * period, 1), (split - by) * lines, 0)
            laid = jnp.where(lax.rem(lane_side - line_side + split, split) == by, moved, laid)
        return laid * (gain * lax.rsqrt(whole / LAGS + 1e-05))

    def finish(owner, corrs, gain):
        for g in range(groups):
            total = normal(corrs[0][g], gain[0][g])
            for w in range(1, W):
                total = total + normal(corrs[w][g], gain[w][g])
            for h in range(split):
                i = g * split + h
                out_ref[pl.ds(i * lines * R + owner, lines, stride=R), :] = total[h * lines:(h + 1) * lines]

    def unit(owner, gain):
        finish(owner, correlate(owner), gain)

    def arrive(owner, w, forward, send, f_send, to):
        if w == 0:
            flag(owner, f_send, to).wait_recv()
        spectrum(owner, w, send, to).wait_recv()
        if forward is False:
            return

        @pl.when(forward)
        def _():
            if w == 0:
                flag(owner, f_send, to).start()
            spectrum(owner, w, send, to).start()

    for step in range(1, C):
        owner = lax.rem(col + step, C)
        zf_copy(owner, col).wait_recv()

        @pl.when(jnp.logical_not(odd) | (owner == partner) if relayed else col >= 0)
        def _():
            for w in range(W):
                z_copy(owner, w, col).wait_recv()

    def source(p):
        return jnp.where(p <= row, row - p, p)

    def receive(p):
        left = p <= row
        owner = source(p)
        if reach == R - 1:
            got = (from_left & (owner == row - 1)) | (from_right & (owner == row + 1))

            @pl.when(jnp.logical_not(got))
            def _():
                for w in range(W):
                    spectrum(owner, w, right_send, lax.rem(row + 1, R)).wait_recv()
        else:
            @pl.when(left)
            def _():
                for w in range(W):
                    arrive(owner, w, has_right & (p >= reach), right_send, rf_send, lax.rem(row + 1, R))

            @pl.when(p > row)
            def _():
                for w in range(W):
                    arrive(owner, w, has_left & (p - row >= reach), left_send, lf_send,
                           lax.rem(row + R - 1, R))

    def batch(ps):
        owners = [row if p == 0 else source(p) for p in ps]
        gain = [gains(owner) for owner in owners]
        for p in ps:
            if p > 0:
                receive(p)
        corrs = [correlate(owner) for owner in owners]
        for owner, corr, g in zip(owners, corrs, gain):
            finish(owner, corr, g)

    if R <= 4:
        for p in range(1, R):
            flag(source(p), rf_send, lax.rem(row + 1, R)).wait_recv()
        for ps in [[0, 1], [2, 3]]:
            batch([p for p in ps if p < R])
    else:
        unit(row, gains(row))

        @pl.loop(1, R)
        def _(p):
            receive(p)
            unit(source(p), gains(source(p)))


    for hop in hops:
        for side in (hop, -hop):
            @pl.when(there(side))
            def _():
                own_flag(side).wait_send()

            done = (row < 0) if side > 0 else (row < 0)
            @pl.when(there(side) & jnp.logical_not(done) & sends(side))
            def _():
                for w in range(W):
                    own_copy(side, w).wait_send()

    for step in range(1, C):
        to = lax.rem(col + step, C)
        zf_copy(col, to).wait_send()
        @pl.when(wanted(to))
        def _():
            for w in range(W):
                z_copy(col, w, to).wait_send()

        if relayed:
            @pl.when(odd & (to != partner))
            def _():
                for w in range(W):
                    z_copy(to, w, partner).wait_send()

    @pl.when(from_right)
    def _():
        for w in range(W):
            spectrum(row + 1, w, left_send, row - 1).wait_send()

    @pl.when(from_left)
    def _():
        for w in range(W):
            spectrum(row - 1, w, right_send, row + 1).wait_send()

    if reach == R - 1:
        return

    @pl.loop(0, R)
    def _(owner):
        @pl.when(has_right & (owner <= row - reach))
        def _():
            flag(owner, rf_send, lax.rem(row + 1, R)).wait_send()
            for w in range(W):
                spectrum(owner, w, right_send, lax.rem(row + 1, R)).wait_send()

        @pl.when(has_left & (owner >= row + reach))
        def _():
            flag(owner, lf_send, lax.rem(row + R - 1, R)).wait_send()
            for w in range(W):
                spectrum(owner, w, left_send, lax.rem(row + R - 1, R)).wait_send()


def body(R, C, z_spectra, n_spectra, z_flags, n_flags, pair_mask):
    windows, bins = z_spectra.shape[1], z_spectra.shape[3]
    rows, blocks = bins // LANES, LAGS // LANES
    inner, turn, outer = tables(bins)

    def interleave(x):
        return x.reshape(1, windows, 2, rows, LANES).transpose(0, 1, 3, 2, 4).reshape(
            1, windows, 2 * rows, LANES)

    reach = min(REACH, R - 1)
    DMA = pltpu.SemaphoreType.DMA
    out = pl.pallas_call(
        functools.partial(kernel, R, C, reach),
        out_shape=pltpu.VMEM((C * blocks * R, LANES), jnp.float32),
        in_specs=[pl.BlockSpec(memory_space=pl.ANY)] * 8,
        out_specs=pl.BlockSpec(memory_space=pltpu.VMEM),
        scratch_shapes=[
            pltpu.VMEM((C, windows, 2 * rows, LANES), jnp.float32),
            pltpu.VMEM((R, windows, 2 * rows, LANES), jnp.float32),
            pltpu.VMEM((C, 1, windows), jnp.int32),
            pltpu.VMEM((R, 1, windows), jnp.int32),
            pltpu.VMEM(pair_mask.shape, jnp.int32),
            pltpu.VMEM(inner.shape, jnp.bfloat16),
            pltpu.VMEM(turn.shape, jnp.float32),
            pltpu.VMEM(outer.shape, jnp.bfloat16),
            DMA((8,)),
            DMA((C, C, windows)), DMA((C, windows)), DMA((C,)), DMA((C,)),
            DMA((R, windows)), DMA((R, windows)), DMA((R, windows)),
            DMA((R,)), DMA((R,)), DMA((R,)),
            DMA((2, reach, windows)), DMA((2, reach)),
            pltpu.SemaphoreType.REGULAR((reach + 1,)), pltpu.SemaphoreType.REGULAR((C,)),
            pltpu.SemaphoreType.REGULAR, pltpu.SemaphoreType.REGULAR,
        ],
        compiler_params=pltpu.CompilerParams(collective_id=0, has_side_effects=True),
        name="correlate",
    )(interleave(z_spectra), interleave(n_spectra), z_flags, n_flags, pair_mask,
      jnp.asarray(inner), jnp.asarray(turn), jnp.asarray(outer))
    return out.reshape(C, blocks, R, LANES).transpose(0, 2, 1, 3).reshape(C, R, LAGS)


def solution(mesh):
    placed = (
        P(("grp", "row", "col"), None, None, None),
        P(("grp", "col", "row"), None, None, None),
        P(("grp", "row", "col"), None),
        P(("grp", "col", "row"), None),
        P(("grp", "row"), "col"),
    )
    return jax.shard_map(
        functools.partial(body, mesh.shape["row"], mesh.shape["col"]), mesh=mesh,
        in_specs=placed, out_specs=P(("grp", "row"), "col", None), check_vma=False,
    )
```

```python
import functools
import math

import jax
import jax.numpy as jnp
import numpy as np
from jax import lax
from jax.experimental import pallas as pl
from jax.experimental.pallas import tpu as pltpu
from jax.sharding import PartitionSpec as P

LAGS = 512
LANES = 128
MESH = pl.DeviceIdType.MESH
REACH = 3


def tables(bins):
    rows = bins // LANES
    period = 2 * rows
    blocks, split = LAGS // period, LANES // period
    kt, short, lane = np.arange(rows), np.arange(period), np.arange(LANES)
    phi = 2 * np.pi * ((short[:, None] * kt[None, :]) % period) / period
    inner = np.block([[np.cos(phi), -np.sin(phi)], [np.sin(phi), np.cos(phi)]])
    psi = np.pi * (short[:, None] * lane[None, :]) / bins
    hop = np.arange(blocks).reshape(-1, split).T.reshape(-1) - blocks // 2
    chi = np.pi * ((period * hop[:, None] * lane[None, :]) % (2 * bins)) / bins
    outer = np.stack([np.cos(chi), -np.sin(chi)]).astype(np.float32)
    high = outer.astype(jnp.bfloat16).astype(np.float32)
    low = (outer - high).astype(jnp.bfloat16).astype(np.float32)
    wide = np.pad(inner, ((0, 0), (0, LANES - inner.shape[1])))
    parts = [wide, np.cos(psi), np.sin(psi), high[0], low[0], high[1], low[1]]
    return np.concatenate(parts, 0).astype(np.float32)


def kernel(R, C, z_hbm, n_hbm, zf_hbm, nf_hbm, mask_hbm, table_hbm, out_ref,
           z_buf, n_buf, zf_buf, nf_buf, mask_buf, table,
           load_sem, n_recv, z_recv, flag_recv, sent, row_ready, col_ready):
    row, col = lax.axis_index("row"), lax.axis_index("col")
    W = z_buf.shape[1]
    bin_rows = z_buf.shape[2] // 2
    period = 2 * bin_rows
    blocks = LAGS // period
    odd = lax.rem(col, 2) == 1
    partner = col + 1 - 2 * lax.rem(col, 2)

    n_load = pltpu.make_async_copy(n_hbm.at[0], n_buf.at[row], n_recv.at[row, 0])
    z_load = pltpu.make_async_copy(z_hbm.at[0], z_buf.at[col], z_recv.at[col])
    nf_load = pltpu.make_async_copy(nf_hbm, nf_buf.at[row], load_sem.at[0])
    zf_load = pltpu.make_async_copy(zf_hbm, zf_buf.at[col], load_sem.at[1])
    mask_load = pltpu.make_async_copy(mask_hbm, mask_buf, load_sem.at[2])
    table_load = pltpu.make_async_copy(table_hbm, table, load_sem.at[3])
    for load in (n_load, z_load, nf_load, zf_load, mask_load, table_load):
        load.start()

    def row_there(hop):
        return (row + hop < R) & (row + hop >= 0)

    barrier = pltpu.get_barrier_semaphore()
    for hop in range(1, R):
        @pl.when(row_there(hop))
        def _():
            pl.semaphore_signal(barrier, inc=1, device_id={"row": row + hop}, device_id_type=MESH)

    for step in range(1, C):
        @pl.when(col + step < C)
        def _():
            pl.semaphore_signal(barrier, inc=1, device_id={"col": col + step}, device_id_type=MESH)

    @pl.when(row + col > 0)
    def _():
        pl.semaphore_wait(barrier, row + col)

    for hop in range(1, R):
        @pl.when(row_there(-hop))
        def _():
            pl.semaphore_signal(row_ready.at[hop - 1], inc=1, device_id={"row": row - hop}, device_id_type=MESH)

    for step in range(1, C):
        @pl.when(col >= step)
        def _():
            pl.semaphore_signal(col_ready.at[step - 1], inc=1, device_id={"col": col - step}, device_id_type=MESH)

    def spectrum(owner, w, to):
        return pltpu.make_async_remote_copy(
            n_buf.at[owner, w], n_buf.at[owner, w], sent.at[0], n_recv.at[owner, w],
            device_id={"row": to}, device_id_type=MESH)

    def n_flag(to):
        return pltpu.make_async_remote_copy(
            nf_buf.at[row], nf_buf.at[row], sent.at[1], flag_recv.at[0],
            device_id={"row": to}, device_id_type=MESH)

    def z_copy(owner, to):
        return pltpu.make_async_remote_copy(
            z_buf.at[owner], z_buf.at[owner], sent.at[2], z_recv.at[owner],
            device_id={"col": to}, device_id_type=MESH)

    def z_flag(to):
        return pltpu.make_async_remote_copy(
            zf_buf.at[col], zf_buf.at[col], sent.at[3], flag_recv.at[1],
            device_id={"col": to}, device_id_type=MESH)

    relay_left, relay_right = odd, row >= 0

    def direct(hop):
        if hop == -2:
            return row_there(hop) & jnp.logical_not(relay_left)
        if hop == 2:
            return row_there(hop) & jnp.logical_not(relay_right)
        return row_there(hop)

    def send_n(hop):
        for w in range(W):
            spectrum(row, w, row + hop).start()

    inside = (row > 0) & (row < R - 1)
    from_left, from_right = inside & relay_right, inside & relay_left

    def relay_n(owner, to):
        for w in range(W):
            spectrum(owner, w, to).wait_recv()
            spectrum(owner, w, to).start()

    n_load.wait()
    nf_load.wait()
    for hop in range(1, R):
        @pl.when(row_there(-hop))
        def _():
            n_flag(row - hop).start()

    lead = jnp.where((row == 2) & relay_left, 1, row)
    for hop in range(1, R):
        @pl.when(lead == hop)
        def _():
            send_n(-hop)

    z_load.wait()
    zf_load.wait()

    for step in range(1, C):
        to = lax.rem(col + step, C)
        wide = (lax.rem(to, 2) == 1) | (to == partner)

        @pl.when(wide)
        def _():
            @pl.when(to > col)
            def _():
                pl.semaphore_wait(col_ready.at[step - 1], 1)

            z_copy(col, to).start()

    for step in range(1, C):
        to = lax.rem(col + step, C)
        wide = (lax.rem(to, 2) == 1) | (to == partner)

        @pl.when(jnp.logical_not(wide) & (to > col))
        def _():
            pl.semaphore_wait(col_ready.at[step - 1], 1)

        z_flag(to).start()

    for hop in range(R - 1, 0, -1):
        @pl.when((lead > hop) & direct(-hop))
        def _():
            send_n(-hop)

    for hop in range(1, R):
        @pl.when(row_there(hop))
        def _():
            pl.semaphore_wait(row_ready.at[hop - 1], 1)
            n_flag(row + hop).start()

        @pl.when(direct(hop))
        def _():
            send_n(hop)

    @pl.when(from_right)
    def _():
        relay_n(row + 1, row - 1)

    @pl.when(from_left)
    def _():
        relay_n(row - 1, row + 1)

    @pl.when(odd)
    def _():
        for step in range(1, C):
            owner = lax.rem(col + step, C)

            @pl.when(owner != partner)
            def _():
                z_copy(owner, partner).wait_recv()
                z_copy(owner, partner).start()

    mask_load.wait()
    table_load.wait()
    spot = lax.broadcasted_iota(jnp.int32, (bin_rows, LANES), 0) + lax.broadcasted_iota(
        jnp.int32, (bin_rows, LANES), 1)
    weight = jnp.where(spot == 0, 1.0, 2.0).astype(jnp.float32)
    split = LANES // period
    lines = blocks // split
    groups = C // split
    lane_side = lax.broadcasted_iota(jnp.int32, (blocks, LANES), 1) // period
    line_side = lax.broadcasted_iota(jnp.int32, (blocks, LANES), 0) // lines

    def spread_out(rows):
        picked = jnp.zeros((blocks, LANES), jnp.float32) + rows[0]
        for h in range(1, split):
            picked = jnp.where(line_side == h, rows[h], picked)
        return picked

    def gains(owner):
        passed = nf_buf[owner].astype(jnp.float32)
        mask = mask_buf[...].astype(jnp.float32)
        here = lax.broadcasted_iota(jnp.int32, mask.shape, 1) == owner
        kept = jnp.sum(jnp.where(here, mask, 0.0), axis=1, keepdims=True)
        each = []
        for i in range(C):
            marks = zf_buf[i].astype(jnp.float32) * passed
            count = jnp.maximum(jnp.sum(marks, axis=1, keepdims=True), 1.0)
            each.append(marks * kept[i:i + 1] / count)
        return [[spread_out([each[g * split + h][:, w:w + 1] for h in range(split)]) for g in range(groups)]
                for w in range(W)]

    def correlate(owner):
        inner = table[:2 * period, :period].astype(jnp.bfloat16)
        turn = table[2 * period:3 * period, :], table[3 * period:4 * period, :]
        outer = jnp.concatenate([table[4 * period:4 * period + 2 * blocks, :], table[4 * period + 2 * blocks:, :]], 1)
        outer = outer.astype(jnp.bfloat16)
        cross = []
        for w in range(W):
            n_real = n_buf[owner, w, pl.ds(0, bin_rows, stride=2), :] * weight
            n_imag = n_buf[owner, w, pl.ds(1, bin_rows, stride=2), :] * weight
            for i in range(C):
                z_real = z_buf[i, w, pl.ds(0, bin_rows, stride=2), :]
                z_imag = z_buf[i, w, pl.ds(1, bin_rows, stride=2), :]
                cross.append(jnp.concatenate(
                    [z_real * n_real + z_imag * n_imag, z_imag * n_real - z_real * n_imag], 0
                ).astype(jnp.bfloat16))
        short = jnp.dot(inner, jnp.concatenate(cross, 1), preferred_element_type=jnp.float32)
        turned = []
        for at in range(W * C):
            real = short[:period, at * LANES:(at + 1) * LANES]
            imag = short[period:, at * LANES:(at + 1) * LANES]
            turned.append(jnp.concatenate(
                [real * turn[0] - imag * turn[1], real * turn[1] + imag * turn[0]], 1).astype(jnp.bfloat16))
        lags = lax.dot_general(outer, jnp.concatenate(turned, 0), (((1,), (1,)), ((), ())),
                               preferred_element_type=jnp.float32)
        lags = lags[:blocks] + lags[blocks:]
        return [[lags[:, (w * groups + g) * LANES:(w * groups + g + 1) * LANES] for g in range(groups)]
                for w in range(W)]

    def normal(corr, gain):
        power = jnp.sum(corr * corr, axis=0, keepdims=True)
        whole = spread_out([jnp.sum(jnp.where(lane_side[:1] == h, power, 0.0), axis=1, keepdims=True)
                            for h in range(split)])
        laid = corr
        for by in range(1, split):
            moved = pltpu.roll(pltpu.roll(corr, by * period, 1), (split - by) * lines, 0)
            laid = jnp.where(lax.rem(lane_side - line_side + split, split) == by, moved, laid)
        return laid * (gain * lax.rsqrt(whole / LAGS + 1e-05))

    def finish(owner, corrs, gain):
        for g in range(groups):
            total = normal(corrs[0][g], gain[0][g])
            for w in range(1, W):
                total = total + normal(corrs[w][g], gain[w][g])
            for h in range(split):
                i = g * split + h
                out_ref[pl.ds(i * lines * R + owner, lines, stride=R), :] = total[h * lines:(h + 1) * lines]

    def pick(p):
        ranks = sorted(range(1, R), key=lambda far: (far == 2, far))
        owner = row * 0
        for at in range(R):
            owners = [at + side * far for far in ranks for side in (-1, 1) if 0 <= at + side * far < R]
            owner = jnp.where(row == at, owners[p - 1], owner)
        return owner

    def receive(owner):
        got = (from_left & (owner == row - 1)) | (from_right & (owner == row + 1))

        @pl.when(jnp.logical_not(got))
        def _():
            for w in range(W):
                spectrum(owner, w, row).wait_recv()

    for step in range(1, C):
        owner = lax.rem(col + step, C)

        @pl.when(jnp.logical_not(odd) | (owner == partner))
        def _():
            z_copy(owner, col).wait_recv()

    flags = zf_buf.at[pl.ds(0, C - 1)]
    pltpu.make_async_copy(flags, flags, flag_recv.at[1]).wait()
    flags = nf_buf.at[pl.ds(0, R - 1)]
    pltpu.make_async_copy(flags, flags, flag_recv.at[0]).wait()
    owners = [row] + [pick(p) for p in range(1, R)]
    gain = None
    for batch in ((0, 1), (2,), (3,)):
        batch = [p for p in batch if p < R]
        for p in batch:
            if p > 0:
                receive(owners[p])
        if gain is None:
            gain = [gains(owner) for owner in owners]
        corrs = [correlate(owners[p]) for p in batch]
        for p, corr in zip(batch, corrs):
            finish(owners[p], corr, gain[p])

    def drain(ref, count, most, sem):
        for k in range(1, most + 1):
            @pl.when(count == k)
            def _():
                some = ref.at[pl.ds(0, k)]
                pltpu.make_async_copy(some, some, sem).wait()

    def ones(*flags):
        return sum(jnp.where(flag, 1, 0) for flag in flags)

    own = ones(*[direct(side * hop) for hop in range(1, R) for side in (1, -1)])
    drain(n_buf, own + ones(from_left, from_right), R, sent.at[0])
    drain(nf_buf, row * 0 + R - 1, R - 1, sent.at[1])
    drain(z_buf, jnp.where(odd, C // 2 + C - 2, C // 2), C, sent.at[2])
    drain(zf_buf, row * 0 + C - 1, C - 1, sent.at[3])


def body(R, C, z_spectra, n_spectra, z_flags, n_flags, pair_mask):
    windows, bins = z_spectra.shape[1], z_spectra.shape[3]
    rows = bins // LANES
    blocks, split = LAGS // (2 * rows), LANES // (2 * rows)
    if R > 4 or C != 4 or C % split:
        return far_body(R, C, z_spectra, n_spectra, z_flags, n_flags, pair_mask)
    table = jnp.asarray(tables(bins))

    def interleave(x):
        return x.reshape(1, windows, 2, rows, LANES).transpose(0, 1, 3, 2, 4).reshape(
            1, windows, 2 * rows, LANES)

    DMA, REGULAR = pltpu.SemaphoreType.DMA, pltpu.SemaphoreType.REGULAR
    lines = blocks // split
    out = pl.pallas_call(
        functools.partial(kernel, R, C),
        out_shape=pltpu.VMEM((C * lines * R, LANES), jnp.float32),
        in_specs=[pl.BlockSpec(memory_space=pl.ANY)] * 6,
        out_specs=pl.BlockSpec(memory_space=pltpu.VMEM),
        scratch_shapes=[
            pltpu.VMEM((C, windows, 2 * rows, LANES), jnp.float32),
            pltpu.VMEM((R, windows, 2 * rows, LANES), jnp.float32),
            pltpu.VMEM((C, 1, windows), jnp.int32),
            pltpu.VMEM((R, 1, windows), jnp.int32),
            pltpu.VMEM(pair_mask.shape, jnp.int32),
            pltpu.VMEM(table.shape, jnp.float32),
            DMA((4,)), DMA((R, windows)), DMA((C,)), DMA((2,)), DMA((4,)),
            REGULAR((R - 1,)), REGULAR((C - 1,)),
        ],
        compiler_params=pltpu.CompilerParams(collective_id=0, has_side_effects=True),
        name="correlate",
    )(interleave(z_spectra), interleave(n_spectra), z_flags, n_flags, pair_mask, table)
    return out.reshape(C, lines, R, LANES).transpose(0, 2, 1, 3).reshape(C, R, LAGS)


def far_tables(bins):
    rows, blocks = bins // LANES, LAGS // LANES
    period = 2 * rows
    kt, short = np.arange(rows), np.arange(period)
    phi = 2 * np.pi * ((short[:, None] * kt[None, :]) % period) / period
    inner = np.block([[np.cos(phi), -np.sin(phi)], [np.sin(phi), np.cos(phi)]])
    lane, t0 = np.arange(LANES), np.arange(LANES)
    psi = np.pi * (t0[:, None] * lane[None, :]) / bins
    turn = np.stack([np.cos(psi), np.sin(psi)]).astype(np.float32)
    hop = np.arange(blocks) - blocks // 2
    chi = np.pi * ((LANES * hop[:, None] * lane[None, :]) % (2 * bins)) / bins
    outer = np.concatenate([np.cos(chi), -np.sin(chi)], 1).astype(np.float32)
    high = outer.astype(jnp.bfloat16)
    low = (outer - high.astype(np.float32)).astype(jnp.bfloat16)
    return inner.astype(jnp.bfloat16), turn, np.concatenate([high, low], 0)


def far_kernel(R, C, reach, z_hbm, n_hbm, zf_hbm, nf_hbm, mask_hbm, inner_hbm, turn_hbm, outer_hbm, out_ref,
           z_buf, n_buf, zf_buf, nf_buf, mask_buf, inner, turn, outer,
           load_sem, z_send, z_recv, zf_send, zf_recv, right_send, left_send, n_recv,
           rf_send, lf_send, nf_recv, own_send, own_f_send, ready, turn_sem):
    row, col = lax.axis_index("row"), lax.axis_index("col")
    W = z_buf.shape[1]
    bin_rows = z_buf.shape[2] // 2
    period = inner.shape[0] // 2
    blocks = outer.shape[0] // 2

    loads = [
        pltpu.make_async_copy(n_hbm.at[0], n_buf.at[row], load_sem.at[0]),
        pltpu.make_async_copy(z_hbm.at[0], z_buf.at[col], load_sem.at[1]),
        pltpu.make_async_copy(nf_hbm, nf_buf.at[row], load_sem.at[2]),
        pltpu.make_async_copy(zf_hbm, zf_buf.at[col], load_sem.at[3]),
        pltpu.make_async_copy(mask_hbm, mask_buf, load_sem.at[4]),
        pltpu.make_async_copy(inner_hbm, inner, load_sem.at[5]),
        pltpu.make_async_copy(turn_hbm, turn, load_sem.at[6]),
        pltpu.make_async_copy(outer_hbm, outer, load_sem.at[7]),
    ]
    for load in loads:
        load.start()

    has_left, has_right = row > 0, row < R - 1
    barrier = pltpu.get_barrier_semaphore()

    def there(hop):
        return (row + hop < R) if hop > 0 else (row + hop >= 0)

    for hop in (-1, 1):
        @pl.when(there(hop))
        def _():
            pl.semaphore_signal(barrier, inc=1, device_id={"row": row + hop}, device_id_type=MESH)

    for step in range(1, C):
        pl.semaphore_signal(barrier, inc=1, device_id={"col": lax.rem(col + step, C)}, device_id_type=MESH)
    pl.semaphore_wait(barrier, C - 1 + jnp.where(has_left, 1, 0) + jnp.where(has_right, 1, 0))

    def tell(hop):
        far = abs(hop) + 1
        back = -1 if hop > 0 else 1
        if far <= reach:
            @pl.when(there(hop) & there(back))
            def _():
                pl.semaphore_signal(ready.at[int(hop < 0), far], inc=1,
                                    device_id={"row": row + back}, device_id_type=MESH)

    def learn(hop):
        @pl.when(there(hop))
        def _():
            pl.semaphore_wait(ready.at[int(hop < 0), abs(hop)], 1)

    tell(1)
    tell(-1)

    def spectrum(owner, w, send, to):
        return pltpu.make_async_remote_copy(
            n_buf.at[owner, w], n_buf.at[owner, w], send.at[owner, w], n_recv.at[owner, w],
            device_id={"row": to}, device_id_type=MESH)

    def flag(owner, send, to):
        return pltpu.make_async_remote_copy(
            nf_buf.at[owner], nf_buf.at[owner], send.at[owner], nf_recv.at[owner],
            device_id={"row": to}, device_id_type=MESH)

    def z_copy(owner, w, to):
        return pltpu.make_async_remote_copy(
            z_buf.at[owner, w], z_buf.at[owner, w], z_send.at[to, w], z_recv.at[owner, w],
            device_id={"col": to}, device_id_type=MESH)

    def zf_copy(owner, to):
        return pltpu.make_async_remote_copy(
            zf_buf.at[owner], zf_buf.at[owner], zf_send.at[to], zf_recv.at[owner],
            device_id={"col": to}, device_id_type=MESH)

    def own_copy(hop, w):
        side, far = int(hop < 0), abs(hop) - 1
        return pltpu.make_async_remote_copy(
            n_buf.at[row, w], n_buf.at[row, w], own_send.at[side, far, w], n_recv.at[row, w],
            device_id={"row": row + hop}, device_id_type=MESH)

    def own_flag(hop):
        side, far = int(hop < 0), abs(hop) - 1
        return pltpu.make_async_remote_copy(
            nf_buf.at[row], nf_buf.at[row], own_f_send.at[side, far], nf_recv.at[row],
            device_id={"row": row + hop}, device_id_type=MESH)

    pairs = C % 2 == 0
    first = (lax.rem(col, 2) == 0) if pairs else (col >= 0)

    def send_own(hop):
        @pl.when(there(hop))
        def _():
            own_flag(hop).start()
            for w in range(W):
                own_copy(hop, w).start()

    for hop in range(2, reach + 1):
        learn(-hop)
        tell(-hop)
    loads[2].wait()
    loads[0].wait()
    @pl.when(first)
    def _():
        for hop in range(reach, 0, -1):
            send_own(-hop)

    send_own(1)
    loads[3].wait()
    loads[1].wait()
    for step in range(1, C):
        zf_copy(col, lax.rem(col + step, C)).start()
    for w in range(W):
        for step in range(1, C):
            z_copy(col, w, lax.rem(col + step, C)).start()
    @pl.when(first)
    def _():
        for hop in range(1, reach + 1):
            @pl.when((row == hop) | ((row > hop) & (hop == reach)))
            def _():
                for w in range(W):
                    own_copy(-hop, w).wait_send()

        if pairs:
            pl.semaphore_signal(turn_sem, inc=1, device_id={"col": lax.rem(col + 1, C)}, device_id_type=MESH)

    @pl.when(jnp.logical_not(first))
    def _():
        send_own(-1)
        held = row == R - 1

        @pl.when(held)
        def _():
            pl.semaphore_wait(turn_sem, 1)

        for hop in range(reach, 1, -1):
            send_own(-hop)

        @pl.when(jnp.logical_not(held))
        def _():
            pl.semaphore_wait(turn_sem, 1)

    for hop in range(2, reach + 1):
        learn(hop)
        tell(hop)
        send_own(hop)
    for load in loads[4:]:
        load.wait()

    spot = lax.broadcasted_iota(jnp.int32, (bin_rows, LANES), 0) + lax.broadcasted_iota(
        jnp.int32, (bin_rows, LANES), 1)
    weight = jnp.where(spot == 0, 1.0, 2.0).astype(jnp.float32)

    def unit(owner):
        pairs = [(i, w) for i in range(C) for w in range(W)]
        n_real = [n_buf[owner, w, pl.ds(0, bin_rows, stride=2), :] * weight for w in range(W)]
        n_imag = [n_buf[owner, w, pl.ds(1, bin_rows, stride=2), :] * weight for w in range(W)]
        cross = []
        for i, w in pairs:
            z_real = z_buf[i, w, pl.ds(0, bin_rows, stride=2), :]
            z_imag = z_buf[i, w, pl.ds(1, bin_rows, stride=2), :]
            cross.append(jnp.concatenate(
                [z_real * n_real[w] + z_imag * n_imag[w], z_imag * n_real[w] - z_real * n_imag[w]], 0
            ).astype(jnp.bfloat16))
        short = jnp.dot(inner[...], jnp.concatenate(cross, 1), preferred_element_type=jnp.float32)
        turned = []
        for at in range(len(pairs)):
            real = short[:period, at * LANES:(at + 1) * LANES]
            imag = short[period:, at * LANES:(at + 1) * LANES]
            for part in range(LANES // period):
                cosine = turn[0, part * period:(part + 1) * period, :]
                sine = turn[1, part * period:(part + 1) * period, :]
                turned.append(jnp.concatenate(
                    [real * cosine - imag * sine, real * sine + imag * cosine], 1).astype(jnp.bfloat16))
        lags = lax.dot_general(outer[...], jnp.concatenate(turned, 0), (((1,), (1,)), ((), ())),
                               preferred_element_type=jnp.float32)
        lags = lags[:blocks] + lags[blocks:]
        n_flag = nf_buf[owner].astype(jnp.float32)
        mask = mask_buf[...].astype(jnp.float32)
        here = lax.broadcasted_iota(jnp.int32, mask.shape, 1) == owner
        kept = jnp.sum(jnp.where(here, mask, 0.0), axis=1, keepdims=True)
        for i in range(C):
            marks = zf_buf[i].astype(jnp.float32) * n_flag
            count = jnp.maximum(jnp.sum(marks, axis=1, keepdims=True), 1.0)
            gain = marks * kept[i:i + 1] / count
            total = jnp.zeros((blocks, LANES), jnp.float32)
            for w in range(W):
                at = i * W + w
                corr = lags[:, at * LANES:(at + 1) * LANES]
                power = jnp.sum(jnp.sum(corr * corr, axis=0, keepdims=True), axis=1, keepdims=True)
                spread = jnp.sqrt(power / LAGS + 1e-05)
                total = total + corr * (gain[:, w:w + 1] / spread)
            out_ref[pl.ds(i * blocks * R + owner, blocks, stride=R), :] = total

    def arrive(owner, w, forward, send, f_send, to):
        if w == 0:
            flag(owner, f_send, to).wait_recv()
        spectrum(owner, w, send, to).wait_recv()
        if forward is False:
            return

        @pl.when(forward)
        def _():
            if w == 0:
                flag(owner, f_send, to).start()
            spectrum(owner, w, send, to).start()

    for step in range(1, C):
        zf_copy(lax.rem(col + C - step, C), lax.rem(col + step, C)).wait_recv()
    for w in range(W):
        for step in range(1, C):
            z_copy(lax.rem(col + C - step, C), w, lax.rem(col + step, C)).wait_recv()
    unit(row)

    def take(p):
        left = p <= row
        owner = jnp.where(left, row - p, p)
        if reach == R - 1:
            for w in range(W):
                arrive(owner, w, False, right_send, rf_send, lax.rem(row + 1, R))
        else:
            @pl.when(left)
            def _():
                for w in range(W):
                    arrive(owner, w, has_right & (p >= reach), right_send, rf_send, lax.rem(row + 1, R))

            @pl.when(p > row)
            def _():
                for w in range(W):
                    arrive(owner, w, has_left & (p - row >= reach), left_send, lf_send,
                           lax.rem(row + R - 1, R))
        unit(owner)

    if R <= 4:
        for p in range(1, R):
            take(p)
    else:
        pl.loop(1, R)(take)

    hops = [sign * hop for hop in range(1, reach + 1) for sign in (1, -1)]
    for hop in hops:
        @pl.when(there(hop))
        def _():
            own_flag(hop).wait_send()
            if hop > 0:
                for w in range(W):
                    own_copy(hop, w).wait_send()
            else:
                waited = first & ((row == -hop) | ((row > -hop) & (-hop == reach)))

                @pl.when(jnp.logical_not(waited))
                def _():
                    for w in range(W):
                        own_copy(hop, w).wait_send()

    for step in range(1, C):
        zf_copy(col, lax.rem(col + step, C)).wait_send()
        for w in range(W):
            z_copy(col, w, lax.rem(col + step, C)).wait_send()

    if reach == R - 1:
        return

    @pl.loop(0, R)
    def _(owner):
        @pl.when(has_right & (owner <= row - reach))
        def _():
            flag(owner, rf_send, lax.rem(row + 1, R)).wait_send()
            for w in range(W):
                spectrum(owner, w, right_send, lax.rem(row + 1, R)).wait_send()

        @pl.when(has_left & (owner >= row + reach))
        def _():
            flag(owner, lf_send, lax.rem(row + R - 1, R)).wait_send()
            for w in range(W):
                spectrum(owner, w, left_send, lax.rem(row + R - 1, R)).wait_send()


def far_body(R, C, z_spectra, n_spectra, z_flags, n_flags, pair_mask):
    windows, bins = z_spectra.shape[1], z_spectra.shape[3]
    rows, blocks = bins // LANES, LAGS // LANES
    inner, turn, outer = far_tables(bins)

    def interleave(x):
        return x.reshape(1, windows, 2, rows, LANES).transpose(0, 1, 3, 2, 4).reshape(
            1, windows, 2 * rows, LANES)

    reach = min(REACH, R - 1)
    DMA = pltpu.SemaphoreType.DMA
    out = pl.pallas_call(
        functools.partial(far_kernel, R, C, reach),
        out_shape=pltpu.VMEM((C * blocks * R, LANES), jnp.float32),
        in_specs=[pl.BlockSpec(memory_space=pl.ANY)] * 8,
        out_specs=pl.BlockSpec(memory_space=pltpu.VMEM),
        scratch_shapes=[
            pltpu.VMEM((C, windows, 2 * rows, LANES), jnp.float32),
            pltpu.VMEM((R, windows, 2 * rows, LANES), jnp.float32),
            pltpu.VMEM((C, 1, windows), jnp.int32),
            pltpu.VMEM((R, 1, windows), jnp.int32),
            pltpu.VMEM(pair_mask.shape, jnp.int32),
            pltpu.VMEM(inner.shape, jnp.bfloat16),
            pltpu.VMEM(turn.shape, jnp.float32),
            pltpu.VMEM(outer.shape, jnp.bfloat16),
            DMA((8,)),
            DMA((C, windows)), DMA((C, windows)), DMA((C,)), DMA((C,)),
            DMA((R, windows)), DMA((R, windows)), DMA((R, windows)),
            DMA((R,)), DMA((R,)), DMA((R,)),
            DMA((2, reach, windows)), DMA((2, reach)), pltpu.SemaphoreType.REGULAR((2, reach + 1)),
            pltpu.SemaphoreType.REGULAR,
        ],
        compiler_params=pltpu.CompilerParams(collective_id=0, has_side_effects=True),
        name="correlate",
    )(interleave(z_spectra), interleave(n_spectra), z_flags, n_flags, pair_mask,
      jnp.asarray(inner), jnp.asarray(turn), jnp.asarray(outer))
    return out.reshape(C, blocks, R, LANES).transpose(0, 2, 1, 3).reshape(C, R, LAGS)


def solution(mesh):
    placed = (
        P(("grp", "row", "col"), None, None, None),
        P(("grp", "col", "row"), None, None, None),
        P(("grp", "row", "col"), None),
        P(("grp", "col", "row"), None),
        P(("grp", "row"), "col"),
    )
    return jax.shard_map(
        functools.partial(body, mesh.shape["row"], mesh.shape["col"]), mesh=mesh,
        in_specs=placed, out_specs=P(("grp", "row"), "col", None), check_vma=False,
    )
```

```python
import functools
import math

import jax
import jax.numpy as jnp
import numpy as np
from jax import lax
from jax.experimental import pallas as pl
from jax.experimental.pallas import tpu as pltpu
from jax.sharding import PartitionSpec as P

LAGS = 512
LANES = 128
MESH = pl.DeviceIdType.MESH
REACH = 3
SENDS = (
    ((0, 1, 3), (0, 3, 5)),
    ((0, 1, 3), (0, 3, 5)),
    ((1, 0, 0), (1, 2, 3), (0, 2, 6)),
    ((1, 0, 0), (1, 2, 3), (2, 0, 6), (0, 2, 6)),
    ((2, 0, 0), (2, 1, 2), (2, 3, 3), (1, 3, 6)),
    ((2, 1, 0), (2, 3, 3), (3, 1, 6), (1, 3, 6)),
    ((3, 0, 0), (3, 1, 2), (3, 2, 2)),
    ((3, 0, 0), (3, 2, 2)),
)
TAKES = ((1, 2, 3), (1, 2, 3), (0, 2, 3), (0, 2, 3), (1, 3, 0), (1, 3, 0), (2, 0, 1), (2, 0, 1))
BATCHES = ((0, 1), (2, 3))
GAIN_AT = 1


def tables(bins):
    rows = bins // LANES
    period = 2 * rows
    blocks, split = LAGS // period, LANES // period
    kt, short, lane = np.arange(rows), np.arange(period), np.arange(LANES)
    phi = 2 * np.pi * ((short[:, None] * kt[None, :]) % period) / period
    inner = np.block([[np.cos(phi), -np.sin(phi)], [np.sin(phi), np.cos(phi)]])
    psi = np.pi * (short[:, None] * lane[None, :]) / bins
    hop = np.arange(blocks).reshape(-1, split).T.reshape(-1) - blocks // 2
    chi = np.pi * ((period * hop[:, None] * lane[None, :]) % (2 * bins)) / bins
    outer = np.stack([np.cos(chi), -np.sin(chi)]).astype(np.float32)
    high = outer.astype(jnp.bfloat16).astype(np.float32)
    low = (outer - high).astype(jnp.bfloat16).astype(np.float32)
    wide = np.pad(inner, ((0, 0), (0, LANES - inner.shape[1])))
    parts = [wide, np.cos(psi), np.sin(psi), high[0], low[0], high[1], low[1]]
    return np.concatenate(parts, 0).astype(np.float32)


def kernel(R, C, z_hbm, n_hbm, zf_hbm, nf_hbm, mask_hbm, table_hbm, out_ref,
           held, flags, mask_buf, table, n_recv, z_recv, flag_recv, sent, row_ready, col_ready):
    row, col = lax.axis_index("row"), lax.axis_index("col")
    W = held.shape[1]
    bin_rows = held.shape[2] // 2
    period = 2 * bin_rows
    blocks = LAGS // period
    odd = lax.rem(col, 2) == 1
    partner = col + 1 - 2 * lax.rem(col, 2)
    place = 2 * row + lax.rem(col, 2)

    def wait_all(ref, count, sem):
        some = ref.at[pl.ds(0, count)]
        pltpu.make_async_copy(some, some, sem).wait()

    n_load = pltpu.make_async_copy(n_hbm.at[0], held.at[row], n_recv.at[row, 0])
    z_load = pltpu.make_async_copy(z_hbm.at[0], held.at[R + col], z_recv.at[col])
    n_load.start()
    pltpu.make_async_copy(nf_hbm, flags.at[row], sent.at[1]).start()
    pltpu.make_async_copy(zf_hbm, flags.at[R + col], sent.at[1]).start()
    z_load.start()

    def row_there(hop):
        return (row + hop < R) & (row + hop >= 0)

    barrier = pltpu.get_barrier_semaphore()
    for hop in range(1, R):
        @pl.when(row_there(hop))
        def _():
            pl.semaphore_signal(barrier, inc=1, device_id={"row": row + hop}, device_id_type=MESH)

    for step in range(1, C):
        @pl.when(col + step < C)
        def _():
            pl.semaphore_signal(barrier, inc=1, device_id={"col": col + step}, device_id_type=MESH)

    @pl.when(row + col > 0)
    def _():
        pl.semaphore_wait(barrier, row + col)

    for hop in range(1, R):
        @pl.when(row_there(-hop))
        def _():
            pl.semaphore_signal(row_ready.at[hop - 1], inc=1, device_id={"row": row - hop}, device_id_type=MESH)

    for step in range(1, C):
        @pl.when(col >= step)
        def _():
            pl.semaphore_signal(col_ready, inc=1, device_id={"col": col - step}, device_id_type=MESH)

    def spectrum(owner, w, to):
        return pltpu.make_async_remote_copy(
            held.at[owner, w], held.at[owner, w], sent.at[0], n_recv.at[owner, w],
            device_id={"row": to}, device_id_type=MESH)

    def z_copy(owner, to):
        return pltpu.make_async_remote_copy(
            held.at[R + owner], held.at[R + owner], sent.at[0], z_recv.at[owner],
            device_id={"col": to}, device_id_type=MESH)

    def flag(slot, **to):
        return pltpu.make_async_remote_copy(
            flags.at[slot], flags.at[slot], sent.at[1], flag_recv, device_id=to, device_id_type=MESH)

    def at(fn):
        for here in range(2 * R):
            @pl.when(place == here)
            def _():
                fn(here)

    def step_sends(number):
        def send(here):
            for owner, to, when in SENDS[here]:
                if when == number:
                    for w in range(W):
                        if owner != here // 2:
                            spectrum(owner, w, to).wait_recv()
                        spectrum(owner, w, to).start()
        if any(when == number for sends in SENDS for _, _, when in sends):
            at(send)

    wait_all(flags, 2, sent.at[1])
    for hop in range(1, R):
        @pl.when(row_there(-hop))
        def _():
            flag(row, row=row - hop).start()

    n_load.wait()
    mask_load = pltpu.make_async_copy(mask_hbm, mask_buf, n_recv.at[row, 0])
    mask_load.start()
    step_sends(0)

    def send_z(step, ahead):
        to = lax.rem(col + step, C)

        @pl.when((to > col) == ahead)
        def _():
            @pl.when(jnp.logical_not(odd) | (lax.rem(to, 2) == 1) | (to == partner))
            def _():
                z_copy(col, to).start()

            flag(R + col, col=to).start()

    z_load.wait()
    table_load = pltpu.make_async_copy(table_hbm, table, z_recv.at[col])
    table_load.start()
    for step in range(1, C):
        send_z(step, False)
    step_sends(1)

    @pl.when(col < C - 1)
    def _():
        pl.semaphore_wait(col_ready, C - 1 - col)

    for step in range(1, C):
        send_z(step, True)
    step_sends(2)
    for hop in range(1, R):
        @pl.when(row_there(hop))
        def _():
            pl.semaphore_wait(row_ready.at[hop - 1], 1)
            flag(row, row=row + hop).start()

        step_sends(2 + hop)

    step_sends(R + 2)

    @pl.when(odd)
    def _():
        for step in range(2, C, 2):
            owner = lax.rem(col + step, C)
            z_copy(owner, partner).wait_recv()
            z_copy(owner, partner).start()

    step_sends(R + 3)
    mask_load.wait()
    table_load.wait()
    spot = lax.broadcasted_iota(jnp.int32, (bin_rows, LANES), 0) + lax.broadcasted_iota(
        jnp.int32, (bin_rows, LANES), 1)
    weight = jnp.where(spot == 0, 1.0, 2.0).astype(jnp.float32)
    split = LANES // period
    lines = blocks // split
    groups = C // split
    lane_side = lax.broadcasted_iota(jnp.int32, (blocks, LANES), 1) // period
    line_side = lax.broadcasted_iota(jnp.int32, (blocks, LANES), 0) // lines

    def spread_out(rows):
        picked = jnp.zeros((blocks, LANES), jnp.float32) + rows[0]
        for h in range(1, split):
            picked = jnp.where(line_side == h, rows[h], picked)
        return picked

    def gains(owner):
        passed = flags[owner].astype(jnp.float32)
        mask = mask_buf[...].astype(jnp.float32)
        here = lax.broadcasted_iota(jnp.int32, mask.shape, 1) == owner
        kept = jnp.sum(jnp.where(here, mask, 0.0), axis=1, keepdims=True)
        each = []
        for i in range(C):
            marks = flags[R + i].astype(jnp.float32) * passed
            count = jnp.maximum(jnp.sum(marks, axis=1, keepdims=True), 1.0)
            each.append(marks * kept[i:i + 1] / count)
        return [[spread_out([each[g * split + h][:, w:w + 1] for h in range(split)]) for g in range(groups)]
                for w in range(W)]

    def correlate(owner):
        inner = table[:2 * period, :period].astype(jnp.bfloat16)
        turn = table[2 * period:3 * period, :], table[3 * period:4 * period, :]
        outer = jnp.concatenate([table[4 * period:4 * period + 2 * blocks, :], table[4 * period + 2 * blocks:, :]], 1)
        outer = outer.astype(jnp.bfloat16)
        cross = []
        for w in range(W):
            n_real = held[owner, w, pl.ds(0, bin_rows, stride=2), :] * weight
            n_imag = held[owner, w, pl.ds(1, bin_rows, stride=2), :] * weight
            for i in range(C):
                z_real = held[R + i, w, pl.ds(0, bin_rows, stride=2), :]
                z_imag = held[R + i, w, pl.ds(1, bin_rows, stride=2), :]
                cross.append(jnp.concatenate(
                    [z_real * n_real + z_imag * n_imag, z_imag * n_real - z_real * n_imag], 0
                ).astype(jnp.bfloat16))
        short = jnp.dot(inner, jnp.concatenate(cross, 1), preferred_element_type=jnp.float32)
        turned = []
        for at in range(W * C):
            real = short[:period, at * LANES:(at + 1) * LANES]
            imag = short[period:, at * LANES:(at + 1) * LANES]
            turned.append(jnp.concatenate(
                [real * turn[0] - imag * turn[1], real * turn[1] + imag * turn[0]], 1).astype(jnp.bfloat16))
        lags = lax.dot_general(outer, jnp.concatenate(turned, 0), (((1,), (1,)), ((), ())),
                               preferred_element_type=jnp.float32)
        lags = lags[:blocks] + lags[blocks:]
        return [[lags[:, (w * groups + g) * LANES:(w * groups + g + 1) * LANES] for g in range(groups)]
                for w in range(W)]

    def normal(corr):
        power = jnp.sum(corr * corr, axis=0, keepdims=True)
        whole = spread_out([jnp.sum(jnp.where(lane_side[:1] == h, power, 0.0), axis=1, keepdims=True)
                            for h in range(split)])
        laid = corr
        for by in range(1, split):
            moved = pltpu.roll(pltpu.roll(corr, by * period, 1), (split - by) * lines, 0)
            laid = jnp.where(lax.rem(lane_side - line_side + split, split) == by, moved, laid)
        return laid * lax.rsqrt(whole / LAGS + 1e-05)

    def finish(owner, units, gain):
        for g in range(groups):
            total = units[0][g] * gain[0][g]
            for w in range(1, W):
                total = total + units[w][g] * gain[w][g]
            for h in range(split):
                i = g * split + h
                out_ref[pl.ds(i * lines * R + owner, lines, stride=R), :] = total[h * lines:(h + 1) * lines]

    def pick(p):
        owner = row * 0
        for here in range(2 * R):
            owner = jnp.where(place == here, TAKES[here][p - 1], owner)
        return owner

    def receive(p):
        def take(here):
            owner = TAKES[here][p - 1]
            if all(passed != owner for passed, _, _ in SENDS[here]):
                for w in range(W):
                    spectrum(owner, w, here // 2).wait_recv()
        at(take)

    for step in range(1, C):
        owner = lax.rem(col + step, C)

        @pl.when(jnp.logical_not(odd & (lax.rem(owner, 2) == 1)))
        def _():
            z_copy(owner, col).wait_recv()

    owners = [row] + [pick(p) for p in range(1, R)]
    done = []
    for number, batch in enumerate(BATCHES):
        if number == GAIN_AT:
            wait_all(flags, R + C - 2, flag_recv)
            gain = [gains(owner) for owner in owners]
        for p in batch:
            if p > 0:
                receive(p)
        corrs = [correlate(owners[p]) for p in batch]
        done += [(p, [[normal(c) for c in part] for part in corr]) for p, corr in zip(batch, corrs)]
    for p, units in done:
        finish(owners[p], units, gain[p])

    def finish_sends(here):
        wait_all(held, len(SENDS[here]) + C - 1, sent.at[0])

    at(finish_sends)
    wait_all(flags, R + C - 2, sent.at[1])


def body(R, C, z_spectra, n_spectra, z_flags, n_flags, pair_mask):
    windows, bins = z_spectra.shape[1], z_spectra.shape[3]
    rows = bins // LANES
    blocks, split = LAGS // (2 * rows), LANES // (2 * rows)
    if 2 * R != len(SENDS) or C % 2 or C % split:
        return far_body(R, C, z_spectra, n_spectra, z_flags, n_flags, pair_mask)
    table = jnp.asarray(tables(bins))

    def interleave(x):
        return x.reshape(1, windows, 2, rows, LANES).transpose(0, 1, 3, 2, 4).reshape(
            1, windows, 2 * rows, LANES)

    DMA, REGULAR = pltpu.SemaphoreType.DMA, pltpu.SemaphoreType.REGULAR
    lines = blocks // split
    out = pl.pallas_call(
        functools.partial(kernel, R, C),
        out_shape=pltpu.VMEM((C * lines * R, LANES), jnp.float32),
        in_specs=[pl.BlockSpec(memory_space=pl.ANY)] * 6,
        out_specs=pl.BlockSpec(memory_space=pltpu.VMEM),
        scratch_shapes=[
            pltpu.VMEM((R + C, windows, 2 * rows, LANES), jnp.float32),
            pltpu.VMEM((R + C, 1, windows), jnp.int32),
            pltpu.VMEM(pair_mask.shape, jnp.int32),
            pltpu.VMEM(table.shape, jnp.float32),
            DMA((R, windows)), DMA((C,)), DMA, DMA((2,)), REGULAR((R - 1,)), REGULAR,
        ],
        compiler_params=pltpu.CompilerParams(collective_id=0, has_side_effects=True),
        name="correlate",
    )(interleave(z_spectra), interleave(n_spectra), z_flags, n_flags, pair_mask, table)
    return out.reshape(C, lines, R, LANES).transpose(0, 2, 1, 3).reshape(C, R, LAGS)


def far_tables(bins):
    rows, blocks = bins // LANES, LAGS // LANES
    period = 2 * rows
    kt, short = np.arange(rows), np.arange(period)
    phi = 2 * np.pi * ((short[:, None] * kt[None, :]) % period) / period
    inner = np.block([[np.cos(phi), -np.sin(phi)], [np.sin(phi), np.cos(phi)]])
    lane, t0 = np.arange(LANES), np.arange(LANES)
    psi = np.pi * (t0[:, None] * lane[None, :]) / bins
    turn = np.stack([np.cos(psi), np.sin(psi)]).astype(np.float32)
    hop = np.arange(blocks) - blocks // 2
    chi = np.pi * ((LANES * hop[:, None] * lane[None, :]) % (2 * bins)) / bins
    outer = np.concatenate([np.cos(chi), -np.sin(chi)], 1).astype(np.float32)
    high = outer.astype(jnp.bfloat16)
    low = (outer - high.astype(np.float32)).astype(jnp.bfloat16)
    return inner.astype(jnp.bfloat16), turn, np.concatenate([high, low], 0)


def far_kernel(R, C, reach, z_hbm, n_hbm, zf_hbm, nf_hbm, mask_hbm, inner_hbm, turn_hbm, outer_hbm, out_ref,
           z_buf, n_buf, zf_buf, nf_buf, mask_buf, inner, turn, outer,
           load_sem, z_send, z_recv, zf_send, zf_recv, right_send, left_send, n_recv,
           rf_send, lf_send, nf_recv, own_send, own_f_send, ready, turn_sem):
    row, col = lax.axis_index("row"), lax.axis_index("col")
    W = z_buf.shape[1]
    bin_rows = z_buf.shape[2] // 2
    period = inner.shape[0] // 2
    blocks = outer.shape[0] // 2

    loads = [
        pltpu.make_async_copy(n_hbm.at[0], n_buf.at[row], load_sem.at[0]),
        pltpu.make_async_copy(z_hbm.at[0], z_buf.at[col], load_sem.at[1]),
        pltpu.make_async_copy(nf_hbm, nf_buf.at[row], load_sem.at[2]),
        pltpu.make_async_copy(zf_hbm, zf_buf.at[col], load_sem.at[3]),
        pltpu.make_async_copy(mask_hbm, mask_buf, load_sem.at[4]),
        pltpu.make_async_copy(inner_hbm, inner, load_sem.at[5]),
        pltpu.make_async_copy(turn_hbm, turn, load_sem.at[6]),
        pltpu.make_async_copy(outer_hbm, outer, load_sem.at[7]),
    ]
    for load in loads:
        load.start()

    has_left, has_right = row > 0, row < R - 1
    barrier = pltpu.get_barrier_semaphore()

    def there(hop):
        return (row + hop < R) if hop > 0 else (row + hop >= 0)

    for hop in (-1, 1):
        @pl.when(there(hop))
        def _():
            pl.semaphore_signal(barrier, inc=1, device_id={"row": row + hop}, device_id_type=MESH)

    for step in range(1, C):
        pl.semaphore_signal(barrier, inc=1, device_id={"col": lax.rem(col + step, C)}, device_id_type=MESH)
    pl.semaphore_wait(barrier, C - 1 + jnp.where(has_left, 1, 0) + jnp.where(has_right, 1, 0))

    def tell(hop):
        far = abs(hop) + 1
        back = -1 if hop > 0 else 1
        if far <= reach:
            @pl.when(there(hop) & there(back))
            def _():
                pl.semaphore_signal(ready.at[int(hop < 0), far], inc=1,
                                    device_id={"row": row + back}, device_id_type=MESH)

    def learn(hop):
        @pl.when(there(hop))
        def _():
            pl.semaphore_wait(ready.at[int(hop < 0), abs(hop)], 1)

    tell(1)
    tell(-1)

    def spectrum(owner, w, send, to):
        return pltpu.make_async_remote_copy(
            n_buf.at[owner, w], n_buf.at[owner, w], send.at[owner, w], n_recv.at[owner, w],
            device_id={"row": to}, device_id_type=MESH)

    def flag(owner, send, to):
        return pltpu.make_async_remote_copy(
            nf_buf.at[owner], nf_buf.at[owner], send.at[owner], nf_recv.at[owner],
            device_id={"row": to}, device_id_type=MESH)

    def z_copy(owner, w, to):
        return pltpu.make_async_remote_copy(
            z_buf.at[owner, w], z_buf.at[owner, w], z_send.at[to, w], z_recv.at[owner, w],
            device_id={"col": to}, device_id_type=MESH)

    def zf_copy(owner, to):
        return pltpu.make_async_remote_copy(
            zf_buf.at[owner], zf_buf.at[owner], zf_send.at[to], zf_recv.at[owner],
            device_id={"col": to}, device_id_type=MESH)

    def own_copy(hop, w):
        side, far = int(hop < 0), abs(hop) - 1
        return pltpu.make_async_remote_copy(
            n_buf.at[row, w], n_buf.at[row, w], own_send.at[side, far, w], n_recv.at[row, w],
            device_id={"row": row + hop}, device_id_type=MESH)

    def own_flag(hop):
        side, far = int(hop < 0), abs(hop) - 1
        return pltpu.make_async_remote_copy(
            nf_buf.at[row], nf_buf.at[row], own_f_send.at[side, far], nf_recv.at[row],
            device_id={"row": row + hop}, device_id_type=MESH)

    pairs = C % 2 == 0
    first = (lax.rem(col, 2) == 0) if pairs else (col >= 0)

    def send_own(hop):
        @pl.when(there(hop))
        def _():
            own_flag(hop).start()
            for w in range(W):
                own_copy(hop, w).start()

    for hop in range(2, reach + 1):
        learn(-hop)
        tell(-hop)
    loads[2].wait()
    loads[0].wait()
    @pl.when(first)
    def _():
        for hop in range(reach, 0, -1):
            send_own(-hop)

    send_own(1)
    loads[3].wait()
    loads[1].wait()
    for step in range(1, C):
        zf_copy(col, lax.rem(col + step, C)).start()
    for w in range(W):
        for step in range(1, C):
            z_copy(col, w, lax.rem(col + step, C)).start()
    @pl.when(first)
    def _():
        for hop in range(1, reach + 1):
            @pl.when((row == hop) | ((row > hop) & (hop == reach)))
            def _():
                for w in range(W):
                    own_copy(-hop, w).wait_send()

        if pairs:
            pl.semaphore_signal(turn_sem, inc=1, device_id={"col": lax.rem(col + 1, C)}, device_id_type=MESH)

    @pl.when(jnp.logical_not(first))
    def _():
        send_own(-1)
        held = row == R - 1

        @pl.when(held)
        def _():
            pl.semaphore_wait(turn_sem, 1)

        for hop in range(reach, 1, -1):
            send_own(-hop)

        @pl.when(jnp.logical_not(held))
        def _():
            pl.semaphore_wait(turn_sem, 1)

    for hop in range(2, reach + 1):
        learn(hop)
        tell(hop)
        send_own(hop)
    for load in loads[4:]:
        load.wait()

    spot = lax.broadcasted_iota(jnp.int32, (bin_rows, LANES), 0) + lax.broadcasted_iota(
        jnp.int32, (bin_rows, LANES), 1)
    weight = jnp.where(spot == 0, 1.0, 2.0).astype(jnp.float32)

    def unit(owner):
        pairs = [(i, w) for i in range(C) for w in range(W)]
        n_real = [n_buf[owner, w, pl.ds(0, bin_rows, stride=2), :] * weight for w in range(W)]
        n_imag = [n_buf[owner, w, pl.ds(1, bin_rows, stride=2), :] * weight for w in range(W)]
        cross = []
        for i, w in pairs:
            z_real = z_buf[i, w, pl.ds(0, bin_rows, stride=2), :]
            z_imag = z_buf[i, w, pl.ds(1, bin_rows, stride=2), :]
            cross.append(jnp.concatenate(
                [z_real * n_real[w] + z_imag * n_imag[w], z_imag * n_real[w] - z_real * n_imag[w]], 0
            ).astype(jnp.bfloat16))
        short = jnp.dot(inner[...], jnp.concatenate(cross, 1), preferred_element_type=jnp.float32)
        turned = []
        for at in range(len(pairs)):
            real = short[:period, at * LANES:(at + 1) * LANES]
            imag = short[period:, at * LANES:(at + 1) * LANES]
            for part in range(LANES // period):
                cosine = turn[0, part * period:(part + 1) * period, :]
                sine = turn[1, part * period:(part + 1) * period, :]
                turned.append(jnp.concatenate(
                    [real * cosine - imag * sine, real * sine + imag * cosine], 1).astype(jnp.bfloat16))
        lags = lax.dot_general(outer[...], jnp.concatenate(turned, 0), (((1,), (1,)), ((), ())),
                               preferred_element_type=jnp.float32)
        lags = lags[:blocks] + lags[blocks:]
        n_flag = nf_buf[owner].astype(jnp.float32)
        mask = mask_buf[...].astype(jnp.float32)
        here = lax.broadcasted_iota(jnp.int32, mask.shape, 1) == owner
        kept = jnp.sum(jnp.where(here, mask, 0.0), axis=1, keepdims=True)
        for i in range(C):
            marks = zf_buf[i].astype(jnp.float32) * n_flag
            count = jnp.maximum(jnp.sum(marks, axis=1, keepdims=True), 1.0)
            gain = marks * kept[i:i + 1] / count
            total = jnp.zeros((blocks, LANES), jnp.float32)
            for w in range(W):
                at = i * W + w
                corr = lags[:, at * LANES:(at + 1) * LANES]
                power = jnp.sum(jnp.sum(corr * corr, axis=0, keepdims=True), axis=1, keepdims=True)
                spread = jnp.sqrt(power / LAGS + 1e-05)
                total = total + corr * (gain[:, w:w + 1] / spread)
            out_ref[pl.ds(i * blocks * R + owner, blocks, stride=R), :] = total

    def arrive(owner, w, forward, send, f_send, to):
        if w == 0:
            flag(owner, f_send, to).wait_recv()
        spectrum(owner, w, send, to).wait_recv()
        if forward is False:
            return

        @pl.when(forward)
        def _():
            if w == 0:
                flag(owner, f_send, to).start()
            spectrum(owner, w, send, to).start()

    for step in range(1, C):
        zf_copy(lax.rem(col + C - step, C), lax.rem(col + step, C)).wait_recv()
    for w in range(W):
        for step in range(1, C):
            z_copy(lax.rem(col + C - step, C), w, lax.rem(col + step, C)).wait_recv()
    unit(row)

    def take(p):
        left = p <= row
        owner = jnp.where(left, row - p, p)
        if reach == R - 1:
            for w in range(W):
                arrive(owner, w, False, right_send, rf_send, lax.rem(row + 1, R))
        else:
            @pl.when(left)
            def _():
                for w in range(W):
                    arrive(owner, w, has_right & (p >= reach), right_send, rf_send, lax.rem(row + 1, R))

            @pl.when(p > row)
            def _():
                for w in range(W):
                    arrive(owner, w, has_left & (p - row >= reach), left_send, lf_send,
                           lax.rem(row + R - 1, R))
        unit(owner)

    if R <= 4:
        for p in range(1, R):
            take(p)
    else:
        pl.loop(1, R)(take)

    hops = [sign * hop for hop in range(1, reach + 1) for sign in (1, -1)]
    for hop in hops:
        @pl.when(there(hop))
        def _():
            own_flag(hop).wait_send()
            if hop > 0:
                for w in range(W):
                    own_copy(hop, w).wait_send()
            else:
                waited = first & ((row == -hop) | ((row > -hop) & (-hop == reach)))

                @pl.when(jnp.logical_not(waited))
                def _():
                    for w in range(W):
                        own_copy(hop, w).wait_send()

    for step in range(1, C):
        zf_copy(col, lax.rem(col + step, C)).wait_send()
        for w in range(W):
            z_copy(col, w, lax.rem(col + step, C)).wait_send()

    if reach == R - 1:
        return

    @pl.loop(0, R)
    def _(owner):
        @pl.when(has_right & (owner <= row - reach))
        def _():
            flag(owner, rf_send, lax.rem(row + 1, R)).wait_send()
            for w in range(W):
                spectrum(owner, w, right_send, lax.rem(row + 1, R)).wait_send()

        @pl.when(has_left & (owner >= row + reach))
        def _():
            flag(owner, lf_send, lax.rem(row + R - 1, R)).wait_send()
            for w in range(W):
                spectrum(owner, w, left_send, lax.rem(row + R - 1, R)).wait_send()


def far_body(R, C, z_spectra, n_spectra, z_flags, n_flags, pair_mask):
    windows, bins = z_spectra.shape[1], z_spectra.shape[3]
    rows, blocks = bins // LANES, LAGS // LANES
    inner, turn, outer = far_tables(bins)

    def interleave(x):
        return x.reshape(1, windows, 2, rows, LANES).transpose(0, 1, 3, 2, 4).reshape(
            1, windows, 2 * rows, LANES)

    reach = min(REACH, R - 1)
    DMA = pltpu.SemaphoreType.DMA
    out = pl.pallas_call(
        functools.partial(far_kernel, R, C, reach),
        out_shape=pltpu.VMEM((C * blocks * R, LANES), jnp.float32),
        in_specs=[pl.BlockSpec(memory_space=pl.ANY)] * 8,
        out_specs=pl.BlockSpec(memory_space=pltpu.VMEM),
        scratch_shapes=[
            pltpu.VMEM((C, windows, 2 * rows, LANES), jnp.float32),
            pltpu.VMEM((R, windows, 2 * rows, LANES), jnp.float32),
            pltpu.VMEM((C, 1, windows), jnp.int32),
            pltpu.VMEM((R, 1, windows), jnp.int32),
            pltpu.VMEM(pair_mask.shape, jnp.int32),
            pltpu.VMEM(inner.shape, jnp.bfloat16),
            pltpu.VMEM(turn.shape, jnp.float32),
            pltpu.VMEM(outer.shape, jnp.bfloat16),
            DMA((8,)),
            DMA((C, windows)), DMA((C, windows)), DMA((C,)), DMA((C,)),
            DMA((R, windows)), DMA((R, windows)), DMA((R, windows)),
            DMA((R,)), DMA((R,)), DMA((R,)),
            DMA((2, reach, windows)), DMA((2, reach)), pltpu.SemaphoreType.REGULAR((2, reach + 1)),
            pltpu.SemaphoreType.REGULAR,
        ],
        compiler_params=pltpu.CompilerParams(collective_id=0, has_side_effects=True),
        name="correlate",
    )(interleave(z_spectra), interleave(n_spectra), z_flags, n_flags, pair_mask,
      jnp.asarray(inner), jnp.asarray(turn), jnp.asarray(outer))
    return out.reshape(C, blocks, R, LANES).transpose(0, 2, 1, 3).reshape(C, R, LAGS)


def solution(mesh):
    placed = (
        P(("grp", "row", "col"), None, None, None),
        P(("grp", "col", "row"), None, None, None),
        P(("grp", "row", "col"), None),
        P(("grp", "col", "row"), None),
        P(("grp", "row"), "col"),
    )
    return jax.shard_map(
        functools.partial(body, mesh.shape["row"], mesh.shape["col"]), mesh=mesh,
        in_specs=placed, out_specs=P(("grp", "row"), "col", None), check_vma=False,
    )
```

```python
import functools
import math

import jax
import jax.numpy as jnp
import numpy as np
from jax import lax
from jax.experimental import pallas as pl
from jax.experimental.pallas import tpu as pltpu
from jax.sharding import PartitionSpec as P

LAGS = 512
LANES = 128
MESH = pl.DeviceIdType.MESH
REACH = 3
SENDS = (
    ((0, 1, (3,)), (0, 3, (5,))),
    ((0, 1, (3,)), (0, 3, (5,))),
    ((1, 0, (0,)), (1, 2, (3,)), (0, 2, (6,))),
    ((1, 0, (0,)), (1, 2, (3,)), (2, 0, (6,)), (0, 2, (6,))),
    ((2, 0, (0,)), (2, 1, (2,)), (2, 3, (3,)), (1, 3, (6,))),
    ((2, 1, (0,)), (2, 3, (3,)), (3, 1, (6,)), (1, 3, (6,))),
    ((3, 0, (0,)), (3, 2, (2,)), (3, 1, (2,))),
    ((3, 0, (0, 2)), (3, 2, (0,))),
)
TAKES = ((1, 2, 3), (1, 3, 2), (0, 2, 3), (0, 2, 3), (1, 3, 0), (1, 3, 0), (2, 0, 1), (2, 0, 1))


def tables(bins):
    rows = bins // LANES
    period = 2 * rows
    blocks, split = LAGS // period, LANES // period
    kt, short, lane = np.arange(rows), np.arange(period), np.arange(LANES)
    phi = 2 * np.pi * ((short[:, None] * kt[None, :]) % period) / period
    inner = np.block([[np.cos(phi), -np.sin(phi)], [np.sin(phi), np.cos(phi)]])
    psi = np.pi * (short[:, None] * lane[None, :]) / bins
    hop = np.arange(blocks).reshape(-1, split).T.reshape(-1) - blocks // 2
    chi = np.pi * ((period * hop[:, None] * lane[None, :]) % (2 * bins)) / bins
    outer = np.stack([np.cos(chi), -np.sin(chi)]).astype(np.float32)
    high = outer.astype(jnp.bfloat16).astype(np.float32)
    low = (outer - high).astype(jnp.bfloat16).astype(np.float32)
    wide = np.pad(inner, ((0, 0), (0, LANES - inner.shape[1])))
    parts = [wide, np.cos(psi), np.sin(psi), high[0], low[0], high[1], low[1]]
    return np.concatenate(parts, 0).astype(np.float32)


def kernel(R, C, z_hbm, n_hbm, zf_hbm, nf_hbm, mask_hbm, table_hbm, out_ref,
           held, flags, mask_buf, table, n_recv, z_recv, flag_recv, sent, row_ready, col_ready):
    row, col = lax.axis_index("row"), lax.axis_index("col")
    W = held.shape[1]
    bin_rows = held.shape[2] // 2
    period = 2 * bin_rows
    blocks = LAGS // period
    odd = lax.rem(col, 2) == 1
    partner = col + 1 - 2 * lax.rem(col, 2)
    place = 2 * row + lax.rem(col, 2)

    def wait_all(ref, count, sem):
        some = ref.at[pl.ds(0, count)]
        pltpu.make_async_copy(some, some, sem).wait()

    n_load = pltpu.make_async_copy(n_hbm.at[0], held.at[row], n_recv.at[row, 0])
    n_parts = [pltpu.make_async_copy(n_hbm.at[0, w], held.at[row, w], n_recv.at[row, 0]) for w in range(W)]
    z_load = pltpu.make_async_copy(z_hbm.at[0], held.at[R + col], z_recv.at[col])
    for part in n_parts:
        part.start()
    pltpu.make_async_copy(nf_hbm, flags.at[row], sent.at[1]).start()
    pltpu.make_async_copy(zf_hbm, flags.at[R + col], sent.at[1]).start()
    z_load.start()

    def row_there(hop):
        return (row + hop < R) & (row + hop >= 0)

    barrier = pltpu.get_barrier_semaphore()
    for hop in range(1, R):
        @pl.when(row_there(hop))
        def _():
            pl.semaphore_signal(barrier, inc=1, device_id={"row": row + hop}, device_id_type=MESH)

    for step in range(1, C):
        @pl.when(col + step < C)
        def _():
            pl.semaphore_signal(barrier, inc=1, device_id={"col": col + step}, device_id_type=MESH)

    @pl.when(row + col > 0)
    def _():
        pl.semaphore_wait(barrier, row + col)

    for hop in range(1, R):
        @pl.when(row_there(-hop))
        def _():
            pl.semaphore_signal(row_ready.at[hop - 1], inc=1, device_id={"row": row - hop}, device_id_type=MESH)

    for step in range(1, C):
        @pl.when(col >= step)
        def _():
            pl.semaphore_signal(col_ready, inc=1, device_id={"col": col - step}, device_id_type=MESH)

    def spectrum(owner, w, to):
        return pltpu.make_async_remote_copy(
            held.at[owner, w], held.at[owner, w], sent.at[0], n_recv.at[owner, w],
            device_id={"row": to}, device_id_type=MESH)

    def z_copy(owner, to):
        return pltpu.make_async_remote_copy(
            held.at[R + owner], held.at[R + owner], sent.at[0], z_recv.at[owner],
            device_id={"col": to}, device_id_type=MESH)

    def flag(slot, **to):
        return pltpu.make_async_remote_copy(
            flags.at[slot], flags.at[slot], sent.at[1], flag_recv, device_id=to, device_id_type=MESH)

    def at(fn):
        for here in range(2 * R):
            @pl.when(place == here)
            def _():
                fn(here)

    def step_sends(number):
        def send(here):
            for owner, to, when in SENDS[here]:
                for w in range(W):
                    if when[w % len(when)] == number:
                        if owner != here // 2:
                            spectrum(owner, w, to).wait_recv()
                        spectrum(owner, w, to).start()
        if any(number in when for sends in SENDS for _, _, when in sends):
            at(send)

    wait_all(flags, 2, sent.at[1])
    for hop in range(1, R):
        @pl.when(row_there(-hop))
        def _():
            flag(row, row=row - hop).start()

    n_load.wait()
    mask_load = pltpu.make_async_copy(mask_hbm, mask_buf, n_recv.at[row, 0])
    mask_load.start()
    step_sends(0)

    def send_z(step, ahead):
        to = lax.rem(col + step, C)

        @pl.when((to > col) == ahead)
        def _():
            @pl.when(jnp.logical_not(odd) | (lax.rem(to, 2) == 1) | (to == partner))
            def _():
                z_copy(col, to).start()

            flag(R + col, col=to).start()

    z_load.wait()
    table_load = pltpu.make_async_copy(table_hbm, table, z_recv.at[col])
    table_load.start()
    for step in range(1, C):
        send_z(step, False)
    step_sends(1)

    @pl.when(col < C - 1)
    def _():
        pl.semaphore_wait(col_ready, C - 1 - col)

    for step in range(1, C):
        send_z(step, True)
    step_sends(2)
    for hop in range(1, R):
        @pl.when(row_there(hop))
        def _():
            pl.semaphore_wait(row_ready.at[hop - 1], 1)
            flag(row, row=row + hop).start()

        step_sends(2 + hop)

    step_sends(R + 2)

    @pl.when(odd)
    def _():
        for step in range(2, C, 2):
            owner = lax.rem(col + step, C)
            z_copy(owner, partner).wait_recv()
            z_copy(owner, partner).start()

    step_sends(R + 3)
    mask_load.wait()
    table_load.wait()
    spot = lax.broadcasted_iota(jnp.int32, (bin_rows, LANES), 0) + lax.broadcasted_iota(
        jnp.int32, (bin_rows, LANES), 1)
    weight = jnp.where(spot == 0, 1.0, 2.0).astype(jnp.float32)
    split = LANES // period
    lines = blocks // split
    groups = C // split
    lane_side = lax.broadcasted_iota(jnp.int32, (blocks, LANES), 1) // period
    line_side = lax.broadcasted_iota(jnp.int32, (blocks, LANES), 0) // lines

    def spread_out(rows):
        picked = jnp.zeros((blocks, LANES), jnp.float32) + rows[0]
        for h in range(1, split):
            picked = jnp.where(line_side == h, rows[h], picked)
        return picked

    def gains(owner):
        passed = flags[owner].astype(jnp.float32)
        mask = mask_buf[...].astype(jnp.float32)
        here = lax.broadcasted_iota(jnp.int32, mask.shape, 1) == owner
        kept = jnp.sum(jnp.where(here, mask, 0.0), axis=1, keepdims=True)
        each = []
        for i in range(C):
            marks = flags[R + i].astype(jnp.float32) * passed
            count = jnp.maximum(jnp.sum(marks, axis=1, keepdims=True), 1.0)
            each.append(marks * kept[i:i + 1] / count)
        return [[spread_out([each[g * split + h][:, w:w + 1] for h in range(split)]) for g in range(groups)]
                for w in range(W)]

    def correlate(owner):
        inner = table[:2 * period, :period].astype(jnp.bfloat16)
        turn = table[2 * period:3 * period, :], table[3 * period:4 * period, :]
        outer = jnp.concatenate([table[4 * period:4 * period + 2 * blocks, :], table[4 * period + 2 * blocks:, :]], 1)
        outer = outer.astype(jnp.bfloat16)
        cross = []
        for w in range(W):
            n_real = held[owner, w, pl.ds(0, bin_rows, stride=2), :] * weight
            n_imag = held[owner, w, pl.ds(1, bin_rows, stride=2), :] * weight
            for i in range(C):
                z_real = held[R + i, w, pl.ds(0, bin_rows, stride=2), :]
                z_imag = held[R + i, w, pl.ds(1, bin_rows, stride=2), :]
                cross.append(jnp.concatenate(
                    [z_real * n_real + z_imag * n_imag, z_imag * n_real - z_real * n_imag], 0
                ).astype(jnp.bfloat16))
        short = jnp.dot(inner, jnp.concatenate(cross, 1), preferred_element_type=jnp.float32)
        turned = []
        for at in range(W * C):
            real = short[:period, at * LANES:(at + 1) * LANES]
            imag = short[period:, at * LANES:(at + 1) * LANES]
            turned.append(jnp.concatenate(
                [real * turn[0] - imag * turn[1], real * turn[1] + imag * turn[0]], 1).astype(jnp.bfloat16))
        lags = lax.dot_general(outer, jnp.concatenate(turned, 0), (((1,), (1,)), ((), ())),
                               preferred_element_type=jnp.float32)
        lags = lags[:blocks] + lags[blocks:]
        return [[lags[:, (w * groups + g) * LANES:(w * groups + g + 1) * LANES] for g in range(groups)]
                for w in range(W)]

    def normal(corr):
        power = jnp.sum(corr * corr, axis=0, keepdims=True)
        whole = spread_out([jnp.sum(jnp.where(lane_side[:1] == h, power, 0.0), axis=1, keepdims=True)
                            for h in range(split)])
        laid = corr
        for by in range(1, split):
            moved = pltpu.roll(pltpu.roll(corr, by * period, 1), (split - by) * lines, 0)
            laid = jnp.where(lax.rem(lane_side - line_side + split, split) == by, moved, laid)
        return laid * lax.rsqrt(whole / LAGS + 1e-05)

    def finish(owner, units, gain):
        for g in range(groups):
            total = units[0][g] * gain[0][g]
            for w in range(1, W):
                total = total + units[w][g] * gain[w][g]
            for h in range(split):
                i = g * split + h
                out_ref[pl.ds(i * lines * R + owner, lines, stride=R), :] = total[h * lines:(h + 1) * lines]

    def pick(p):
        owner = row * 0
        for here in range(2 * R):
            owner = jnp.where(place == here, TAKES[here][p - 1], owner)
        return owner

    def receive(p):
        def take(here):
            owner = TAKES[here][p - 1]
            if all(passed != owner for passed, _, _ in SENDS[here]):
                for w in range(W):
                    spectrum(owner, w, here // 2).wait_recv()
        at(take)

    for step in range(1, C):
        owner = lax.rem(col + step, C)

        @pl.when(jnp.logical_not(odd & (lax.rem(owner, 2) == 1)))
        def _():
            z_copy(owner, col).wait_recv()

    owners = [row] + [pick(p) for p in range(1, R)]
    gain = []

    def run(batches, keep):
        done = []
        for batch in batches:
            for p in batch:
                if p > 0:
                    receive(p)
            corrs = [correlate(owners[p]) for p in batch]
            done += [(p, [[normal(c) for c in part] for part in corr]) for p, corr in zip(batch, corrs)]
            if not gain:
                wait_all(flags, R + C - 2, flag_recv)
                gain.extend(gains(owner) for owner in owners)
            if not keep:
                for p, units in done:
                    finish(owners[p], units, gain[p])
                done = []
        for p, units in done:
            finish(owners[p], units, gain[p])

    run([(0, 1)], False)
    rest = list(range(2, R))
    together = jnp.logical_not(odd) & (row == 1)

    @pl.when(together)
    def _():
        run([rest], True)

    @pl.when(jnp.logical_not(together))
    def _():
        run([[p] for p in rest], False)

    def finish_sends(here):
        wait_all(held, len(SENDS[here]) + C - 1, sent.at[0])

    at(finish_sends)
    wait_all(flags, R + C - 2, sent.at[1])


def body(R, C, z_spectra, n_spectra, z_flags, n_flags, pair_mask):
    windows, bins = z_spectra.shape[1], z_spectra.shape[3]
    rows = bins // LANES
    blocks, split = LAGS // (2 * rows), LANES // (2 * rows)
    if 2 * R != len(SENDS) or C % 2 or C % split:
        return far_body(R, C, z_spectra, n_spectra, z_flags, n_flags, pair_mask)
    table = jnp.asarray(tables(bins))

    def interleave(x):
        return x.reshape(1, windows, 2, rows, LANES).transpose(0, 1, 3, 2, 4).reshape(
            1, windows, 2 * rows, LANES)

    DMA, REGULAR = pltpu.SemaphoreType.DMA, pltpu.SemaphoreType.REGULAR
    lines = blocks // split
    out = pl.pallas_call(
        functools.partial(kernel, R, C),
        out_shape=pltpu.VMEM((C * lines * R, LANES), jnp.float32),
        in_specs=[pl.BlockSpec(memory_space=pl.ANY)] * 6,
        out_specs=pl.BlockSpec(memory_space=pltpu.VMEM),
        scratch_shapes=[
            pltpu.VMEM((R + C, windows, 2 * rows, LANES), jnp.float32),
            pltpu.VMEM((R + C, 1, windows), jnp.int32),
            pltpu.VMEM(pair_mask.shape, jnp.int32),
            pltpu.VMEM(table.shape, jnp.float32),
            DMA((R, windows)), DMA((C,)), DMA, DMA((2,)), REGULAR((R - 1,)), REGULAR,
        ],
        compiler_params=pltpu.CompilerParams(collective_id=0, has_side_effects=True),
        name="correlate",
    )(interleave(z_spectra), interleave(n_spectra), z_flags, n_flags, pair_mask, table)
    return out.reshape(C, lines, R, LANES).transpose(0, 2, 1, 3).reshape(C, R, LAGS)


def far_tables(bins):
    rows, blocks = bins // LANES, LAGS // LANES
    period = 2 * rows
    kt, short = np.arange(rows), np.arange(period)
    phi = 2 * np.pi * ((short[:, None] * kt[None, :]) % period) / period
    inner = np.block([[np.cos(phi), -np.sin(phi)], [np.sin(phi), np.cos(phi)]])
    lane, t0 = np.arange(LANES), np.arange(LANES)
    psi = np.pi * (t0[:, None] * lane[None, :]) / bins
    turn = np.stack([np.cos(psi), np.sin(psi)]).astype(np.float32)
    hop = np.arange(blocks) - blocks // 2
    chi = np.pi * ((LANES * hop[:, None] * lane[None, :]) % (2 * bins)) / bins
    outer = np.concatenate([np.cos(chi), -np.sin(chi)], 1).astype(np.float32)
    high = outer.astype(jnp.bfloat16)
    low = (outer - high.astype(np.float32)).astype(jnp.bfloat16)
    return inner.astype(jnp.bfloat16), turn, np.concatenate([high, low], 0)


def far_kernel(R, C, reach, z_hbm, n_hbm, zf_hbm, nf_hbm, mask_hbm, inner_hbm, turn_hbm, outer_hbm, out_ref,
           z_buf, n_buf, zf_buf, nf_buf, mask_buf, inner, turn, outer,
           load_sem, z_send, z_recv, zf_send, zf_recv, right_send, left_send, n_recv,
           rf_send, lf_send, nf_recv, own_send, own_f_send, ready, turn_sem):
    row, col = lax.axis_index("row"), lax.axis_index("col")
    W = z_buf.shape[1]
    bin_rows = z_buf.shape[2] // 2
    period = inner.shape[0] // 2
    blocks = outer.shape[0] // 2

    loads = [
        pltpu.make_async_copy(n_hbm.at[0], n_buf.at[row], load_sem.at[0]),
        pltpu.make_async_copy(z_hbm.at[0], z_buf.at[col], load_sem.at[1]),
        pltpu.make_async_copy(nf_hbm, nf_buf.at[row], load_sem.at[2]),
        pltpu.make_async_copy(zf_hbm, zf_buf.at[col], load_sem.at[3]),
        pltpu.make_async_copy(mask_hbm, mask_buf, load_sem.at[4]),
        pltpu.make_async_copy(inner_hbm, inner, load_sem.at[5]),
        pltpu.make_async_copy(turn_hbm, turn, load_sem.at[6]),
        pltpu.make_async_copy(outer_hbm, outer, load_sem.at[7]),
    ]
    for load in loads:
        load.start()

    has_left, has_right = row > 0, row < R - 1
    barrier = pltpu.get_barrier_semaphore()

    def there(hop):
        return (row + hop < R) if hop > 0 else (row + hop >= 0)

    for hop in (-1, 1):
        @pl.when(there(hop))
        def _():
            pl.semaphore_signal(barrier, inc=1, device_id={"row": row + hop}, device_id_type=MESH)

    for step in range(1, C):
        pl.semaphore_signal(barrier, inc=1, device_id={"col": lax.rem(col + step, C)}, device_id_type=MESH)
    pl.semaphore_wait(barrier, C - 1 + jnp.where(has_left, 1, 0) + jnp.where(has_right, 1, 0))

    def tell(hop):
        far = abs(hop) + 1
        back = -1 if hop > 0 else 1
        if far <= reach:
            @pl.when(there(hop) & there(back))
            def _():
                pl.semaphore_signal(ready.at[int(hop < 0), far], inc=1,
                                    device_id={"row": row + back}, device_id_type=MESH)

    def learn(hop):
        @pl.when(there(hop))
        def _():
            pl.semaphore_wait(ready.at[int(hop < 0), abs(hop)], 1)

    tell(1)
    tell(-1)

    def spectrum(owner, w, send, to):
        return pltpu.make_async_remote_copy(
            n_buf.at[owner, w], n_buf.at[owner, w], send.at[owner, w], n_recv.at[owner, w],
            device_id={"row": to}, device_id_type=MESH)

    def flag(owner, send, to):
        return pltpu.make_async_remote_copy(
            nf_buf.at[owner], nf_buf.at[owner], send.at[owner], nf_recv.at[owner],
            device_id={"row": to}, device_id_type=MESH)

    def z_copy(owner, w, to):
        return pltpu.make_async_remote_copy(
            z_buf.at[owner, w], z_buf.at[owner, w], z_send.at[to, w], z_recv.at[owner, w],
            device_id={"col": to}, device_id_type=MESH)

    def zf_copy(owner, to):
        return pltpu.make_async_remote_copy(
            zf_buf.at[owner], zf_buf.at[owner], zf_send.at[to], zf_recv.at[owner],
            device_id={"col": to}, device_id_type=MESH)

    def own_copy(hop, w):
        side, far = int(hop < 0), abs(hop) - 1
        return pltpu.make_async_remote_copy(
            n_buf.at[row, w], n_buf.at[row, w], own_send.at[side, far, w], n_recv.at[row, w],
            device_id={"row": row + hop}, device_id_type=MESH)

    def own_flag(hop):
        side, far = int(hop < 0), abs(hop) - 1
        return pltpu.make_async_remote_copy(
            nf_buf.at[row], nf_buf.at[row], own_f_send.at[side, far], nf_recv.at[row],
            device_id={"row": row + hop}, device_id_type=MESH)

    pairs = C % 2 == 0
    first = (lax.rem(col, 2) == 0) if pairs else (col >= 0)

    def send_own(hop):
        @pl.when(there(hop))
        def _():
            own_flag(hop).start()
            for w in range(W):
                own_copy(hop, w).start()

    for hop in range(2, reach + 1):
        learn(-hop)
        tell(-hop)
    loads[2].wait()
    loads[0].wait()
    @pl.when(first)
    def _():
        for hop in range(reach, 0, -1):
            send_own(-hop)

    send_own(1)
    loads[3].wait()
    loads[1].wait()
    for step in range(1, C):
        zf_copy(col, lax.rem(col + step, C)).start()
    for w in range(W):
        for step in range(1, C):
            z_copy(col, w, lax.rem(col + step, C)).start()
    @pl.when(first)
    def _():
        for hop in range(1, reach + 1):
            @pl.when((row == hop) | ((row > hop) & (hop == reach)))
            def _():
                for w in range(W):
                    own_copy(-hop, w).wait_send()

        if pairs:
            pl.semaphore_signal(turn_sem, inc=1, device_id={"col": lax.rem(col + 1, C)}, device_id_type=MESH)

    @pl.when(jnp.logical_not(first))
    def _():
        send_own(-1)
        held = row == R - 1

        @pl.when(held)
        def _():
            pl.semaphore_wait(turn_sem, 1)

        for hop in range(reach, 1, -1):
            send_own(-hop)

        @pl.when(jnp.logical_not(held))
        def _():
            pl.semaphore_wait(turn_sem, 1)

    for hop in range(2, reach + 1):
        learn(hop)
        tell(hop)
        send_own(hop)
    for load in loads[4:]:
        load.wait()

    spot = lax.broadcasted_iota(jnp.int32, (bin_rows, LANES), 0) + lax.broadcasted_iota(
        jnp.int32, (bin_rows, LANES), 1)
    weight = jnp.where(spot == 0, 1.0, 2.0).astype(jnp.float32)

    def unit(owner):
        pairs = [(i, w) for i in range(C) for w in range(W)]
        n_real = [n_buf[owner, w, pl.ds(0, bin_rows, stride=2), :] * weight for w in range(W)]
        n_imag = [n_buf[owner, w, pl.ds(1, bin_rows, stride=2), :] * weight for w in range(W)]
        cross = []
        for i, w in pairs:
            z_real = z_buf[i, w, pl.ds(0, bin_rows, stride=2), :]
            z_imag = z_buf[i, w, pl.ds(1, bin_rows, stride=2), :]
            cross.append(jnp.concatenate(
                [z_real * n_real[w] + z_imag * n_imag[w], z_imag * n_real[w] - z_real * n_imag[w]], 0
            ).astype(jnp.bfloat16))
        short = jnp.dot(inner[...], jnp.concatenate(cross, 1), preferred_element_type=jnp.float32)
        turned = []
        for at in range(len(pairs)):
            real = short[:period, at * LANES:(at + 1) * LANES]
            imag = short[period:, at * LANES:(at + 1) * LANES]
            for part in range(LANES // period):
                cosine = turn[0, part * period:(part + 1) * period, :]
                sine = turn[1, part * period:(part + 1) * period, :]
                turned.append(jnp.concatenate(
                    [real * cosine - imag * sine, real * sine + imag * cosine], 1).astype(jnp.bfloat16))
        lags = lax.dot_general(outer[...], jnp.concatenate(turned, 0), (((1,), (1,)), ((), ())),
                               preferred_element_type=jnp.float32)
        lags = lags[:blocks] + lags[blocks:]
        n_flag = nf_buf[owner].astype(jnp.float32)
        mask = mask_buf[...].astype(jnp.float32)
        here = lax.broadcasted_iota(jnp.int32, mask.shape, 1) == owner
        kept = jnp.sum(jnp.where(here, mask, 0.0), axis=1, keepdims=True)
        for i in range(C):
            marks = zf_buf[i].astype(jnp.float32) * n_flag
            count = jnp.maximum(jnp.sum(marks, axis=1, keepdims=True), 1.0)
            gain = marks * kept[i:i + 1] / count
            total = jnp.zeros((blocks, LANES), jnp.float32)
            for w in range(W):
                at = i * W + w
                corr = lags[:, at * LANES:(at + 1) * LANES]
                power = jnp.sum(jnp.sum(corr * corr, axis=0, keepdims=True), axis=1, keepdims=True)
                spread = jnp.sqrt(power / LAGS + 1e-05)
                total = total + corr * (gain[:, w:w + 1] / spread)
            out_ref[pl.ds(i * blocks * R + owner, blocks, stride=R), :] = total

    def arrive(owner, w, forward, send, f_send, to):
        if w == 0:
            flag(owner, f_send, to).wait_recv()
        spectrum(owner, w, send, to).wait_recv()
        if forward is False:
            return

        @pl.when(forward)
        def _():
            if w == 0:
                flag(owner, f_send, to).start()
            spectrum(owner, w, send, to).start()

    for step in range(1, C):
        zf_copy(lax.rem(col + C - step, C), lax.rem(col + step, C)).wait_recv()
    for w in range(W):
        for step in range(1, C):
            z_copy(lax.rem(col + C - step, C), w, lax.rem(col + step, C)).wait_recv()
    unit(row)

    def take(p):
        left = p <= row
        owner = jnp.where(left, row - p, p)
        if reach == R - 1:
            for w in range(W):
                arrive(owner, w, False, right_send, rf_send, lax.rem(row + 1, R))
        else:
            @pl.when(left)
            def _():
                for w in range(W):
                    arrive(owner, w, has_right & (p >= reach), right_send, rf_send, lax.rem(row + 1, R))

            @pl.when(p > row)
            def _():
                for w in range(W):
                    arrive(owner, w, has_left & (p - row >= reach), left_send, lf_send,
                           lax.rem(row + R - 1, R))
        unit(owner)

    if R <= 4:
        for p in range(1, R):
            take(p)
    else:
        pl.loop(1, R)(take)

    hops = [sign * hop for hop in range(1, reach + 1) for sign in (1, -1)]
    for hop in hops:
        @pl.when(there(hop))
        def _():
            own_flag(hop).wait_send()
            if hop > 0:
                for w in range(W):
                    own_copy(hop, w).wait_send()
            else:
                waited = first & ((row == -hop) | ((row > -hop) & (-hop == reach)))

                @pl.when(jnp.logical_not(waited))
                def _():
                    for w in range(W):
                        own_copy(hop, w).wait_send()

    for step in range(1, C):
        zf_copy(col, lax.rem(col + step, C)).wait_send()
        for w in range(W):
            z_copy(col, w, lax.rem(col + step, C)).wait_send()

    if reach == R - 1:
        return

    @pl.loop(0, R)
    def _(owner):
        @pl.when(has_right & (owner <= row - reach))
        def _():
            flag(owner, rf_send, lax.rem(row + 1, R)).wait_send()
            for w in range(W):
                spectrum(owner, w, right_send, lax.rem(row + 1, R)).wait_send()

        @pl.when(has_left & (owner >= row + reach))
        def _():
            flag(owner, lf_send, lax.rem(row + R - 1, R)).wait_send()
            for w in range(W):
                spectrum(owner, w, left_send, lax.rem(row + R - 1, R)).wait_send()


def far_body(R, C, z_spectra, n_spectra, z_flags, n_flags, pair_mask):
    windows, bins = z_spectra.shape[1], z_spectra.shape[3]
    rows, blocks = bins // LANES, LAGS // LANES
    inner, turn, outer = far_tables(bins)

    def interleave(x):
        return x.reshape(1, windows, 2, rows, LANES).transpose(0, 1, 3, 2, 4).reshape(
            1, windows, 2 * rows, LANES)

    reach = min(REACH, R - 1)
    DMA = pltpu.SemaphoreType.DMA
    out = pl.pallas_call(
        functools.partial(far_kernel, R, C, reach),
        out_shape=pltpu.VMEM((C * blocks * R, LANES), jnp.float32),
        in_specs=[pl.BlockSpec(memory_space=pl.ANY)] * 8,
        out_specs=pl.BlockSpec(memory_space=pltpu.VMEM),
        scratch_shapes=[
            pltpu.VMEM((C, windows, 2 * rows, LANES), jnp.float32),
            pltpu.VMEM((R, windows, 2 * rows, LANES), jnp.float32),
            pltpu.VMEM((C, 1, windows), jnp.int32),
            pltpu.VMEM((R, 1, windows), jnp.int32),
            pltpu.VMEM(pair_mask.shape, jnp.int32),
            pltpu.VMEM(inner.shape, jnp.bfloat16),
            pltpu.VMEM(turn.shape, jnp.float32),
            pltpu.VMEM(outer.shape, jnp.bfloat16),
            DMA((8,)),
            DMA((C, windows)), DMA((C, windows)), DMA((C,)), DMA((C,)),
            DMA((R, windows)), DMA((R, windows)), DMA((R, windows)),
            DMA((R,)), DMA((R,)), DMA((R,)),
            DMA((2, reach, windows)), DMA((2, reach)), pltpu.SemaphoreType.REGULAR((2, reach + 1)),
            pltpu.SemaphoreType.REGULAR,
        ],
        compiler_params=pltpu.CompilerParams(collective_id=0, has_side_effects=True),
        name="correlate",
    )(interleave(z_spectra), interleave(n_spectra), z_flags, n_flags, pair_mask,
      jnp.asarray(inner), jnp.asarray(turn), jnp.asarray(outer))
    return out.reshape(C, blocks, R, LANES).transpose(0, 2, 1, 3).reshape(C, R, LAGS)


def solution(mesh):
    placed = (
        P(("grp", "row", "col"), None, None, None),
        P(("grp", "col", "row"), None, None, None),
        P(("grp", "row", "col"), None),
        P(("grp", "col", "row"), None),
        P(("grp", "row"), "col"),
    )
    return jax.shard_map(
        functools.partial(body, mesh.shape["row"], mesh.shape["col"]), mesh=mesh,
        in_specs=placed, out_specs=P(("grp", "row"), "col", None), check_vma=False,
    )
```

```python
import functools
import math

import jax
import jax.numpy as jnp
import numpy as np
from jax import lax
from jax.experimental import pallas as pl
from jax.experimental.pallas import tpu as pltpu
from jax.sharding import PartitionSpec as P

LAGS = 512
LANES = 128
MESH = pl.DeviceIdType.MESH
REACH = 3
SENDS = (
    ((0, 1, (3,)), (0, 3, (5,)), (2, 1, (8, -1))),
    ((0, 1, (3,)), (0, 3, (5,)), (2, 1, (7, -1))),
    ((1, 0, (0,)), (1, 2, (3,)), (0, 2, (6,))),
    ((1, 0, (0,)), (1, 2, (3,)), (2, 0, (-1, 6)), (0, 2, (6,))),
    ((2, 0, (0,)), (2, 1, (-1, 2)), (2, 3, (3,)), (1, 3, (6,))),
    ((2, 1, (-1, 0)), (2, 0, (0, -1)), (2, 3, (3,)), (3, 1, (6,)), (1, 3, (6,))),
    ((3, 0, (0,)), (3, 2, (2,)), (3, 1, (2,))),
    ((3, 2, (0,)), (3, 0, (2,))),
)
TAKES = ((1, 2, 3), (1, 2, 3), (0, 2, 3), (0, 2, 3), (1, 3, 0), (1, 3, 0), (2, 0, 1), (2, 0, 1))


def tables(bins):
    rows = bins // LANES
    period = 2 * rows
    blocks, split = LAGS // period, LANES // period
    kt, short, lane = np.arange(rows), np.arange(period), np.arange(LANES)
    phi = 2 * np.pi * ((short[:, None] * kt[None, :]) % period) / period
    inner = np.block([[np.cos(phi), -np.sin(phi)], [np.sin(phi), np.cos(phi)]])
    psi = np.pi * (short[:, None] * lane[None, :]) / bins
    hop = np.arange(blocks).reshape(-1, split).T.reshape(-1) - blocks // 2
    chi = np.pi * ((period * hop[:, None] * lane[None, :]) % (2 * bins)) / bins
    outer = np.stack([np.cos(chi), -np.sin(chi)]).astype(np.float32)
    high = outer.astype(jnp.bfloat16).astype(np.float32)
    low = (outer - high).astype(jnp.bfloat16).astype(np.float32)
    wide = np.pad(inner, ((0, 0), (0, LANES - inner.shape[1])))
    parts = [wide, np.cos(psi), np.sin(psi), high[0], low[0], high[1], low[1]]
    return np.concatenate(parts, 0).astype(np.float32)


def kernel(R, C, z_hbm, n_hbm, zf_hbm, nf_hbm, mask_hbm, table_hbm, out_ref,
           held, flags, mask_buf, table, n_recv, z_recv, flag_recv, sent, row_ready, col_ready):
    row, col = lax.axis_index("row"), lax.axis_index("col")
    W = z_hbm.shape[1]
    bin_rows = held.shape[1] // 2
    period = 2 * bin_rows
    blocks = LAGS // period
    odd = lax.rem(col, 2) == 1
    partner = col + 1 - 2 * lax.rem(col, 2)
    place = 2 * row + lax.rem(col, 2)

    def wait_all(ref, count, sem):
        some = ref.at[pl.ds(0, count)]
        pltpu.make_async_copy(some, some, sem).wait()

    def n_slots(owner):
        return held.at[pl.ds(owner * W, W)]

    def z_slots(owner):
        return held.at[pl.ds((R + owner) * W, W)]

    n_load = pltpu.make_async_copy(n_hbm.at[0], n_slots(row), n_recv.at[row, 0])
    z_load = pltpu.make_async_copy(z_hbm.at[0], z_slots(col), z_recv.at[col])
    for w in range(W):
        pltpu.make_async_copy(n_hbm.at[0, w], held.at[row * W + w], n_recv.at[row, 0]).start()

    pltpu.make_async_copy(nf_hbm, flags.at[row], sent.at[1]).start()
    pltpu.make_async_copy(zf_hbm, flags.at[R + col], sent.at[1]).start()
    z_load.start()

    def row_there(hop):
        return (row + hop < R) & (row + hop >= 0)

    barrier = pltpu.get_barrier_semaphore()
    for hop in range(1, R):
        @pl.when(row_there(hop))
        def _():
            pl.semaphore_signal(barrier, inc=1, device_id={"row": row + hop}, device_id_type=MESH)

    for step in range(1, C):
        @pl.when(col + step < C)
        def _():
            pl.semaphore_signal(barrier, inc=1, device_id={"col": col + step}, device_id_type=MESH)

    @pl.when(row + col > 0)
    def _():
        pl.semaphore_wait(barrier, row + col)

    for hop in range(1, R):
        @pl.when(row_there(-hop))
        def _():
            pl.semaphore_signal(row_ready.at[hop - 1], inc=1, device_id={"row": row - hop}, device_id_type=MESH)

    for step in range(1, C):
        @pl.when(col >= step)
        def _():
            pl.semaphore_signal(col_ready, inc=1, device_id={"col": col - step}, device_id_type=MESH)

    def spectrum(owner, w, to):
        return pltpu.make_async_remote_copy(
            held.at[owner * W + w], held.at[owner * W + w], sent.at[0], n_recv.at[owner, w],
            device_id={"row": to}, device_id_type=MESH)

    def z_copy(owner, to):
        return pltpu.make_async_remote_copy(
            z_slots(owner), z_slots(owner), sent.at[0], z_recv.at[owner],
            device_id={"col": to}, device_id_type=MESH)

    def flag(slot, **to):
        return pltpu.make_async_remote_copy(
            flags.at[slot], flags.at[slot], sent.at[1], flag_recv, device_id=to, device_id_type=MESH)

    def at(fn):
        for here in range(2 * R):
            @pl.when(place == here)
            def _():
                fn(here)

    def step_sends(number):
        def send(here):
            for owner, to, when in SENDS[here]:
                for w in range(W):
                    if when[w % len(when)] == number:
                        if owner != here // 2:
                            spectrum(owner, w, to).wait_recv()
                        spectrum(owner, w, to).start()
        if any(number in when for sends in SENDS for _, _, when in sends):
            at(send)

    wait_all(flags, 2, sent.at[1])
    for hop in range(1, R):
        @pl.when(row_there(-hop))
        def _():
            flag(row, row=row - hop).start()

    n_load.wait()
    mask_load = pltpu.make_async_copy(mask_hbm, mask_buf, n_recv.at[row, 0])
    mask_load.start()
    step_sends(0)

    def send_z(step, ahead):
        to = lax.rem(col + step, C)

        @pl.when((to > col) == ahead)
        def _():
            @pl.when(jnp.logical_not(odd) | (lax.rem(to, 2) == 1) | (to == partner))
            def _():
                z_copy(col, to).start()

            flag(R + col, col=to).start()

    z_load.wait()
    table_load = pltpu.make_async_copy(table_hbm, table, z_recv.at[col])
    table_load.start()
    for step in range(1, C):
        send_z(step, False)
    step_sends(1)

    @pl.when(col < C - 1)
    def _():
        pl.semaphore_wait(col_ready, C - 1 - col)

    for step in range(1, C):
        send_z(step, True)
    step_sends(2)
    for hop in range(1, R):
        @pl.when(row_there(hop))
        def _():
            pl.semaphore_wait(row_ready.at[hop - 1], 1)
            flag(row, row=row + hop).start()

        step_sends(2 + hop)

    step_sends(R + 2)

    @pl.when(odd)
    def _():
        for step in range(2, C, 2):
            owner = lax.rem(col + step, C)
            z_copy(owner, partner).wait_recv()
            z_copy(owner, partner).start()

    step_sends(R + 3)
    mask_load.wait()
    table_load.wait()
    spot = lax.broadcasted_iota(jnp.int32, (bin_rows, LANES), 0) + lax.broadcasted_iota(
        jnp.int32, (bin_rows, LANES), 1)
    weight = jnp.where(spot == 0, 1.0, 2.0).astype(jnp.float32)
    split = LANES // period
    lines = blocks // split
    groups = C // split
    lane_side = lax.broadcasted_iota(jnp.int32, (blocks, LANES), 1) // period
    line_side = lax.broadcasted_iota(jnp.int32, (blocks, LANES), 0) // lines

    def spread_out(rows):
        picked = jnp.zeros((blocks, LANES), jnp.float32) + rows[0]
        for h in range(1, split):
            picked = jnp.where(line_side == h, rows[h], picked)
        return picked

    def gains(owner):
        passed = flags[owner].astype(jnp.float32)
        mask = mask_buf[...].astype(jnp.float32)
        here = lax.broadcasted_iota(jnp.int32, mask.shape, 1) == owner
        kept = jnp.sum(jnp.where(here, mask, 0.0), axis=1, keepdims=True)
        each = []
        for i in range(C):
            marks = flags[R + i].astype(jnp.float32) * passed
            count = jnp.maximum(jnp.sum(marks, axis=1, keepdims=True), 1.0)
            each.append(marks * kept[i:i + 1] / count)
        return [[spread_out([each[g * split + h][:, w:w + 1] for h in range(split)]) for g in range(groups)]
                for w in range(W)]

    def correlate(owner):
        inner = table[:2 * period, :period].astype(jnp.bfloat16)
        turn = table[2 * period:3 * period, :], table[3 * period:4 * period, :]
        outer = jnp.concatenate([table[4 * period:4 * period + 2 * blocks, :], table[4 * period + 2 * blocks:, :]], 1)
        outer = outer.astype(jnp.bfloat16)
        cross = []
        for w in range(W):
            n_real = held[owner * W + w, pl.ds(0, bin_rows, stride=2), :] * weight
            n_imag = held[owner * W + w, pl.ds(1, bin_rows, stride=2), :] * weight
            for i in range(C):
                z_real = held[(R + i) * W + w, pl.ds(0, bin_rows, stride=2), :]
                z_imag = held[(R + i) * W + w, pl.ds(1, bin_rows, stride=2), :]
                cross.append(jnp.concatenate(
                    [z_real * n_real + z_imag * n_imag, z_imag * n_real - z_real * n_imag], 0
                ).astype(jnp.bfloat16))
        short = jnp.dot(inner, jnp.concatenate(cross, 1), preferred_element_type=jnp.float32)
        turned = []
        for at in range(W * C):
            real = short[:period, at * LANES:(at + 1) * LANES]
            imag = short[period:, at * LANES:(at + 1) * LANES]
            turned.append(jnp.concatenate(
                [real * turn[0] - imag * turn[1], real * turn[1] + imag * turn[0]], 1).astype(jnp.bfloat16))
        lags = lax.dot_general(outer, jnp.concatenate(turned, 0), (((1,), (1,)), ((), ())),
                               preferred_element_type=jnp.float32)
        lags = lags[:blocks] + lags[blocks:]
        return [[lags[:, (w * groups + g) * LANES:(w * groups + g + 1) * LANES] for g in range(groups)]
                for w in range(W)]

    def normal(corr):
        power = jnp.sum(corr * corr, axis=0, keepdims=True)
        whole = spread_out([jnp.sum(jnp.where(lane_side[:1] == h, power, 0.0), axis=1, keepdims=True)
                            for h in range(split)])
        laid = corr
        for by in range(1, split):
            moved = pltpu.roll(pltpu.roll(corr, by * period, 1), (split - by) * lines, 0)
            laid = jnp.where(lax.rem(lane_side - line_side + split, split) == by, moved, laid)
        return laid * lax.rsqrt(whole / LAGS + 1e-05)

    def finish(owner, units, gain):
        for g in range(groups):
            total = units[0][g] * gain[0][g]
            for w in range(1, W):
                total = total + units[w][g] * gain[w][g]
            for h in range(split):
                i = g * split + h
                out_ref[pl.ds(i * lines * R + owner, lines, stride=R), :] = total[h * lines:(h + 1) * lines]

    def pick(p):
        owner = row * 0
        for here in range(2 * R):
            owner = jnp.where(place == here, TAKES[here][p - 1], owner)
        return owner

    def receive(p):
        def take(here):
            owner = TAKES[here][p - 1]
            passed = [when for passed, _, when in SENDS[here] if passed == owner]
            for w in range(W):
                if all(when[w % len(when)] < 0 for when in passed):
                    spectrum(owner, w, here // 2).wait_recv()
        at(take)

    for step in range(1, C):
        owner = lax.rem(col + step, C)

        @pl.when(jnp.logical_not(odd & (lax.rem(owner, 2) == 1)))
        def _():
            z_copy(owner, col).wait_recv()

    owners = [row] + [pick(p) for p in range(1, R)]

    def run(*steps):
        done, gain = [], []
        for step in steps:
            if step == "send":
                step_sends(R + 4)
            elif step == "gain":
                wait_all(flags, R + C - 2, flag_recv)
                gain = [gains(owner) for owner in owners]
            else:
                for p in step:
                    if p > 0:
                        receive(p)
                corrs = [correlate(owners[p]) for p in step]
                done += [(p, [[normal(c) for c in part] for part in corr]) for p, corr in zip(step, corrs)]
            if gain:
                for p, units in done:
                    finish(owners[p], units, gain[p])
                done = []

    alone = jnp.logical_not(odd) & (row == 0)
    together = jnp.logical_not(odd) & (row == 1)

    @pl.when(alone)
    def _():
        run([0], "send", [1], "gain", [2], [3])

    @pl.when(together)
    def _():
        run([0, 1], "send", "gain", [2, 3])

    @pl.when(jnp.logical_not(alone | together))
    def _():
        run([0, 1], "send", "gain", [2], [3])

    def finish_sends(here):
        windows = sum(when[w % len(when)] >= 0 for _, _, when in SENDS[here] for w in range(W))
        wait_all(held, windows + (C - 1) * W, sent.at[0])

    at(finish_sends)
    wait_all(flags, R + C - 2, sent.at[1])


def body(R, C, z_spectra, n_spectra, z_flags, n_flags, pair_mask):
    windows, bins = z_spectra.shape[1], z_spectra.shape[3]
    rows = bins // LANES
    blocks, split = LAGS // (2 * rows), LANES // (2 * rows)
    if 2 * R != len(SENDS) or C % 2 or C % split:
        return far_body(R, C, z_spectra, n_spectra, z_flags, n_flags, pair_mask)
    table = jnp.asarray(tables(bins))

    def interleave(x):
        return x.reshape(1, windows, 2, rows, LANES).transpose(0, 1, 3, 2, 4).reshape(
            1, windows, 2 * rows, LANES)

    DMA, REGULAR = pltpu.SemaphoreType.DMA, pltpu.SemaphoreType.REGULAR
    lines = blocks // split
    out = pl.pallas_call(
        functools.partial(kernel, R, C),
        out_shape=pltpu.VMEM((C * lines * R, LANES), jnp.float32),
        in_specs=[pl.BlockSpec(memory_space=pl.ANY)] * 6,
        out_specs=pl.BlockSpec(memory_space=pltpu.VMEM),
        scratch_shapes=[
            pltpu.VMEM(((R + C) * windows, 2 * rows, LANES), jnp.float32),
            pltpu.VMEM((R + C, 1, windows), jnp.int32),
            pltpu.VMEM(pair_mask.shape, jnp.int32),
            pltpu.VMEM(table.shape, jnp.float32),
            DMA((R, windows)), DMA((C,)), DMA, DMA((2,)), REGULAR((R - 1,)), REGULAR,
        ],
        compiler_params=pltpu.CompilerParams(collective_id=0, has_side_effects=True),
        name="correlate",
    )(interleave(z_spectra), interleave(n_spectra), z_flags, n_flags, pair_mask, table)
    return out.reshape(C, lines, R, LANES).transpose(0, 2, 1, 3).reshape(C, R, LAGS)


def far_tables(bins):
    rows, blocks = bins // LANES, LAGS // LANES
    period = 2 * rows
    kt, short = np.arange(rows), np.arange(period)
    phi = 2 * np.pi * ((short[:, None] * kt[None, :]) % period) / period
    inner = np.block([[np.cos(phi), -np.sin(phi)], [np.sin(phi), np.cos(phi)]])
    lane, t0 = np.arange(LANES), np.arange(LANES)
    psi = np.pi * (t0[:, None] * lane[None, :]) / bins
    turn = np.stack([np.cos(psi), np.sin(psi)]).astype(np.float32)
    hop = np.arange(blocks) - blocks // 2
    chi = np.pi * ((LANES * hop[:, None] * lane[None, :]) % (2 * bins)) / bins
    outer = np.concatenate([np.cos(chi), -np.sin(chi)], 1).astype(np.float32)
    high = outer.astype(jnp.bfloat16)
    low = (outer - high.astype(np.float32)).astype(jnp.bfloat16)
    return inner.astype(jnp.bfloat16), turn, np.concatenate([high, low], 0)


def far_kernel(R, C, reach, z_hbm, n_hbm, zf_hbm, nf_hbm, mask_hbm, inner_hbm, turn_hbm, outer_hbm, out_ref,
           z_buf, n_buf, zf_buf, nf_buf, mask_buf, inner, turn, outer,
           load_sem, z_send, z_recv, zf_send, zf_recv, right_send, left_send, n_recv,
           rf_send, lf_send, nf_recv, own_send, own_f_send, ready, turn_sem):
    row, col = lax.axis_index("row"), lax.axis_index("col")
    W = z_buf.shape[1]
    bin_rows = z_buf.shape[2] // 2
    period = inner.shape[0] // 2
    blocks = outer.shape[0] // 2

    loads = [
        pltpu.make_async_copy(n_hbm.at[0], n_buf.at[row], load_sem.at[0]),
        pltpu.make_async_copy(z_hbm.at[0], z_buf.at[col], load_sem.at[1]),
        pltpu.make_async_copy(nf_hbm, nf_buf.at[row], load_sem.at[2]),
        pltpu.make_async_copy(zf_hbm, zf_buf.at[col], load_sem.at[3]),
        pltpu.make_async_copy(mask_hbm, mask_buf, load_sem.at[4]),
        pltpu.make_async_copy(inner_hbm, inner, load_sem.at[5]),
        pltpu.make_async_copy(turn_hbm, turn, load_sem.at[6]),
        pltpu.make_async_copy(outer_hbm, outer, load_sem.at[7]),
    ]
    for load in loads:
        load.start()

    has_left, has_right = row > 0, row < R - 1
    barrier = pltpu.get_barrier_semaphore()

    def there(hop):
        return (row + hop < R) if hop > 0 else (row + hop >= 0)

    for hop in (-1, 1):
        @pl.when(there(hop))
        def _():
            pl.semaphore_signal(barrier, inc=1, device_id={"row": row + hop}, device_id_type=MESH)

    for step in range(1, C):
        pl.semaphore_signal(barrier, inc=1, device_id={"col": lax.rem(col + step, C)}, device_id_type=MESH)
    pl.semaphore_wait(barrier, C - 1 + jnp.where(has_left, 1, 0) + jnp.where(has_right, 1, 0))

    def tell(hop):
        far = abs(hop) + 1
        back = -1 if hop > 0 else 1
        if far <= reach:
            @pl.when(there(hop) & there(back))
            def _():
                pl.semaphore_signal(ready.at[int(hop < 0), far], inc=1,
                                    device_id={"row": row + back}, device_id_type=MESH)

    def learn(hop):
        @pl.when(there(hop))
        def _():
            pl.semaphore_wait(ready.at[int(hop < 0), abs(hop)], 1)

    tell(1)
    tell(-1)

    def spectrum(owner, w, send, to):
        return pltpu.make_async_remote_copy(
            n_buf.at[owner, w], n_buf.at[owner, w], send.at[owner, w], n_recv.at[owner, w],
            device_id={"row": to}, device_id_type=MESH)

    def flag(owner, send, to):
        return pltpu.make_async_remote_copy(
            nf_buf.at[owner], nf_buf.at[owner], send.at[owner], nf_recv.at[owner],
            device_id={"row": to}, device_id_type=MESH)

    def z_copy(owner, w, to):
        return pltpu.make_async_remote_copy(
            z_buf.at[owner, w], z_buf.at[owner, w], z_send.at[to, w], z_recv.at[owner, w],
            device_id={"col": to}, device_id_type=MESH)

    def zf_copy(owner, to):
        return pltpu.make_async_remote_copy(
            zf_buf.at[owner], zf_buf.at[owner], zf_send.at[to], zf_recv.at[owner],
            device_id={"col": to}, device_id_type=MESH)

    def own_copy(hop, w):
        side, far = int(hop < 0), abs(hop) - 1
        return pltpu.make_async_remote_copy(
            n_buf.at[row, w], n_buf.at[row, w], own_send.at[side, far, w], n_recv.at[row, w],
            device_id={"row": row + hop}, device_id_type=MESH)

    def own_flag(hop):
        side, far = int(hop < 0), abs(hop) - 1
        return pltpu.make_async_remote_copy(
            nf_buf.at[row], nf_buf.at[row], own_f_send.at[side, far], nf_recv.at[row],
            device_id={"row": row + hop}, device_id_type=MESH)

    pairs = C % 2 == 0
    first = (lax.rem(col, 2) == 0) if pairs else (col >= 0)

    def send_own(hop):
        @pl.when(there(hop))
        def _():
            own_flag(hop).start()
            for w in range(W):
                own_copy(hop, w).start()

    for hop in range(2, reach + 1):
        learn(-hop)
        tell(-hop)
    loads[2].wait()
    loads[0].wait()
    @pl.when(first)
    def _():
        for hop in range(reach, 0, -1):
            send_own(-hop)

    send_own(1)
    loads[3].wait()
    loads[1].wait()
    for step in range(1, C):
        zf_copy(col, lax.rem(col + step, C)).start()
    for w in range(W):
        for step in range(1, C):
            z_copy(col, w, lax.rem(col + step, C)).start()
    @pl.when(first)
    def _():
        for hop in range(1, reach + 1):
            @pl.when((row == hop) | ((row > hop) & (hop == reach)))
            def _():
                for w in range(W):
                    own_copy(-hop, w).wait_send()

        if pairs:
            pl.semaphore_signal(turn_sem, inc=1, device_id={"col": lax.rem(col + 1, C)}, device_id_type=MESH)

    @pl.when(jnp.logical_not(first))
    def _():
        send_own(-1)
        held = row == R - 1

        @pl.when(held)
        def _():
            pl.semaphore_wait(turn_sem, 1)

        for hop in range(reach, 1, -1):
            send_own(-hop)

        @pl.when(jnp.logical_not(held))
        def _():
            pl.semaphore_wait(turn_sem, 1)

    for hop in range(2, reach + 1):
        learn(hop)
        tell(hop)
        send_own(hop)
    for load in loads[4:]:
        load.wait()

    spot = lax.broadcasted_iota(jnp.int32, (bin_rows, LANES), 0) + lax.broadcasted_iota(
        jnp.int32, (bin_rows, LANES), 1)
    weight = jnp.where(spot == 0, 1.0, 2.0).astype(jnp.float32)

    def unit(owner):
        pairs = [(i, w) for i in range(C) for w in range(W)]
        n_real = [n_buf[owner, w, pl.ds(0, bin_rows, stride=2), :] * weight for w in range(W)]
        n_imag = [n_buf[owner, w, pl.ds(1, bin_rows, stride=2), :] * weight for w in range(W)]
        cross = []
        for i, w in pairs:
            z_real = z_buf[i, w, pl.ds(0, bin_rows, stride=2), :]
            z_imag = z_buf[i, w, pl.ds(1, bin_rows, stride=2), :]
            cross.append(jnp.concatenate(
                [z_real * n_real[w] + z_imag * n_imag[w], z_imag * n_real[w] - z_real * n_imag[w]], 0
            ).astype(jnp.bfloat16))
        short = jnp.dot(inner[...], jnp.concatenate(cross, 1), preferred_element_type=jnp.float32)
        turned = []
        for at in range(len(pairs)):
            real = short[:period, at * LANES:(at + 1) * LANES]
            imag = short[period:, at * LANES:(at + 1) * LANES]
            for part in range(LANES // period):
                cosine = turn[0, part * period:(part + 1) * period, :]
                sine = turn[1, part * period:(part + 1) * period, :]
                turned.append(jnp.concatenate(
                    [real * cosine - imag * sine, real * sine + imag * cosine], 1).astype(jnp.bfloat16))
        lags = lax.dot_general(outer[...], jnp.concatenate(turned, 0), (((1,), (1,)), ((), ())),
                               preferred_element_type=jnp.float32)
        lags = lags[:blocks] + lags[blocks:]
        n_flag = nf_buf[owner].astype(jnp.float32)
        mask = mask_buf[...].astype(jnp.float32)
        here = lax.broadcasted_iota(jnp.int32, mask.shape, 1) == owner
        kept = jnp.sum(jnp.where(here, mask, 0.0), axis=1, keepdims=True)
        for i in range(C):
            marks = zf_buf[i].astype(jnp.float32) * n_flag
            count = jnp.maximum(jnp.sum(marks, axis=1, keepdims=True), 1.0)
            gain = marks * kept[i:i + 1] / count
            total = jnp.zeros((blocks, LANES), jnp.float32)
            for w in range(W):
                at = i * W + w
                corr = lags[:, at * LANES:(at + 1) * LANES]
                power = jnp.sum(jnp.sum(corr * corr, axis=0, keepdims=True), axis=1, keepdims=True)
                spread = jnp.sqrt(power / LAGS + 1e-05)
                total = total + corr * (gain[:, w:w + 1] / spread)
            out_ref[pl.ds(i * blocks * R + owner, blocks, stride=R), :] = total

    def arrive(owner, w, forward, send, f_send, to):
        if w == 0:
            flag(owner, f_send, to).wait_recv()
        spectrum(owner, w, send, to).wait_recv()
        if forward is False:
            return

        @pl.when(forward)
        def _():
            if w == 0:
                flag(owner, f_send, to).start()
            spectrum(owner, w, send, to).start()

    for step in range(1, C):
        zf_copy(lax.rem(col + C - step, C), lax.rem(col + step, C)).wait_recv()
    for w in range(W):
        for step in range(1, C):
            z_copy(lax.rem(col + C - step, C), w, lax.rem(col + step, C)).wait_recv()
    unit(row)

    def take(p):
        left = p <= row
        owner = jnp.where(left, row - p, p)
        if reach == R - 1:
            for w in range(W):
                arrive(owner, w, False, right_send, rf_send, lax.rem(row + 1, R))
        else:
            @pl.when(left)
            def _():
                for w in range(W):
                    arrive(owner, w, has_right & (p >= reach), right_send, rf_send, lax.rem(row + 1, R))

            @pl.when(p > row)
            def _():
                for w in range(W):
                    arrive(owner, w, has_left & (p - row >= reach), left_send, lf_send,
                           lax.rem(row + R - 1, R))
        unit(owner)

    if R <= 4:
        for p in range(1, R):
            take(p)
    else:
        pl.loop(1, R)(take)

    hops = [sign * hop for hop in range(1, reach + 1) for sign in (1, -1)]
    for hop in hops:
        @pl.when(there(hop))
        def _():
            own_flag(hop).wait_send()
            if hop > 0:
                for w in range(W):
                    own_copy(hop, w).wait_send()
            else:
                waited = first & ((row == -hop) | ((row > -hop) & (-hop == reach)))

                @pl.when(jnp.logical_not(waited))
                def _():
                    for w in range(W):
                        own_copy(hop, w).wait_send()

    for step in range(1, C):
        zf_copy(col, lax.rem(col + step, C)).wait_send()
        for w in range(W):
            z_copy(col, w, lax.rem(col + step, C)).wait_send()

    if reach == R - 1:
        return

    @pl.loop(0, R)
    def _(owner):
        @pl.when(has_right & (owner <= row - reach))
        def _():
            flag(owner, rf_send, lax.rem(row + 1, R)).wait_send()
            for w in range(W):
                spectrum(owner, w, right_send, lax.rem(row + 1, R)).wait_send()

        @pl.when(has_left & (owner >= row + reach))
        def _():
            flag(owner, lf_send, lax.rem(row + R - 1, R)).wait_send()
            for w in range(W):
                spectrum(owner, w, left_send, lax.rem(row + R - 1, R)).wait_send()


def far_body(R, C, z_spectra, n_spectra, z_flags, n_flags, pair_mask):
    windows, bins = z_spectra.shape[1], z_spectra.shape[3]
    rows, blocks = bins // LANES, LAGS // LANES
    inner, turn, outer = far_tables(bins)

    def interleave(x):
        return x.reshape(1, windows, 2, rows, LANES).transpose(0, 1, 3, 2, 4).reshape(
            1, windows, 2 * rows, LANES)

    reach = min(REACH, R - 1)
    DMA = pltpu.SemaphoreType.DMA
    out = pl.pallas_call(
        functools.partial(far_kernel, R, C, reach),
        out_shape=pltpu.VMEM((C * blocks * R, LANES), jnp.float32),
        in_specs=[pl.BlockSpec(memory_space=pl.ANY)] * 8,
        out_specs=pl.BlockSpec(memory_space=pltpu.VMEM),
        scratch_shapes=[
            pltpu.VMEM((C, windows, 2 * rows, LANES), jnp.float32),
            pltpu.VMEM((R, windows, 2 * rows, LANES), jnp.float32),
            pltpu.VMEM((C, 1, windows), jnp.int32),
            pltpu.VMEM((R, 1, windows), jnp.int32),
            pltpu.VMEM(pair_mask.shape, jnp.int32),
            pltpu.VMEM(inner.shape, jnp.bfloat16),
            pltpu.VMEM(turn.shape, jnp.float32),
            pltpu.VMEM(outer.shape, jnp.bfloat16),
            DMA((8,)),
            DMA((C, windows)), DMA((C, windows)), DMA((C,)), DMA((C,)),
            DMA((R, windows)), DMA((R, windows)), DMA((R, windows)),
            DMA((R,)), DMA((R,)), DMA((R,)),
            DMA((2, reach, windows)), DMA((2, reach)), pltpu.SemaphoreType.REGULAR((2, reach + 1)),
            pltpu.SemaphoreType.REGULAR,
        ],
        compiler_params=pltpu.CompilerParams(collective_id=0, has_side_effects=True),
        name="correlate",
    )(interleave(z_spectra), interleave(n_spectra), z_flags, n_flags, pair_mask,
      jnp.asarray(inner), jnp.asarray(turn), jnp.asarray(outer))
    return out.reshape(C, blocks, R, LANES).transpose(0, 2, 1, 3).reshape(C, R, LAGS)


def solution(mesh):
    placed = (
        P(("grp", "row", "col"), None, None, None),
        P(("grp", "col", "row"), None, None, None),
        P(("grp", "row", "col"), None),
        P(("grp", "col", "row"), None),
        P(("grp", "row"), "col"),
    )
    return jax.shard_map(
        functools.partial(body, mesh.shape["row"], mesh.shape["col"]), mesh=mesh,
        in_specs=placed, out_specs=P(("grp", "row"), "col", None), check_vma=False,
    )
```

```python
import functools
import math

import jax
import jax.numpy as jnp
import numpy as np
from jax import lax
from jax.experimental import pallas as pl
from jax.experimental.pallas import tpu as pltpu
from jax.sharding import PartitionSpec as P

LAGS = 512
LANES = 128
MESH = pl.DeviceIdType.MESH
REACH = 3
SENDS = (
    ((0, 1, (3,)), (0, 3, (5,)), (2, 1, (8, -1))),
    ((0, 1, (3,)), (0, 3, (5,)), (2, 1, (7, -1))),
    ((1, 0, (0,)), (1, 2, (3,)), (0, 2, (6,))),
    ((1, 0, (0,)), (1, 2, (3,)), (2, 0, (-1, 6)), (0, 2, (6,))),
    ((2, 0, (0,)), (2, 1, (-1, 2)), (2, 3, (3,)), (1, 3, (6,))),
    ((2, 1, (-1, 0)), (2, 0, (0, -1)), (2, 3, (3,)), (3, 1, (6,)), (1, 3, (6,))),
    ((3, 0, (0,)), (3, 2, (2,)), (3, 1, (2,))),
    ((3, 2, (1,)), (3, 0, (2,))),
)
TAKES = ((1, 2, 3), (1, 2, 3), (0, 2, 3), (0, 2, 3), (1, 3, 0), (1, 3, 0), (2, 0, 1), (2, 0, 1))


def tables(bins):
    rows = bins // LANES
    period = 2 * rows
    blocks, split = LAGS // period, LANES // period
    kt, short, lane = np.arange(rows), np.arange(period), np.arange(LANES)
    phi = 2 * np.pi * ((short[:, None] * kt[None, :]) % period) / period
    inner = np.block([[np.cos(phi), -np.sin(phi)], [np.sin(phi), np.cos(phi)]])
    psi = np.pi * (short[:, None] * lane[None, :]) / bins
    hop = np.arange(blocks).reshape(-1, split).T.reshape(-1) - blocks // 2
    chi = np.pi * ((period * hop[:, None] * lane[None, :]) % (2 * bins)) / bins
    outer = np.stack([np.cos(chi), -np.sin(chi)]).astype(np.float32)
    high = outer.astype(jnp.bfloat16).astype(np.float32)
    low = (outer - high).astype(jnp.bfloat16).astype(np.float32)
    wide = np.pad(inner, ((0, 0), (0, LANES - inner.shape[1])))
    parts = [wide, np.cos(psi), np.sin(psi), high[0], low[0], high[1], low[1]]
    return np.concatenate(parts, 0).astype(np.float32)


def kernel(R, C, z_hbm, n_hbm, zf_hbm, nf_hbm, mask_hbm, table_hbm, out_ref,
           held, flags, mask_buf, table, n_recv, z_recv, flag_recv, sent, row_ready, col_ready):
    row, col = lax.axis_index("row"), lax.axis_index("col")
    W = z_hbm.shape[1]
    bin_rows = held.shape[1] // 2
    period = 2 * bin_rows
    blocks = LAGS // period
    odd = lax.rem(col, 2) == 1
    partner = col + 1 - 2 * lax.rem(col, 2)
    place = 2 * row + lax.rem(col, 2)

    def wait_all(ref, count, sem):
        some = ref.at[pl.ds(0, count)]
        pltpu.make_async_copy(some, some, sem).wait()

    def n_slots(owner):
        return held.at[pl.ds(owner * W, W)]

    def z_slots(owner):
        return held.at[pl.ds((R + owner) * W, W)]

    n_load = pltpu.make_async_copy(n_hbm.at[0], n_slots(row), n_recv.at[row, 0])
    z_load = pltpu.make_async_copy(z_hbm.at[0], z_slots(col), z_recv.at[col])
    for w in range(W):
        for half in range(2):
            some = pl.ds(half * bin_rows, bin_rows)
            pltpu.make_async_copy(n_hbm.at[0, w, some], held.at[row * W + w, some], n_recv.at[row, 0]).start()

    pltpu.make_async_copy(nf_hbm, flags.at[row], sent.at[1]).start()
    pltpu.make_async_copy(zf_hbm, flags.at[R + col], sent.at[1]).start()
    z_load.start()

    def row_there(hop):
        return (row + hop < R) & (row + hop >= 0)

    barrier = pltpu.get_barrier_semaphore()
    for hop in range(1, R):
        @pl.when(row_there(hop))
        def _():
            pl.semaphore_signal(barrier, inc=1, device_id={"row": row + hop}, device_id_type=MESH)

    for step in range(1, C):
        @pl.when(col + step < C)
        def _():
            pl.semaphore_signal(barrier, inc=1, device_id={"col": col + step}, device_id_type=MESH)

    @pl.when(row + col > 0)
    def _():
        pl.semaphore_wait(barrier, row + col)

    for hop in range(1, R):
        @pl.when(row_there(-hop))
        def _():
            pl.semaphore_signal(row_ready.at[hop - 1], inc=1, device_id={"row": row - hop}, device_id_type=MESH)

    for step in range(1, C):
        @pl.when(col >= step)
        def _():
            pl.semaphore_signal(col_ready, inc=1, device_id={"col": col - step}, device_id_type=MESH)

    def spectrum(owner, w, to):
        return pltpu.make_async_remote_copy(
            held.at[owner * W + w], held.at[owner * W + w], sent.at[0], n_recv.at[owner, w],
            device_id={"row": to}, device_id_type=MESH)

    def z_copy(owner, to):
        return pltpu.make_async_remote_copy(
            z_slots(owner), z_slots(owner), sent.at[0], z_recv.at[owner],
            device_id={"col": to}, device_id_type=MESH)

    def flag(slot, **to):
        return pltpu.make_async_remote_copy(
            flags.at[slot], flags.at[slot], sent.at[1], flag_recv, device_id=to, device_id_type=MESH)

    def at(fn):
        for here in range(2 * R):
            @pl.when(place == here)
            def _():
                fn(here)

    def step_sends(number):
        def send(here):
            for owner, to, when in SENDS[here]:
                for w in range(W):
                    if when[w % len(when)] == number:
                        if owner != here // 2:
                            spectrum(owner, w, to).wait_recv()
                        spectrum(owner, w, to).start()
        if any(number in when for sends in SENDS for _, _, when in sends):
            at(send)

    wait_all(flags, 2, sent.at[1])
    for hop in range(1, R):
        @pl.when(row_there(-hop))
        def _():
            flag(row, row=row - hop).start()

    n_load.wait()
    mask_load = pltpu.make_async_copy(mask_hbm, mask_buf, n_recv.at[row, 0])
    mask_load.start()
    step_sends(0)

    def send_z(step, ahead):
        to = lax.rem(col + step, C)

        @pl.when((to > col) == ahead)
        def _():
            @pl.when(jnp.logical_not(odd) | (lax.rem(to, 2) == 1) | (to == partner))
            def _():
                z_copy(col, to).start()

            flag(R + col, col=to).start()

    z_load.wait()
    table_load = pltpu.make_async_copy(table_hbm, table, z_recv.at[col])
    table_load.start()
    for step in range(1, C):
        send_z(step, False)
    step_sends(1)

    @pl.when(col < C - 1)
    def _():
        pl.semaphore_wait(col_ready, C - 1 - col)

    for step in range(1, C):
        send_z(step, True)
    step_sends(2)
    for hop in range(1, R):
        @pl.when(row_there(hop))
        def _():
            pl.semaphore_wait(row_ready.at[hop - 1], 1)
            flag(row, row=row + hop).start()

        step_sends(2 + hop)

    step_sends(R + 2)

    @pl.when(odd)
    def _():
        for step in range(2, C, 2):
            owner = lax.rem(col + step, C)
            z_copy(owner, partner).wait_recv()
            z_copy(owner, partner).start()

    step_sends(R + 3)
    mask_load.wait()
    table_load.wait()
    spot = lax.broadcasted_iota(jnp.int32, (bin_rows, LANES), 0) + lax.broadcasted_iota(
        jnp.int32, (bin_rows, LANES), 1)
    weight = jnp.where(spot == 0, 1.0, 2.0).astype(jnp.float32)
    split = LANES // period
    lines = blocks // split
    groups = C // split
    lane_side = lax.broadcasted_iota(jnp.int32, (blocks, LANES), 1) // period
    line_side = lax.broadcasted_iota(jnp.int32, (blocks, LANES), 0) // lines

    def spread_out(rows):
        picked = jnp.zeros((blocks, LANES), jnp.float32) + rows[0]
        for h in range(1, split):
            picked = jnp.where(line_side == h, rows[h], picked)
        return picked

    def gains(owner):
        passed = flags[owner].astype(jnp.float32)
        mask = mask_buf[...].astype(jnp.float32)
        here = lax.broadcasted_iota(jnp.int32, mask.shape, 1) == owner
        kept = jnp.sum(jnp.where(here, mask, 0.0), axis=1, keepdims=True)
        each = []
        for i in range(C):
            marks = flags[R + i].astype(jnp.float32) * passed
            count = jnp.maximum(jnp.sum(marks, axis=1, keepdims=True), 1.0)
            each.append(marks * kept[i:i + 1] / count)
        return [[spread_out([each[g * split + h][:, w:w + 1] for h in range(split)]) for g in range(groups)]
                for w in range(W)]

    def correlate(owner):
        inner = table[:2 * period, :period].astype(jnp.bfloat16)
        turn = table[2 * period:3 * period, :], table[3 * period:4 * period, :]
        outer = jnp.concatenate([table[4 * period:4 * period + 2 * blocks, :], table[4 * period + 2 * blocks:, :]], 1)
        outer = outer.astype(jnp.bfloat16)
        cross = []
        for w in range(W):
            n_real = held[owner * W + w, pl.ds(0, bin_rows, stride=2), :] * weight
            n_imag = held[owner * W + w, pl.ds(1, bin_rows, stride=2), :] * weight
            for i in range(C):
                z_real = held[(R + i) * W + w, pl.ds(0, bin_rows, stride=2), :]
                z_imag = held[(R + i) * W + w, pl.ds(1, bin_rows, stride=2), :]
                cross.append(jnp.concatenate(
                    [z_real * n_real + z_imag * n_imag, z_imag * n_real - z_real * n_imag], 0
                ).astype(jnp.bfloat16))
        short = jnp.dot(inner, jnp.concatenate(cross, 1), preferred_element_type=jnp.float32)
        turned = []
        for at in range(W * C):
            real = short[:period, at * LANES:(at + 1) * LANES]
            imag = short[period:, at * LANES:(at + 1) * LANES]
            turned.append(jnp.concatenate(
                [real * turn[0] - imag * turn[1], real * turn[1] + imag * turn[0]], 1).astype(jnp.bfloat16))
        lags = lax.dot_general(outer, jnp.concatenate(turned, 0), (((1,), (1,)), ((), ())),
                               preferred_element_type=jnp.float32)
        lags = lags[:blocks] + lags[blocks:]
        return [[lags[:, (w * groups + g) * LANES:(w * groups + g + 1) * LANES] for g in range(groups)]
                for w in range(W)]

    def normal(corr):
        power = jnp.sum(corr * corr, axis=0, keepdims=True)
        whole = spread_out([jnp.sum(jnp.where(lane_side[:1] == h, power, 0.0), axis=1, keepdims=True)
                            for h in range(split)])
        laid = corr
        for by in range(1, split):
            moved = pltpu.roll(pltpu.roll(corr, by * period, 1), (split - by) * lines, 0)
            laid = jnp.where(lax.rem(lane_side - line_side + split, split) == by, moved, laid)
        return laid * lax.rsqrt(whole / LAGS + 1e-05)

    def finish(owner, units, gain):
        for g in range(groups):
            total = units[0][g] * gain[0][g]
            for w in range(1, W):
                total = total + units[w][g] * gain[w][g]
            for h in range(split):
                i = g * split + h
                out_ref[pl.ds(i * lines * R + owner, lines, stride=R), :] = total[h * lines:(h + 1) * lines]

    def pick(p):
        owner = row * 0
        for here in range(2 * R):
            owner = jnp.where(place == here, TAKES[here][p - 1], owner)
        return owner

    def receive(p):
        def take(here):
            owner = TAKES[here][p - 1]
            passed = [when for passed, _, when in SENDS[here] if passed == owner]
            for w in range(W):
                if all(when[w % len(when)] < 0 for when in passed):
                    spectrum(owner, w, here // 2).wait_recv()
        at(take)

    for step in range(1, C):
        owner = lax.rem(col + step, C)

        @pl.when(jnp.logical_not(odd & (lax.rem(owner, 2) == 1)))
        def _():
            z_copy(owner, col).wait_recv()

    owners = [row] + [pick(p) for p in range(1, R)]

    def run(*steps):
        done, gain = [], []
        for step in steps:
            if step == "send":
                step_sends(R + 4)
            elif step == "gain":
                wait_all(flags, R + C - 2, flag_recv)
                gain = [gains(owner) for owner in owners]
            else:
                for p in step:
                    if p > 0:
                        receive(p)
                corrs = [correlate(owners[p]) for p in step]
                done += [(p, [[normal(c) for c in part] for part in corr]) for p, corr in zip(step, corrs)]
            if gain:
                for p, units in done:
                    finish(owners[p], units, gain[p])
                done = []

    alone = jnp.logical_not(odd) & (row == 0)
    together = jnp.logical_not(odd) & (row == 1)

    @pl.when(alone)
    def _():
        run([0], "send", [1], [2], "gain", [3])

    @pl.when(together)
    def _():
        run([0, 1], "send", "gain", [2, 3])

    @pl.when(jnp.logical_not(alone | together))
    def _():
        run([0, 1], "send", "gain", [2], [3])

    def finish_sends(here):
        windows = sum(when[w % len(when)] >= 0 for _, _, when in SENDS[here] for w in range(W))
        wait_all(held, windows + (C - 1) * W, sent.at[0])

    at(finish_sends)
    wait_all(flags, R + C - 2, sent.at[1])


def body(R, C, z_spectra, n_spectra, z_flags, n_flags, pair_mask):
    windows, bins = z_spectra.shape[1], z_spectra.shape[3]
    rows = bins // LANES
    blocks, split = LAGS // (2 * rows), LANES // (2 * rows)
    if 2 * R != len(SENDS) or C % 2 or C % split:
        return far_body(R, C, z_spectra, n_spectra, z_flags, n_flags, pair_mask)
    table = jnp.asarray(tables(bins))

    def interleave(x):
        return x.reshape(1, windows, 2, rows, LANES).transpose(0, 1, 3, 2, 4).reshape(
            1, windows, 2 * rows, LANES)

    DMA, REGULAR = pltpu.SemaphoreType.DMA, pltpu.SemaphoreType.REGULAR
    lines = blocks // split
    out = pl.pallas_call(
        functools.partial(kernel, R, C),
        out_shape=pltpu.VMEM((C * lines * R, LANES), jnp.float32),
        in_specs=[pl.BlockSpec(memory_space=pl.ANY)] * 6,
        out_specs=pl.BlockSpec(memory_space=pltpu.VMEM),
        scratch_shapes=[
            pltpu.VMEM(((R + C) * windows, 2 * rows, LANES), jnp.float32),
            pltpu.VMEM((R + C, 1, windows), jnp.int32),
            pltpu.VMEM(pair_mask.shape, jnp.int32),
            pltpu.VMEM(table.shape, jnp.float32),
            DMA((R, windows)), DMA((C,)), DMA, DMA((2,)), REGULAR((R - 1,)), REGULAR,
        ],
        compiler_params=pltpu.CompilerParams(collective_id=0, has_side_effects=True),
        name="correlate",
    )(interleave(z_spectra), interleave(n_spectra), z_flags, n_flags, pair_mask, table)
    return out.reshape(C, lines, R, LANES).transpose(0, 2, 1, 3).reshape(C, R, LAGS)


def far_tables(bins):
    rows, blocks = bins // LANES, LAGS // LANES
    period = 2 * rows
    kt, short = np.arange(rows), np.arange(period)
    phi = 2 * np.pi * ((short[:, None] * kt[None, :]) % period) / period
    inner = np.block([[np.cos(phi), -np.sin(phi)], [np.sin(phi), np.cos(phi)]])
    lane, t0 = np.arange(LANES), np.arange(LANES)
    psi = np.pi * (t0[:, None] * lane[None, :]) / bins
    turn = np.stack([np.cos(psi), np.sin(psi)]).astype(np.float32)
    hop = np.arange(blocks) - blocks // 2
    chi = np.pi * ((LANES * hop[:, None] * lane[None, :]) % (2 * bins)) / bins
    outer = np.concatenate([np.cos(chi), -np.sin(chi)], 1).astype(np.float32)
    high = outer.astype(jnp.bfloat16)
    low = (outer - high.astype(np.float32)).astype(jnp.bfloat16)
    return inner.astype(jnp.bfloat16), turn, np.concatenate([high, low], 0)


def far_kernel(R, C, reach, z_hbm, n_hbm, zf_hbm, nf_hbm, mask_hbm, inner_hbm, turn_hbm, outer_hbm, out_ref,
           z_buf, n_buf, zf_buf, nf_buf, mask_buf, inner, turn, outer,
           load_sem, z_send, z_recv, zf_send, zf_recv, right_send, left_send, n_recv,
           rf_send, lf_send, nf_recv, own_send, own_f_send, ready, turn_sem):
    row, col = lax.axis_index("row"), lax.axis_index("col")
    W = z_buf.shape[1]
    bin_rows = z_buf.shape[2] // 2
    period = inner.shape[0] // 2
    blocks = outer.shape[0] // 2

    loads = [
        pltpu.make_async_copy(n_hbm.at[0], n_buf.at[row], load_sem.at[0]),
        pltpu.make_async_copy(z_hbm.at[0], z_buf.at[col], load_sem.at[1]),
        pltpu.make_async_copy(nf_hbm, nf_buf.at[row], load_sem.at[2]),
        pltpu.make_async_copy(zf_hbm, zf_buf.at[col], load_sem.at[3]),
        pltpu.make_async_copy(mask_hbm, mask_buf, load_sem.at[4]),
        pltpu.make_async_copy(inner_hbm, inner, load_sem.at[5]),
        pltpu.make_async_copy(turn_hbm, turn, load_sem.at[6]),
        pltpu.make_async_copy(outer_hbm, outer, load_sem.at[7]),
    ]
    for load in loads:
        load.start()

    has_left, has_right = row > 0, row < R - 1
    barrier = pltpu.get_barrier_semaphore()

    def there(hop):
        return (row + hop < R) if hop > 0 else (row + hop >= 0)

    for hop in (-1, 1):
        @pl.when(there(hop))
        def _():
            pl.semaphore_signal(barrier, inc=1, device_id={"row": row + hop}, device_id_type=MESH)

    for step in range(1, C):
        pl.semaphore_signal(barrier, inc=1, device_id={"col": lax.rem(col + step, C)}, device_id_type=MESH)
    pl.semaphore_wait(barrier, C - 1 + jnp.where(has_left, 1, 0) + jnp.where(has_right, 1, 0))

    def tell(hop):
        far = abs(hop) + 1
        back = -1 if hop > 0 else 1
        if far <= reach:
            @pl.when(there(hop) & there(back))
            def _():
                pl.semaphore_signal(ready.at[int(hop < 0), far], inc=1,
                                    device_id={"row": row + back}, device_id_type=MESH)

    def learn(hop):
        @pl.when(there(hop))
        def _():
            pl.semaphore_wait(ready.at[int(hop < 0), abs(hop)], 1)

    tell(1)
    tell(-1)

    def spectrum(owner, w, send, to):
        return pltpu.make_async_remote_copy(
            n_buf.at[owner, w], n_buf.at[owner, w], send.at[owner, w], n_recv.at[owner, w],
            device_id={"row": to}, device_id_type=MESH)

    def flag(owner, send, to):
        return pltpu.make_async_remote_copy(
            nf_buf.at[owner], nf_buf.at[owner], send.at[owner], nf_recv.at[owner],
            device_id={"row": to}, device_id_type=MESH)

    def z_copy(owner, w, to):
        return pltpu.make_async_remote_copy(
            z_buf.at[owner, w], z_buf.at[owner, w], z_send.at[to, w], z_recv.at[owner, w],
            device_id={"col": to}, device_id_type=MESH)

    def zf_copy(owner, to):
        return pltpu.make_async_remote_copy(
            zf_buf.at[owner], zf_buf.at[owner], zf_send.at[to], zf_recv.at[owner],
            device_id={"col": to}, device_id_type=MESH)

    def own_copy(hop, w):
        side, far = int(hop < 0), abs(hop) - 1
        return pltpu.make_async_remote_copy(
            n_buf.at[row, w], n_buf.at[row, w], own_send.at[side, far, w], n_recv.at[row, w],
            device_id={"row": row + hop}, device_id_type=MESH)

    def own_flag(hop):
        side, far = int(hop < 0), abs(hop) - 1
        return pltpu.make_async_remote_copy(
            nf_buf.at[row], nf_buf.at[row], own_f_send.at[side, far], nf_recv.at[row],
            device_id={"row": row + hop}, device_id_type=MESH)

    pairs = C % 2 == 0
    first = (lax.rem(col, 2) == 0) if pairs else (col >= 0)

    def send_own(hop):
        @pl.when(there(hop))
        def _():
            own_flag(hop).start()
            for w in range(W):
                own_copy(hop, w).start()

    for hop in range(2, reach + 1):
        learn(-hop)
        tell(-hop)
    loads[2].wait()
    loads[0].wait()
    @pl.when(first)
    def _():
        for hop in range(reach, 0, -1):
            send_own(-hop)

    send_own(1)
    loads[3].wait()
    loads[1].wait()
    for step in range(1, C):
        zf_copy(col, lax.rem(col + step, C)).start()
    for w in range(W):
        for step in range(1, C):
            z_copy(col, w, lax.rem(col + step, C)).start()
    @pl.when(first)
    def _():
        for hop in range(1, reach + 1):
            @pl.when((row == hop) | ((row > hop) & (hop == reach)))
            def _():
                for w in range(W):
                    own_copy(-hop, w).wait_send()

        if pairs:
            pl.semaphore_signal(turn_sem, inc=1, device_id={"col": lax.rem(col + 1, C)}, device_id_type=MESH)

    @pl.when(jnp.logical_not(first))
    def _():
        send_own(-1)
        held = row == R - 1

        @pl.when(held)
        def _():
            pl.semaphore_wait(turn_sem, 1)

        for hop in range(reach, 1, -1):
            send_own(-hop)

        @pl.when(jnp.logical_not(held))
        def _():
            pl.semaphore_wait(turn_sem, 1)

    for hop in range(2, reach + 1):
        learn(hop)
        tell(hop)
        send_own(hop)
    for load in loads[4:]:
        load.wait()

    spot = lax.broadcasted_iota(jnp.int32, (bin_rows, LANES), 0) + lax.broadcasted_iota(
        jnp.int32, (bin_rows, LANES), 1)
    weight = jnp.where(spot == 0, 1.0, 2.0).astype(jnp.float32)

    def unit(owner):
        pairs = [(i, w) for i in range(C) for w in range(W)]
        n_real = [n_buf[owner, w, pl.ds(0, bin_rows, stride=2), :] * weight for w in range(W)]
        n_imag = [n_buf[owner, w, pl.ds(1, bin_rows, stride=2), :] * weight for w in range(W)]
        cross = []
        for i, w in pairs:
            z_real = z_buf[i, w, pl.ds(0, bin_rows, stride=2), :]
            z_imag = z_buf[i, w, pl.ds(1, bin_rows, stride=2), :]
            cross.append(jnp.concatenate(
                [z_real * n_real[w] + z_imag * n_imag[w], z_imag * n_real[w] - z_real * n_imag[w]], 0
            ).astype(jnp.bfloat16))
        short = jnp.dot(inner[...], jnp.concatenate(cross, 1), preferred_element_type=jnp.float32)
        turned = []
        for at in range(len(pairs)):
            real = short[:period, at * LANES:(at + 1) * LANES]
            imag = short[period:, at * LANES:(at + 1) * LANES]
            for part in range(LANES // period):
                cosine = turn[0, part * period:(part + 1) * period, :]
                sine = turn[1, part * period:(part + 1) * period, :]
                turned.append(jnp.concatenate(
                    [real * cosine - imag * sine, real * sine + imag * cosine], 1).astype(jnp.bfloat16))
        lags = lax.dot_general(outer[...], jnp.concatenate(turned, 0), (((1,), (1,)), ((), ())),
                               preferred_element_type=jnp.float32)
        lags = lags[:blocks] + lags[blocks:]
        n_flag = nf_buf[owner].astype(jnp.float32)
        mask = mask_buf[...].astype(jnp.float32)
        here = lax.broadcasted_iota(jnp.int32, mask.shape, 1) == owner
        kept = jnp.sum(jnp.where(here, mask, 0.0), axis=1, keepdims=True)
        for i in range(C):
            marks = zf_buf[i].astype(jnp.float32) * n_flag
            count = jnp.maximum(jnp.sum(marks, axis=1, keepdims=True), 1.0)
            gain = marks * kept[i:i + 1] / count
            total = jnp.zeros((blocks, LANES), jnp.float32)
            for w in range(W):
                at = i * W + w
                corr = lags[:, at * LANES:(at + 1) * LANES]
                power = jnp.sum(jnp.sum(corr * corr, axis=0, keepdims=True), axis=1, keepdims=True)
                spread = jnp.sqrt(power / LAGS + 1e-05)
                total = total + corr * (gain[:, w:w + 1] / spread)
            out_ref[pl.ds(i * blocks * R + owner, blocks, stride=R), :] = total

    def arrive(owner, w, forward, send, f_send, to):
        if w == 0:
            flag(owner, f_send, to).wait_recv()
        spectrum(owner, w, send, to).wait_recv()
        if forward is False:
            return

        @pl.when(forward)
        def _():
            if w == 0:
                flag(owner, f_send, to).start()
            spectrum(owner, w, send, to).start()

    for step in range(1, C):
        zf_copy(lax.rem(col + C - step, C), lax.rem(col + step, C)).wait_recv()
    for w in range(W):
        for step in range(1, C):
            z_copy(lax.rem(col + C - step, C), w, lax.rem(col + step, C)).wait_recv()
    unit(row)

    def take(p):
        left = p <= row
        owner = jnp.where(left, row - p, p)
        if reach == R - 1:
            for w in range(W):
                arrive(owner, w, False, right_send, rf_send, lax.rem(row + 1, R))
        else:
            @pl.when(left)
            def _():
                for w in range(W):
                    arrive(owner, w, has_right & (p >= reach), right_send, rf_send, lax.rem(row + 1, R))

            @pl.when(p > row)
            def _():
                for w in range(W):
                    arrive(owner, w, has_left & (p - row >= reach), left_send, lf_send,
                           lax.rem(row + R - 1, R))
        unit(owner)

    if R <= 4:
        for p in range(1, R):
            take(p)
    else:
        pl.loop(1, R)(take)

    hops = [sign * hop for hop in range(1, reach + 1) for sign in (1, -1)]
    for hop in hops:
        @pl.when(there(hop))
        def _():
            own_flag(hop).wait_send()
            if hop > 0:
                for w in range(W):
                    own_copy(hop, w).wait_send()
            else:
                waited = first & ((row == -hop) | ((row > -hop) & (-hop == reach)))

                @pl.when(jnp.logical_not(waited))
                def _():
                    for w in range(W):
                        own_copy(hop, w).wait_send()

    for step in range(1, C):
        zf_copy(col, lax.rem(col + step, C)).wait_send()
        for w in range(W):
            z_copy(col, w, lax.rem(col + step, C)).wait_send()

    if reach == R - 1:
        return

    @pl.loop(0, R)
    def _(owner):
        @pl.when(has_right & (owner <= row - reach))
        def _():
            flag(owner, rf_send, lax.rem(row + 1, R)).wait_send()
            for w in range(W):
                spectrum(owner, w, right_send, lax.rem(row + 1, R)).wait_send()

        @pl.when(has_left & (owner >= row + reach))
        def _():
            flag(owner, lf_send, lax.rem(row + R - 1, R)).wait_send()
            for w in range(W):
                spectrum(owner, w, left_send, lax.rem(row + R - 1, R)).wait_send()


def far_body(R, C, z_spectra, n_spectra, z_flags, n_flags, pair_mask):
    windows, bins = z_spectra.shape[1], z_spectra.shape[3]
    rows, blocks = bins // LANES, LAGS // LANES
    inner, turn, outer = far_tables(bins)

    def interleave(x):
        return x.reshape(1, windows, 2, rows, LANES).transpose(0, 1, 3, 2, 4).reshape(
            1, windows, 2 * rows, LANES)

    reach = min(REACH, R - 1)
    DMA = pltpu.SemaphoreType.DMA
    out = pl.pallas_call(
        functools.partial(far_kernel, R, C, reach),
        out_shape=pltpu.VMEM((C * blocks * R, LANES), jnp.float32),
        in_specs=[pl.BlockSpec(memory_space=pl.ANY)] * 8,
        out_specs=pl.BlockSpec(memory_space=pltpu.VMEM),
        scratch_shapes=[
            pltpu.VMEM((C, windows, 2 * rows, LANES), jnp.float32),
            pltpu.VMEM((R, windows, 2 * rows, LANES), jnp.float32),
            pltpu.VMEM((C, 1, windows), jnp.int32),
            pltpu.VMEM((R, 1, windows), jnp.int32),
            pltpu.VMEM(pair_mask.shape, jnp.int32),
            pltpu.VMEM(inner.shape, jnp.bfloat16),
            pltpu.VMEM(turn.shape, jnp.float32),
            pltpu.VMEM(outer.shape, jnp.bfloat16),
            DMA((8,)),
            DMA((C, windows)), DMA((C, windows)), DMA((C,)), DMA((C,)),
            DMA((R, windows)), DMA((R, windows)), DMA((R, windows)),
            DMA((R,)), DMA((R,)), DMA((R,)),
            DMA((2, reach, windows)), DMA((2, reach)), pltpu.SemaphoreType.REGULAR((2, reach + 1)),
            pltpu.SemaphoreType.REGULAR,
        ],
        compiler_params=pltpu.CompilerParams(collective_id=0, has_side_effects=True),
        name="correlate",
    )(interleave(z_spectra), interleave(n_spectra), z_flags, n_flags, pair_mask,
      jnp.asarray(inner), jnp.asarray(turn), jnp.asarray(outer))
    return out.reshape(C, blocks, R, LANES).transpose(0, 2, 1, 3).reshape(C, R, LAGS)


def solution(mesh):
    placed = (
        P(("grp", "row", "col"), None, None, None),
        P(("grp", "col", "row"), None, None, None),
        P(("grp", "row", "col"), None),
        P(("grp", "col", "row"), None),
        P(("grp", "row"), "col"),
    )
    return jax.shard_map(
        functools.partial(body, mesh.shape["row"], mesh.shape["col"]), mesh=mesh,
        in_specs=placed, out_specs=P(("grp", "row"), "col", None), check_vma=False,
    )
```

```python
import functools
import math

import jax
import jax.numpy as jnp
import numpy as np
from jax import lax
from jax.experimental import pallas as pl
from jax.experimental.pallas import tpu as pltpu
from jax.sharding import PartitionSpec as P

LAGS = 512
LANES = 128
MESH = pl.DeviceIdType.MESH
REACH = 3
SENDS = (
    ((0, 1, (3,)), (0, 3, (5,)), (2, 1, (8, -1))),
    ((0, 1, (3,)), (0, 3, (5,)), (2, 1, (7, -1))),
    ((1, 0, (0,)), (1, 2, (3,)), (0, 2, (6,))),
    ((1, 0, (0,)), (1, 2, (3,)), (2, 0, (-1, 6)), (0, 2, (6,))),
    ((2, 0, (0,)), (2, 1, (-1, 2)), (2, 3, (3,)), (1, 3, (6,))),
    ((2, 1, (-1, 0)), (2, 0, (0, -1)), (2, 3, (3,)), (3, 1, (6,)), (1, 3, (6,))),
    ((3, 0, (0,)), (3, 1, (2,)), (3, 2, (2,))),
    ((3, 2, (1,)), (3, 0, (2,))),
)
TAKES = ((1, 2, 3), (1, 2, 3), (0, 2, 3), (0, 2, 3), (1, 3, 0), (1, 3, 0), (2, 0, 1), (2, 0, 1))


def tables(bins):
    rows = bins // LANES
    period = 2 * rows
    blocks, split = LAGS // period, LANES // period
    kt, short, lane = np.arange(rows), np.arange(period), np.arange(LANES)
    phi = 2 * np.pi * ((short[:, None] * kt[None, :]) % period) / period
    inner = np.block([[np.cos(phi), -np.sin(phi)], [np.sin(phi), np.cos(phi)]])
    psi = np.pi * (short[:, None] * lane[None, :]) / bins
    hop = np.arange(blocks).reshape(-1, split).T.reshape(-1) - blocks // 2
    chi = np.pi * ((period * hop[:, None] * lane[None, :]) % (2 * bins)) / bins
    outer = np.stack([np.cos(chi), -np.sin(chi)]).astype(np.float32)
    high = outer.astype(jnp.bfloat16).astype(np.float32)
    low = (outer - high).astype(jnp.bfloat16).astype(np.float32)
    wide = np.pad(inner, ((0, 0), (0, LANES - inner.shape[1])))
    parts = [wide, np.cos(psi), np.sin(psi), high[0], low[0], high[1], low[1]]
    return np.concatenate(parts, 0).astype(np.float32)


def kernel(R, C, z_hbm, n_hbm, zf_hbm, nf_hbm, mask_hbm, table_hbm, out_ref,
           held, flags, mask_buf, table, n_recv, z_recv, flag_recv, sent, row_ready, col_ready):
    row, col = lax.axis_index("row"), lax.axis_index("col")
    W = z_hbm.shape[1]
    bin_rows = held.shape[1] // 2
    period = 2 * bin_rows
    blocks = LAGS // period
    odd = lax.rem(col, 2) == 1
    partner = col + 1 - 2 * lax.rem(col, 2)
    place = 2 * row + lax.rem(col, 2)

    def wait_all(ref, count, sem):
        some = ref.at[pl.ds(0, count)]
        pltpu.make_async_copy(some, some, sem).wait()

    def n_slots(owner):
        return held.at[pl.ds(owner * W, W)]

    def z_slots(owner):
        return held.at[pl.ds((R + owner) * W, W)]

    n_load = pltpu.make_async_copy(n_hbm.at[0], n_slots(row), n_recv.at[row, 0])
    z_load = pltpu.make_async_copy(z_hbm.at[0], z_slots(col), z_recv.at[col])
    for w in range(W):
        for half in range(2):
            some = pl.ds(half * bin_rows, bin_rows)
            pltpu.make_async_copy(n_hbm.at[0, w, some], held.at[row * W + w, some], n_recv.at[row, 0]).start()

    pltpu.make_async_copy(nf_hbm, flags.at[row], sent.at[1]).start()
    pltpu.make_async_copy(zf_hbm, flags.at[R + col], sent.at[1]).start()
    z_load.start()

    def row_there(hop):
        return (row + hop < R) & (row + hop >= 0)

    barrier = pltpu.get_barrier_semaphore()
    for hop in range(1, R):
        @pl.when(row_there(hop))
        def _():
            pl.semaphore_signal(barrier, inc=1, device_id={"row": row + hop}, device_id_type=MESH)

    for step in range(1, C):
        @pl.when(col + step < C)
        def _():
            pl.semaphore_signal(barrier, inc=1, device_id={"col": col + step}, device_id_type=MESH)

    @pl.when(row + col > 0)
    def _():
        pl.semaphore_wait(barrier, row + col)

    for hop in range(1, R):
        @pl.when(row_there(-hop))
        def _():
            pl.semaphore_signal(row_ready.at[hop - 1], inc=1, device_id={"row": row - hop}, device_id_type=MESH)

    for step in range(1, C):
        @pl.when(col >= step)
        def _():
            pl.semaphore_signal(col_ready, inc=1, device_id={"col": col - step}, device_id_type=MESH)

    def spectrum(owner, w, to):
        return pltpu.make_async_remote_copy(
            held.at[owner * W + w], held.at[owner * W + w], sent.at[0], n_recv.at[owner, w],
            device_id={"row": to}, device_id_type=MESH)

    def z_copy(owner, to):
        return pltpu.make_async_remote_copy(
            z_slots(owner), z_slots(owner), sent.at[0], z_recv.at[owner],
            device_id={"col": to}, device_id_type=MESH)

    def flag(slot, **to):
        return pltpu.make_async_remote_copy(
            flags.at[slot], flags.at[slot], sent.at[1], flag_recv, device_id=to, device_id_type=MESH)

    def at(fn):
        for here in range(2 * R):
            @pl.when(place == here)
            def _():
                fn(here)

    def step_sends(number):
        def send(here):
            for owner, to, when in SENDS[here]:
                for w in range(W):
                    if when[w % len(when)] == number:
                        if owner != here // 2:
                            spectrum(owner, w, to).wait_recv()
                        spectrum(owner, w, to).start()
        if any(number in when for sends in SENDS for _, _, when in sends):
            at(send)

    wait_all(flags, 2, sent.at[1])
    for hop in range(1, R):
        @pl.when(row_there(-hop))
        def _():
            flag(row, row=row - hop).start()

    n_load.wait()
    mask_load = pltpu.make_async_copy(mask_hbm, mask_buf, n_recv.at[row, 0])
    mask_load.start()
    step_sends(0)

    def send_z(step, ahead):
        to = lax.rem(col + step, C)

        @pl.when((to > col) == ahead)
        def _():
            @pl.when(jnp.logical_not(odd) | (lax.rem(to, 2) == 1) | (to == partner))
            def _():
                z_copy(col, to).start()

            flag(R + col, col=to).start()

    z_load.wait()
    table_load = pltpu.make_async_copy(table_hbm, table, z_recv.at[col])
    table_load.start()
    for step in range(1, C):
        send_z(step, False)
    step_sends(1)

    @pl.when(col < C - 1)
    def _():
        pl.semaphore_wait(col_ready, C - 1 - col)

    for step in range(1, C):
        send_z(step, True)
    step_sends(2)
    for hop in range(1, R):
        @pl.when(row_there(hop))
        def _():
            pl.semaphore_wait(row_ready.at[hop - 1], 1)
            flag(row, row=row + hop).start()

        step_sends(2 + hop)

    step_sends(R + 2)

    @pl.when(odd)
    def _():
        for step in range(2, C, 2):
            owner = lax.rem(col + step, C)
            z_copy(owner, partner).wait_recv()
            z_copy(owner, partner).start()

    step_sends(R + 3)
    mask_load.wait()
    table_load.wait()
    spot = lax.broadcasted_iota(jnp.int32, (bin_rows, LANES), 0) + lax.broadcasted_iota(
        jnp.int32, (bin_rows, LANES), 1)
    weight = jnp.where(spot == 0, 1.0, 2.0).astype(jnp.float32)
    split = LANES // period
    lines = blocks // split
    groups = C // split
    lane_side = lax.broadcasted_iota(jnp.int32, (blocks, LANES), 1) // period
    line_side = lax.broadcasted_iota(jnp.int32, (blocks, LANES), 0) // lines

    def spread_out(rows):
        picked = jnp.zeros((blocks, LANES), jnp.float32) + rows[0]
        for h in range(1, split):
            picked = jnp.where(line_side == h, rows[h], picked)
        return picked

    def gains(owner):
        passed = flags[owner].astype(jnp.float32)
        mask = mask_buf[...].astype(jnp.float32)
        here = lax.broadcasted_iota(jnp.int32, mask.shape, 1) == owner
        kept = jnp.sum(jnp.where(here, mask, 0.0), axis=1, keepdims=True)
        each = []
        for i in range(C):
            marks = flags[R + i].astype(jnp.float32) * passed
            count = jnp.maximum(jnp.sum(marks, axis=1, keepdims=True), 1.0)
            each.append(marks * kept[i:i + 1] / count)
        return [[spread_out([each[g * split + h][:, w:w + 1] for h in range(split)]) for g in range(groups)]
                for w in range(W)]

    def correlate(owner):
        inner = table[:2 * period, :period].astype(jnp.bfloat16)
        turn = table[2 * period:3 * period, :], table[3 * period:4 * period, :]
        outer = jnp.concatenate([table[4 * period:4 * period + 2 * blocks, :], table[4 * period + 2 * blocks:, :]], 1)
        outer = outer.astype(jnp.bfloat16)
        cross = []
        for w in range(W):
            n_real = held[owner * W + w, pl.ds(0, bin_rows, stride=2), :] * weight
            n_imag = held[owner * W + w, pl.ds(1, bin_rows, stride=2), :] * weight
            for i in range(C):
                z_real = held[(R + i) * W + w, pl.ds(0, bin_rows, stride=2), :]
                z_imag = held[(R + i) * W + w, pl.ds(1, bin_rows, stride=2), :]
                cross.append(jnp.concatenate(
                    [z_real * n_real + z_imag * n_imag, z_imag * n_real - z_real * n_imag], 0
                ).astype(jnp.bfloat16))
        short = jnp.dot(inner, jnp.concatenate(cross, 1), preferred_element_type=jnp.float32)
        turned = []
        for at in range(W * C):
            real = short[:period, at * LANES:(at + 1) * LANES]
            imag = short[period:, at * LANES:(at + 1) * LANES]
            turned.append(jnp.concatenate(
                [real * turn[0] - imag * turn[1], real * turn[1] + imag * turn[0]], 1).astype(jnp.bfloat16))
        lags = lax.dot_general(outer, jnp.concatenate(turned, 0), (((1,), (1,)), ((), ())),
                               preferred_element_type=jnp.float32)
        lags = lags[:blocks] + lags[blocks:]
        return [[lags[:, (w * groups + g) * LANES:(w * groups + g + 1) * LANES] for g in range(groups)]
                for w in range(W)]

    def normal(corr):
        power = jnp.sum(corr * corr, axis=0, keepdims=True)
        whole = spread_out([jnp.sum(jnp.where(lane_side[:1] == h, power, 0.0), axis=1, keepdims=True)
                            for h in range(split)])
        laid = corr
        for by in range(1, split):
            moved = pltpu.roll(pltpu.roll(corr, by * period, 1), (split - by) * lines, 0)
            laid = jnp.where(lax.rem(lane_side - line_side + split, split) == by, moved, laid)
        return laid * lax.rsqrt(whole / LAGS + 1e-05)

    def finish(owner, units, gain):
        for g in range(groups):
            total = units[0][g] * gain[0][g]
            for w in range(1, W):
                total = total + units[w][g] * gain[w][g]
            for h in range(split):
                i = g * split + h
                out_ref[pl.ds(i * lines * R + owner, lines, stride=R), :] = total[h * lines:(h + 1) * lines]

    def pick(p):
        owner = row * 0
        for here in range(2 * R):
            owner = jnp.where(place == here, TAKES[here][p - 1], owner)
        return owner

    def receive(p):
        def take(here):
            owner = TAKES[here][p - 1]
            passed = [when for passed, _, when in SENDS[here] if passed == owner]
            for w in range(W):
                if all(when[w % len(when)] < 0 for when in passed):
                    spectrum(owner, w, here // 2).wait_recv()
        at(take)

    for step in range(1, C):
        owner = lax.rem(col + step, C)

        @pl.when(jnp.logical_not(odd & (lax.rem(owner, 2) == 1)))
        def _():
            z_copy(owner, col).wait_recv()

    owners = [row] + [pick(p) for p in range(1, R)]

    def run(*steps):
        done, gain = [], []
        for step in steps:
            if step == "send":
                step_sends(R + 4)
            elif step == "gain":
                wait_all(flags, R + C - 2, flag_recv)
                gain = [gains(owner) for owner in owners]
            else:
                for p in step:
                    if p > 0:
                        receive(p)
                corrs = [correlate(owners[p]) for p in step]
                done += [(p, [[normal(c) for c in part] for part in corr]) for p, corr in zip(step, corrs)]
            if gain:
                for p, units in done:
                    finish(owners[p], units, gain[p])
                done = []

    alone = jnp.logical_not(odd) & (row == 0)
    together = jnp.logical_not(odd) & (row == 1)

    @pl.when(alone)
    def _():
        run([0], "send", [1], [2], "gain", [3])

    @pl.when(together)
    def _():
        run([0, 1], "send", "gain", [2, 3])

    @pl.when(jnp.logical_not(alone | together))
    def _():
        run([0, 1], "send", "gain", [2], [3])

    def finish_sends(here):
        windows = sum(when[w % len(when)] >= 0 for _, _, when in SENDS[here] for w in range(W))
        wait_all(held, windows + (C - 1) * W, sent.at[0])

    at(finish_sends)
    wait_all(flags, R + C - 2, sent.at[1])


def body(R, C, z_spectra, n_spectra, z_flags, n_flags, pair_mask):
    windows, bins = z_spectra.shape[1], z_spectra.shape[3]
    rows = bins // LANES
    blocks, split = LAGS // (2 * rows), LANES // (2 * rows)
    if 2 * R != len(SENDS) or C % 2 or C % split:
        return far_body(R, C, z_spectra, n_spectra, z_flags, n_flags, pair_mask)
    table = jnp.asarray(tables(bins))

    def interleave(x):
        return x.reshape(1, windows, 2, rows, LANES).transpose(0, 1, 3, 2, 4).reshape(
            1, windows, 2 * rows, LANES)

    DMA, REGULAR = pltpu.SemaphoreType.DMA, pltpu.SemaphoreType.REGULAR
    lines = blocks // split
    out = pl.pallas_call(
        functools.partial(kernel, R, C),
        out_shape=pltpu.VMEM((C * lines * R, LANES), jnp.float32),
        in_specs=[pl.BlockSpec(memory_space=pl.ANY)] * 6,
        out_specs=pl.BlockSpec(memory_space=pltpu.VMEM),
        scratch_shapes=[
            pltpu.VMEM(((R + C) * windows, 2 * rows, LANES), jnp.float32),
            pltpu.VMEM((R + C, 1, windows), jnp.int32),
            pltpu.VMEM(pair_mask.shape, jnp.int32),
            pltpu.VMEM(table.shape, jnp.float32),
            DMA((R, windows)), DMA((C,)), DMA, DMA((2,)), REGULAR((R - 1,)), REGULAR,
        ],
        compiler_params=pltpu.CompilerParams(collective_id=0, has_side_effects=True),
        name="correlate",
    )(interleave(z_spectra), interleave(n_spectra), z_flags, n_flags, pair_mask, table)
    return out.reshape(C, lines, R, LANES).transpose(0, 2, 1, 3).reshape(C, R, LAGS)


def far_tables(bins):
    rows, blocks = bins // LANES, LAGS // LANES
    period = 2 * rows
    kt, short = np.arange(rows), np.arange(period)
    phi = 2 * np.pi * ((short[:, None] * kt[None, :]) % period) / period
    inner = np.block([[np.cos(phi), -np.sin(phi)], [np.sin(phi), np.cos(phi)]])
    lane, t0 = np.arange(LANES), np.arange(LANES)
    psi = np.pi * (t0[:, None] * lane[None, :]) / bins
    turn = np.stack([np.cos(psi), np.sin(psi)]).astype(np.float32)
    hop = np.arange(blocks) - blocks // 2
    chi = np.pi * ((LANES * hop[:, None] * lane[None, :]) % (2 * bins)) / bins
    outer = np.concatenate([np.cos(chi), -np.sin(chi)], 1).astype(np.float32)
    high = outer.astype(jnp.bfloat16)
    low = (outer - high.astype(np.float32)).astype(jnp.bfloat16)
    return inner.astype(jnp.bfloat16), turn, np.concatenate([high, low], 0)


def far_kernel(R, C, reach, z_hbm, n_hbm, zf_hbm, nf_hbm, mask_hbm, inner_hbm, turn_hbm, outer_hbm, out_ref,
           z_buf, n_buf, zf_buf, nf_buf, mask_buf, inner, turn, outer,
           load_sem, z_send, z_recv, zf_send, zf_recv, right_send, left_send, n_recv,
           rf_send, lf_send, nf_recv, own_send, own_f_send, ready, turn_sem):
    row, col = lax.axis_index("row"), lax.axis_index("col")
    W = z_buf.shape[1]
    bin_rows = z_buf.shape[2] // 2
    period = inner.shape[0] // 2
    blocks = outer.shape[0] // 2

    loads = [
        pltpu.make_async_copy(n_hbm.at[0], n_buf.at[row], load_sem.at[0]),
        pltpu.make_async_copy(z_hbm.at[0], z_buf.at[col], load_sem.at[1]),
        pltpu.make_async_copy(nf_hbm, nf_buf.at[row], load_sem.at[2]),
        pltpu.make_async_copy(zf_hbm, zf_buf.at[col], load_sem.at[3]),
        pltpu.make_async_copy(mask_hbm, mask_buf, load_sem.at[4]),
        pltpu.make_async_copy(inner_hbm, inner, load_sem.at[5]),
        pltpu.make_async_copy(turn_hbm, turn, load_sem.at[6]),
        pltpu.make_async_copy(outer_hbm, outer, load_sem.at[7]),
    ]
    for load in loads:
        load.start()

    has_left, has_right = row > 0, row < R - 1
    barrier = pltpu.get_barrier_semaphore()

    def there(hop):
        return (row + hop < R) if hop > 0 else (row + hop >= 0)

    for hop in (-1, 1):
        @pl.when(there(hop))
        def _():
            pl.semaphore_signal(barrier, inc=1, device_id={"row": row + hop}, device_id_type=MESH)

    for step in range(1, C):
        pl.semaphore_signal(barrier, inc=1, device_id={"col": lax.rem(col + step, C)}, device_id_type=MESH)
    pl.semaphore_wait(barrier, C - 1 + jnp.where(has_left, 1, 0) + jnp.where(has_right, 1, 0))

    def tell(hop):
        far = abs(hop) + 1
        back = -1 if hop > 0 else 1
        if far <= reach:
            @pl.when(there(hop) & there(back))
            def _():
                pl.semaphore_signal(ready.at[int(hop < 0), far], inc=1,
                                    device_id={"row": row + back}, device_id_type=MESH)

    def learn(hop):
        @pl.when(there(hop))
        def _():
            pl.semaphore_wait(ready.at[int(hop < 0), abs(hop)], 1)

    tell(1)
    tell(-1)

    def spectrum(owner, w, send, to):
        return pltpu.make_async_remote_copy(
            n_buf.at[owner, w], n_buf.at[owner, w], send.at[owner, w], n_recv.at[owner, w],
            device_id={"row": to}, device_id_type=MESH)

    def flag(owner, send, to):
        return pltpu.make_async_remote_copy(
            nf_buf.at[owner], nf_buf.at[owner], send.at[owner], nf_recv.at[owner],
            device_id={"row": to}, device_id_type=MESH)

    def z_copy(owner, w, to):
        return pltpu.make_async_remote_copy(
            z_buf.at[owner, w], z_buf.at[owner, w], z_send.at[to, w], z_recv.at[owner, w],
            device_id={"col": to}, device_id_type=MESH)

    def zf_copy(owner, to):
        return pltpu.make_async_remote_copy(
            zf_buf.at[owner], zf_buf.at[owner], zf_send.at[to], zf_recv.at[owner],
            device_id={"col": to}, device_id_type=MESH)

    def own_copy(hop, w):
        side, far = int(hop < 0), abs(hop) - 1
        return pltpu.make_async_remote_copy(
            n_buf.at[row, w], n_buf.at[row, w], own_send.at[side, far, w], n_recv.at[row, w],
            device_id={"row": row + hop}, device_id_type=MESH)

    def own_flag(hop):
        side, far = int(hop < 0), abs(hop) - 1
        return pltpu.make_async_remote_copy(
            nf_buf.at[row], nf_buf.at[row], own_f_send.at[side, far], nf_recv.at[row],
            device_id={"row": row + hop}, device_id_type=MESH)

    pairs = C % 2 == 0
    first = (lax.rem(col, 2) == 0) if pairs else (col >= 0)

    def send_own(hop):
        @pl.when(there(hop))
        def _():
            own_flag(hop).start()
            for w in range(W):
                own_copy(hop, w).start()

    for hop in range(2, reach + 1):
        learn(-hop)
        tell(-hop)
    loads[2].wait()
    loads[0].wait()
    @pl.when(first)
    def _():
        for hop in range(reach, 0, -1):
            send_own(-hop)

    send_own(1)
    loads[3].wait()
    loads[1].wait()
    for step in range(1, C):
        zf_copy(col, lax.rem(col + step, C)).start()
    for w in range(W):
        for step in range(1, C):
            z_copy(col, w, lax.rem(col + step, C)).start()
    @pl.when(first)
    def _():
        for hop in range(1, reach + 1):
            @pl.when((row == hop) | ((row > hop) & (hop == reach)))
            def _():
                for w in range(W):
                    own_copy(-hop, w).wait_send()

        if pairs:
            pl.semaphore_signal(turn_sem, inc=1, device_id={"col": lax.rem(col + 1, C)}, device_id_type=MESH)

    @pl.when(jnp.logical_not(first))
    def _():
        send_own(-1)
        held = row == R - 1

        @pl.when(held)
        def _():
            pl.semaphore_wait(turn_sem, 1)

        for hop in range(reach, 1, -1):
            send_own(-hop)

        @pl.when(jnp.logical_not(held))
        def _():
            pl.semaphore_wait(turn_sem, 1)

    for hop in range(2, reach + 1):
        learn(hop)
        tell(hop)
        send_own(hop)
    for load in loads[4:]:
        load.wait()

    spot = lax.broadcasted_iota(jnp.int32, (bin_rows, LANES), 0) + lax.broadcasted_iota(
        jnp.int32, (bin_rows, LANES), 1)
    weight = jnp.where(spot == 0, 1.0, 2.0).astype(jnp.float32)

    def unit(owner):
        pairs = [(i, w) for i in range(C) for w in range(W)]
        n_real = [n_buf[owner, w, pl.ds(0, bin_rows, stride=2), :] * weight for w in range(W)]
        n_imag = [n_buf[owner, w, pl.ds(1, bin_rows, stride=2), :] * weight for w in range(W)]
        cross = []
        for i, w in pairs:
            z_real = z_buf[i, w, pl.ds(0, bin_rows, stride=2), :]
            z_imag = z_buf[i, w, pl.ds(1, bin_rows, stride=2), :]
            cross.append(jnp.concatenate(
                [z_real * n_real[w] + z_imag * n_imag[w], z_imag * n_real[w] - z_real * n_imag[w]], 0
            ).astype(jnp.bfloat16))
        short = jnp.dot(inner[...], jnp.concatenate(cross, 1), preferred_element_type=jnp.float32)
        turned = []
        for at in range(len(pairs)):
            real = short[:period, at * LANES:(at + 1) * LANES]
            imag = short[period:, at * LANES:(at + 1) * LANES]
            for part in range(LANES // period):
                cosine = turn[0, part * period:(part + 1) * period, :]
                sine = turn[1, part * period:(part + 1) * period, :]
                turned.append(jnp.concatenate(
                    [real * cosine - imag * sine, real * sine + imag * cosine], 1).astype(jnp.bfloat16))
        lags = lax.dot_general(outer[...], jnp.concatenate(turned, 0), (((1,), (1,)), ((), ())),
                               preferred_element_type=jnp.float32)
        lags = lags[:blocks] + lags[blocks:]
        n_flag = nf_buf[owner].astype(jnp.float32)
        mask = mask_buf[...].astype(jnp.float32)
        here = lax.broadcasted_iota(jnp.int32, mask.shape, 1) == owner
        kept = jnp.sum(jnp.where(here, mask, 0.0), axis=1, keepdims=True)
        for i in range(C):
            marks = zf_buf[i].astype(jnp.float32) * n_flag
            count = jnp.maximum(jnp.sum(marks, axis=1, keepdims=True), 1.0)
            gain = marks * kept[i:i + 1] / count
            total = jnp.zeros((blocks, LANES), jnp.float32)
            for w in range(W):
                at = i * W + w
                corr = lags[:, at * LANES:(at + 1) * LANES]
                power = jnp.sum(jnp.sum(corr * corr, axis=0, keepdims=True), axis=1, keepdims=True)
                spread = jnp.sqrt(power / LAGS + 1e-05)
                total = total + corr * (gain[:, w:w + 1] / spread)
            out_ref[pl.ds(i * blocks * R + owner, blocks, stride=R), :] = total

    def arrive(owner, w, forward, send, f_send, to):
        if w == 0:
            flag(owner, f_send, to).wait_recv()
        spectrum(owner, w, send, to).wait_recv()
        if forward is False:
            return

        @pl.when(forward)
        def _():
            if w == 0:
                flag(owner, f_send, to).start()
            spectrum(owner, w, send, to).start()

    for step in range(1, C):
        zf_copy(lax.rem(col + C - step, C), lax.rem(col + step, C)).wait_recv()
    for w in range(W):
        for step in range(1, C):
            z_copy(lax.rem(col + C - step, C), w, lax.rem(col + step, C)).wait_recv()
    unit(row)

    def take(p):
        left = p <= row
        owner = jnp.where(left, row - p, p)
        if reach == R - 1:
            for w in range(W):
                arrive(owner, w, False, right_send, rf_send, lax.rem(row + 1, R))
        else:
            @pl.when(left)
            def _():
                for w in range(W):
                    arrive(owner, w, has_right & (p >= reach), right_send, rf_send, lax.rem(row + 1, R))

            @pl.when(p > row)
            def _():
                for w in range(W):
                    arrive(owner, w, has_left & (p - row >= reach), left_send, lf_send,
                           lax.rem(row + R - 1, R))
        unit(owner)

    if R <= 4:
        for p in range(1, R):
            take(p)
    else:
        pl.loop(1, R)(take)

    hops = [sign * hop for hop in range(1, reach + 1) for sign in (1, -1)]
    for hop in hops:
        @pl.when(there(hop))
        def _():
            own_flag(hop).wait_send()
            if hop > 0:
                for w in range(W):
                    own_copy(hop, w).wait_send()
            else:
                waited = first & ((row == -hop) | ((row > -hop) & (-hop == reach)))

                @pl.when(jnp.logical_not(waited))
                def _():
                    for w in range(W):
                        own_copy(hop, w).wait_send()

    for step in range(1, C):
        zf_copy(col, lax.rem(col + step, C)).wait_send()
        for w in range(W):
            z_copy(col, w, lax.rem(col + step, C)).wait_send()

    if reach == R - 1:
        return

    @pl.loop(0, R)
    def _(owner):
        @pl.when(has_right & (owner <= row - reach))
        def _():
            flag(owner, rf_send, lax.rem(row + 1, R)).wait_send()
            for w in range(W):
                spectrum(owner, w, right_send, lax.rem(row + 1, R)).wait_send()

        @pl.when(has_left & (owner >= row + reach))
        def _():
            flag(owner, lf_send, lax.rem(row + R - 1, R)).wait_send()
            for w in range(W):
                spectrum(owner, w, left_send, lax.rem(row + R - 1, R)).wait_send()


def far_body(R, C, z_spectra, n_spectra, z_flags, n_flags, pair_mask):
    windows, bins = z_spectra.shape[1], z_spectra.shape[3]
    rows, blocks = bins // LANES, LAGS // LANES
    inner, turn, outer = far_tables(bins)

    def interleave(x):
        return x.reshape(1, windows, 2, rows, LANES).transpose(0, 1, 3, 2, 4).reshape(
            1, windows, 2 * rows, LANES)

    reach = min(REACH, R - 1)
    DMA = pltpu.SemaphoreType.DMA
    out = pl.pallas_call(
        functools.partial(far_kernel, R, C, reach),
        out_shape=pltpu.VMEM((C * blocks * R, LANES), jnp.float32),
        in_specs=[pl.BlockSpec(memory_space=pl.ANY)] * 8,
        out_specs=pl.BlockSpec(memory_space=pltpu.VMEM),
        scratch_shapes=[
            pltpu.VMEM((C, windows, 2 * rows, LANES), jnp.float32),
            pltpu.VMEM((R, windows, 2 * rows, LANES), jnp.float32),
            pltpu.VMEM((C, 1, windows), jnp.int32),
            pltpu.VMEM((R, 1, windows), jnp.int32),
            pltpu.VMEM(pair_mask.shape, jnp.int32),
            pltpu.VMEM(inner.shape, jnp.bfloat16),
            pltpu.VMEM(turn.shape, jnp.float32),
            pltpu.VMEM(outer.shape, jnp.bfloat16),
            DMA((8,)),
            DMA((C, windows)), DMA((C, windows)), DMA((C,)), DMA((C,)),
            DMA((R, windows)), DMA((R, windows)), DMA((R, windows)),
            DMA((R,)), DMA((R,)), DMA((R,)),
            DMA((2, reach, windows)), DMA((2, reach)), pltpu.SemaphoreType.REGULAR((2, reach + 1)),
            pltpu.SemaphoreType.REGULAR,
        ],
        compiler_params=pltpu.CompilerParams(collective_id=0, has_side_effects=True),
        name="correlate",
    )(interleave(z_spectra), interleave(n_spectra), z_flags, n_flags, pair_mask,
      jnp.asarray(inner), jnp.asarray(turn), jnp.asarray(outer))
    return out.reshape(C, blocks, R, LANES).transpose(0, 2, 1, 3).reshape(C, R, LAGS)


def solution(mesh):
    placed = (
        P(("grp", "row", "col"), None, None, None),
        P(("grp", "col", "row"), None, None, None),
        P(("grp", "row", "col"), None),
        P(("grp", "col", "row"), None),
        P(("grp", "row"), "col"),
    )
    return jax.shard_map(
        functools.partial(body, mesh.shape["row"], mesh.shape["col"]), mesh=mesh,
        in_specs=placed, out_specs=P(("grp", "row"), "col", None), check_vma=False,
    )
```
